32 devices in a mesh: batch: 4 (over y, x), seq: 8 (over z, core).
Axes of the slice: x: 2, y: 2, z: 4, core: 2. Of those that a mesh axis runs over, the one named last changes fastest.
Arguments:
- inputs: bfloat16 [16, 3072, 512], P('batch', 'seq'), may hold values from -6 to 6
- cotangent: bfloat16 [16, 3072, 512], P('batch', 'seq'), may hold values from -6 to 6
- doc_lengths: int32 [16, 8], P('batch'), may hold values from 1 to 1536, 3072 in all within a row
- pool_weight: bfloat16 [1536, 512], replicated, may hold values from -0.15625 to 0.15625
- pool_bias: float32 [512], replicated, may hold values from -3 to 3
- gain_one: float32 [512], replicated, may hold values from 0.25 to 1.75
- shift_one: float32 [512], replicated, may hold values from -1.75 to 1.75
- query_weight: bfloat16 [512, 512], replicated, may hold values from -0.375 to 0.375
- key_weight: bfloat16 [512, 512], replicated, may hold values from -0.375 to 0.375
- value_weight: bfloat16 [512, 512], replicated, may hold values from -0.25 to 0.25
- out_weight: bfloat16 [512, 512], replicated, may hold values from -0.75 to 0.75
- slopes: float32 [8], replicated, may hold values from 0.0003 to 0.1
- gain_two: float32 [512], replicated, may hold values from 0.25 to 1.75
- shift_two: float32 [512], replicated, may hold values from -1.75 to 1.75
- inner_weight: bfloat16 [512, 2048], replicated, may hold values from -0.25 to 0.25
- inner_bias: float32 [2048], replicated, may hold values from -3 to 3
- outer_weight: bfloat16 [2048, 512], replicated, may hold values from -0.125 to 0.125
- outer_bias: float32 [512], replicated, may hold values from -3 to 3
- up_weight: bfloat16 [512, 1536], replicated, may hold values from -0.25 to 0.25
- up_bias: float32 [1536], replicated, may hold values from -3 to 3
Outputs:
- output: bfloat16 [16, 3072, 512], P('batch', 'seq')
- input_grad: float32 [16, 3072, 512], P('batch', 'seq')
- grad_pool_weight: float32 [1536, 512], replicated
- grad_pool_bias: float32 [512], replicated
- grad_gain_one: float32 [512], replicated
- grad_shift_one: float32 [512], replicated
- grad_query_weight: float32 [512, 512], replicated
- grad_key_weight: float32 [512, 512], replicated
- grad_value_weight: float32 [512, 512], replicated
- grad_out_weight: float32 [512, 512], replicated
- grad_slopes: float32 [8], replicated
- grad_gain_two: float32 [512], replicated
- grad_shift_two: float32 [512], replicated
- grad_inner_weight: float32 [512, 2048], replicated
- grad_inner_bias: float32 [2048], replicated
- grad_outer_weight: float32 [2048, 512], replicated
- grad_outer_bias: float32 [512], replicated
- grad_up_weight: float32 [512, 1536], replicated
- grad_up_bias: float32 [1536], replicated
The draws below stay inside these ranges and needn't reach their ends.
Inputs may be any that keep to these rules, and one draw needn't show every extreme that they name: `doc_lengths`: the 8 document lengths of each row sum to 3072.
All inputs are finite; a program needn't handle non-finite values.
Results may differ from the reference program's by a relative error of at most 0.015.
Values may be sent and summed in bfloat16 or wider, within the bound.
A program may use at most 256 MiB of HBM per device.

```python
import math
import jax
import jax.numpy as jnp
import numpy as np
from jax import lax

D = 512
HEADS = 8
FF = 2048
NDOC = 8
ROWS = 16
ROW_LEN = 3072


def block_scale(stream_key, extent, cuts, least, high):
    factor_of = 1.0
    for position, blocks in cuts:
        draws = jax.random.uniform(jax.random.fold_in(jax.random.fold_in(stream_key, 6), position), (blocks,), jnp.float32, least / len(cuts), high / len(cuts))
        factor_of = factor_of * jnp.repeat(jnp.exp(draws), extent[position] // blocks).reshape((-1,) + (1,) * (len(extent) - 1 - position))
    return factor_of


def profile(amount, total, bound, lean):
    loads = [(1 << 20) // math.isqrt(rank ** lean) + 1 for rank in range(2, amount + 1)]
    rest, given = total - bound - (amount - 1), [1] * (amount - 1)
    while rest > 0:
        movable = [i for i in range(amount - 1) if given[i] < bound]
        whole, remaining = sum([loads[i] for i in movable]), rest
        for i in movable:
            more = min(bound - given[i], max(1, remaining * loads[i] // whole), rest)
            given[i] = given[i] + more
            rest = rest - more
    return np.array([bound] + given)


def ragged(stream_key, count, total, limit, skew):
    if count == 2:
        one = jax.random.randint(stream_key, (), max(1, total - limit), min(limit, total - 1) + 1)
        return jnp.stack([one, total - one])
    sizes = jnp.asarray(profile(count, total, limit, skew), jnp.int32)
    pairs = (count - 1) // 2
    source_of, sink = sizes[1:1 + 2 * pairs:2], sizes[2:2 + 2 * pairs:2]
    room = jnp.minimum(source_of - 1, limit - sink)
    moved = jax.random.randint(jax.random.fold_in(stream_key, 1), (pairs,), 0, 1 << 20) % (room + 1)
    sizes = sizes.at[1:1 + 2 * pairs:2].set(source_of - moved).at[2:2 + 2 * pairs:2].set(sink + moved)
    return sizes[jax.random.permutation(jax.random.fold_in(stream_key, 2), count)]


def centred(key, dims, deviation, reach, shards=(), kind=jnp.bfloat16):
    loudness = block_scale(key, dims, shards, -0.22, 0.18) if shards else 1.0
    drawn = jax.random.normal(key, dims, jnp.float32) * deviation * loudness
    return jnp.minimum(jnp.maximum(drawn, -reach), reach).astype(kind)


def setup_inputs(seed: int = 0) -> dict:
    streams_of = jax.random.split(jax.random.key(seed), 21)
    inputs = centred(streams_of[0], (ROWS, ROW_LEN, D), 1.0, 6.0, ((0, 4), (1, 8)))
    cotangent = centred(streams_of[1], (ROWS, ROW_LEN, D), 1.0, 6.0, ((0, 4), (1, 8)))
    doc_lengths = jax.vmap(lambda own: ragged(own, NDOC, ROW_LEN, ROW_LEN // 2, 2))(jax.random.split(streams_of[2], ROWS)).reshape((ROWS, NDOC)).astype(jnp.int32)
    pool_weight = centred(streams_of[3], (3 * D, D), (3 * D) ** -0.5, 0.15625)
    pool_bias = centred(streams_of[4], (D,), 0.5, 3.0, (), jnp.float32)
    gain_one = jnp.clip(1.0 + 0.15 * jax.random.normal(streams_of[5], (D,), jnp.float32), 0.25, 1.75)
    shift_one = centred(streams_of[6], (D,), 0.3, 1.75, (), jnp.float32)
    query_weight = centred(streams_of[7], (D, D), (D // 2) ** -0.5, 0.375)
    key_weight = centred(streams_of[8], (D, D), (D // 2) ** -0.5, 0.375)
    value_weight = centred(streams_of[9], (D, D), D ** -0.5, 0.25)
    out_weight = centred(streams_of[10], (D, D), (D // 8) ** -0.5, 0.75)
    slopes = jnp.clip(jnp.exp(jax.random.uniform(streams_of[11], (HEADS,), jnp.float32, math.log(0.0003), math.log(0.1))), 0.0003, 0.1)
    gain_two = jnp.clip(1.0 + 0.15 * jax.random.normal(streams_of[12], (D,), jnp.float32), 0.25, 1.75)
    shift_two = centred(streams_of[13], (D,), 0.3, 1.75, (), jnp.float32)
    inner_weight = centred(streams_of[14], (D, FF), D ** -0.5, 0.25)
    inner_bias = centred(streams_of[15], (FF,), 0.5, 3.0, (), jnp.float32)
    outer_weight = centred(streams_of[16], (FF, D), FF ** -0.5, 0.125)
    outer_bias = centred(streams_of[17], (D,), 0.5, 3.0, (), jnp.float32)
    up_weight = centred(streams_of[18], (D, 3 * D), D ** -0.5, 0.25)
    up_bias = centred(streams_of[19], (3 * D,), 0.5, 3.0, (), jnp.float32)
    return {"inputs": inputs, "cotangent": cotangent, "doc_lengths": doc_lengths, "pool_weight": pool_weight, "pool_bias": pool_bias, "gain_one": gain_one, "shift_one": shift_one, "query_weight": query_weight, "key_weight": key_weight, "value_weight": value_weight, "out_weight": out_weight, "slopes": slopes, "gain_two": gain_two, "shift_two": shift_two, "inner_weight": inner_weight, "inner_bias": inner_bias, "outer_weight": outer_weight, "outer_bias": outer_bias, "up_weight": up_weight, "up_bias": up_bias}


@jax.custom_vjp
def low(v):
    return lax.optimization_barrier(v.astype(jnp.bfloat16)).astype(jnp.float32)

@jax.custom_vjp
def low_back(v):
    return v

def low_keep(v):
    return (low(v), None)

def low_pass(kept, grad):
    return (grad,)

def back_keep(v):
    return (v, None)

def back_low(kept, grad):
    return (low(grad),)
low.defvjp(low_keep, low_pass)
low_back.defvjp(back_keep, back_low)
norm_eps = 1e-05

def matmul(left, right):
    return jnp.dot(left, right, precision=lax.Precision.HIGHEST)

def norm_rows(values_in, norm_gain, norm_shift):
    centre = values_in - lax.optimization_barrier(jnp.mean(values_in, axis=-1, keepdims=True))
    spread = lax.optimization_barrier(jnp.mean(centre * centre, axis=-1, keepdims=True))
    return centre * lax.rsqrt(spread + norm_eps) * norm_gain + norm_shift

def forward(weights, row_bytes, lengths):
    pool_weight, pool_bias, gain_one, shift_one, query_weight, key_weight, value_weight, out_weight, slopes, gain_two, shift_two, inner_weight, inner_bias, outer_weight, outer_bias, up_weight, up_bias = weights
    row_len = row_bytes.shape[0]
    feature_width = row_bytes.shape[1]
    short_len = row_len // 3
    head_count = slopes.shape[0]
    head_dim = feature_width // head_count
    score_scale = head_dim ** (-0.5)
    shifted = jnp.concatenate([jnp.zeros((2, feature_width), jnp.float32), row_bytes[:-2]], axis=0)
    groups = shifted.reshape(short_len, 3 * feature_width)
    pooled = low_back(matmul(groups, pool_weight) + pool_bias)
    normed_one = low(norm_rows(pooled, gain_one, shift_one))
    query = low(low_back(matmul(normed_one, query_weight))).reshape(short_len, head_count, head_dim)
    key_rows = low(low_back(matmul(normed_one, key_weight))).reshape(short_len, head_count, head_dim)
    value_rows = low(low_back(matmul(normed_one, value_weight))).reshape(short_len, head_count, head_dim)
    doc_ends = jnp.cumsum(lengths)
    positions = jnp.arange(short_len, dtype=jnp.int32)
    doc_ids = lax.optimization_barrier(jnp.sum((doc_ends[None, :] <= 3 * positions[:, None]).astype(jnp.int32), axis=1))
    distance = (positions[:, None] - positions[None, :]).astype(jnp.float32)
    allowed = (distance >= 0.0) & (doc_ids[:, None] == doc_ids[None, :])
    raw_scores = jnp.einsum('qhd,khd->hqk', query, key_rows, precision=lax.Precision.HIGHEST) * score_scale
    raw_scores = raw_scores - slopes[:, None, None] * distance[None]
    masked = jnp.where(allowed[None], low_back(raw_scores), -1e+30)
    probs = low(jax.nn.softmax(masked, axis=-1))
    attended = jnp.einsum('hqk,khd->qhd', probs, value_rows, precision=lax.Precision.HIGHEST)
    attended = low(low_back(attended.reshape(short_len, feature_width)))
    residual_one = pooled + low_back(matmul(attended, out_weight))
    normed_two = low(norm_rows(residual_one, gain_two, shift_two))
    inner_sum = low_back(matmul(normed_two, inner_weight) + inner_bias)
    activated = low(jax.nn.gelu(inner_sum, approximate=False))
    residual_two = residual_one + low_back(matmul(activated, outer_weight) + outer_bias)
    raised = low_back(matmul(low(residual_two), up_weight) + up_bias)
    return row_bytes + raised.reshape(row_len, feature_width)

def reference(inputs, cotangent, doc_lengths, pool_weight, pool_bias, gain_one, shift_one, query_weight, key_weight, value_weight, out_weight, slopes, gain_two, shift_two, inner_weight, inner_bias, outer_weight, outer_bias, up_weight, up_bias):
    weights = tuple((item.astype(jnp.float32) for item in (pool_weight, pool_bias, gain_one, shift_one, query_weight, key_weight, value_weight, out_weight, slopes, gain_two, shift_two, inner_weight, inner_bias, outer_weight, outer_bias, up_weight, up_bias)))

    def one_row(carry, item):
        row_bytes, row_grad, lengths = item

        def apply(weight_set, row_in):
            return forward(weight_set, row_in, lengths)
        value_out, backward = jax.vjp(apply, weights, row_bytes.astype(jnp.float32))
        grad_weights, grad_row = backward(row_grad.astype(jnp.float32))
        summed = tuple((before + after for before, after in zip(carry, grad_weights)))
        return (summed, (value_out.astype(jnp.bfloat16), grad_row))
    start = tuple((jnp.zeros_like(item) for item in weights))
    totals, (output, input_grad) = lax.scan(one_row, start, (inputs, cotangent, doc_lengths))
    return (output, input_grad, totals[0], totals[1], totals[2], totals[3], totals[4], totals[5], totals[6], totals[7], totals[8], totals[9], totals[10], totals[11], totals[12], totals[13], totals[14], totals[15], totals[16])
```

```python
import functools
import math

import jax
import jax.numpy as jnp
from jax import lax
from jax.experimental import pallas as pl
from jax.experimental.pallas import tpu as pltpu
from jax.sharding import PartitionSpec as P

norm_eps = 1e-05

MESH = pl.DeviceIdType.MESH
half = jnp.bfloat16
full = jnp.float32


class Place:
    def __init__(self, batch_size, seq_size):
        side = math.isqrt(batch_size)
        self.depth = seq_size // 2
        self.batch = lax.axis_index("batch")
        self.seq = lax.axis_index("seq")
        self.core = self.seq % 2
        self.level = self.seq // 2
        high, low = self.batch // side, self.batch % side
        self.first = jnp.where(self.core == 0, low, high)
        self.second = jnp.where(self.core == 0, high, low)
        self.side = side
        self.sizes = (2, side, side, self.depth)
        self.where = (self.core, self.first, self.second, self.level)

    def batch_at(self, first, second):
        return jnp.where(
            self.core == 0, second * self.side + first, first * self.side + second
        )

    def partner(self, stage, step):
        member = (self.where[stage] + step) % self.sizes[stage]
        if stage == 0:
            return (self.batch, self.level * 2 + member)
        if stage == 1:
            return (self.batch_at(member, self.second), self.seq)
        if stage == 2:
            return (self.batch_at(self.first, member), self.seq)
        return (self.batch, member * 2 + self.core)

    def partners(self):
        return [
            self.partner(stage, step)
            for stage in range(4)
            for step in range(1, self.sizes[stage])
        ]


def sum_slots(batch_size, seq_size):
    return 1 + 2 * (math.isqrt(batch_size) - 1) + seq_size // 2 - 1


class SumPieces:
    def __init__(self, place, chunks, mine, landing, out, sems):
        self.place, self.chunks = place, chunks
        self.mine, self.landing, self.out = mine, landing, out
        self.sent, self.got, self.back_sent, self.back_got = sems
        self.starts = [sum(chunks[:c]) for c in range(len(chunks))]
        sizes = place.sizes
        self.slot = [sum(s - 1 for s in sizes[:stage]) for stage in range(4)]
        self.land = {}
        at = 0
        for c in range(len(chunks)):
            for stage in range(4):
                for step in range(1, sizes[stage]):
                    self.land[c, stage, step] = at
                    at += self.rows(c, stage)

    @staticmethod
    def landing_rows(batch_size, seq_size, chunks):
        side = math.isqrt(batch_size)
        rows, left = 0, sum(chunks)
        for size in (2, side, side, seq_size // 2):
            left //= size
            rows += left * (size - 1)
        return rows

    def rows(self, c, stage):
        count = self.chunks[c]
        for size in self.place.sizes[: stage + 1]:
            count //= size
        return count

    def begin(self, c, stage):
        at = self.starts[c]
        for t in range(stage):
            at = at + self.place.where[t] * self.rows(c, t)
        return at

    def scatter(self, c, stage, step):
        count = self.rows(c, stage)
        member = (self.place.where[stage] + step) % self.place.sizes[stage]
        at = pl.multiple_of(self.begin(c, stage) + member * count, 16)
        slot = self.slot[stage] + step - 1
        return pltpu.make_async_remote_copy(
            src_ref=self.mine.at[pl.ds(at, count), :],
            dst_ref=self.landing.at[pl.ds(self.land[c, stage, step], count), :],
            send_sem=self.sent.at[c, slot],
            recv_sem=self.got.at[c, slot],
            device_id=self.place.partner(stage, step),
            device_id_type=MESH,
        )

    def gather(self, c, stage, step):
        count = self.rows(c, stage)
        at = pl.multiple_of(self.begin(c, stage + 1), 16)
        slot = self.slot[stage] + step - 1
        return pltpu.make_async_remote_copy(
            src_ref=self.out.at[pl.ds(at, count), :],
            dst_ref=self.out.at[pl.ds(at, count), :],
            send_sem=self.back_sent.at[c, slot],
            recv_sem=self.back_got.at[c, slot],
            device_id=self.place.partner(stage, step),
            device_id_type=MESH,
        )

    def add(self, c, stage):
        count = self.rows(c, stage)
        at = self.begin(c, stage + 1)
        target = self.out if stage == 3 else self.mine
        part = min(count, 128)

        def body(i, carry):
            here = pl.multiple_of(at + i * part, 16)
            total = self.mine[pl.ds(here, part), :].astype(full)
            for step in range(1, self.place.sizes[stage]):
                there = pl.multiple_of(self.land[c, stage, step] + i * part, 16)
                total = total + self.landing[pl.ds(there, part), :].astype(full)
            target[pl.ds(here, part), :] = total.astype(half)
            return carry

        lax.fori_loop(0, count // part, body, 0)

    def steps(self, stage):
        return range(1, self.place.sizes[stage])

    def advance(self, c, event):
        if 1 <= event <= 4:
            for step in self.steps(event - 1):
                self.scatter(c, event - 1, step).wait_recv()
            self.add(c, event - 1)
        if event <= 3:
            for step in self.steps(event):
                self.scatter(c, event, step).start()
        else:
            stage = 7 - event
            if event >= 5:
                for step in self.steps(stage + 1):
                    self.gather(c, stage + 1, step).wait_recv()
            if event <= 7:
                for step in self.steps(stage):
                    self.gather(c, stage, step).start()

    def finish(self):
        for c in range(len(self.chunks)):
            for stage in range(4):
                for step in self.steps(stage):
                    self.scatter(c, stage, step).wait_send()
                    self.gather(c, stage, step).wait_send()


class SumSmall:
    def __init__(self, place, block, landing, sems):
        self.place, self.block, self.landing = place, block, landing
        self.sent, self.got = sems
        sizes = place.sizes
        self.slot = [sum(s - 1 for s in sizes[:stage]) for stage in range(4)]
        self.base = [sum(sizes[:stage]) for stage in range(4)]

    def copy(self, stage, step):
        slot = self.slot[stage] + step - 1
        return pltpu.make_async_remote_copy(
            src_ref=self.block.at[stage],
            dst_ref=self.landing.at[self.base[stage] + self.place.where[stage]],
            send_sem=self.sent.at[slot],
            recv_sem=self.got.at[slot],
            device_id=self.place.partner(stage, step),
            device_id_type=MESH,
        )

    def send(self, stage):
        self.landing[self.base[stage] + self.place.where[stage]] = self.block[stage]
        for step in range(1, self.place.sizes[stage]):
            self.copy(stage, step).start()

    def receive(self, stage):
        for step in range(1, self.place.sizes[stage]):
            self.copy(stage, step).wait_recv()
        total = self.landing[self.base[stage]]
        for member in range(1, self.place.sizes[stage]):
            total = total + self.landing[self.base[stage] + member]
        self.block[stage + 1] = total

    def finish(self):
        for stage in range(4):
            for step in range(1, self.place.sizes[stage]):
                self.copy(stage, step).wait_send()


def sum_kernel(batch_size, seq_size, chunks, lag, big_ref, small_ref, big_out, small_out,
               mine, landing, small_block, small_landing, *sems):
    place = Place(batch_size, seq_size)
    barrier = pltpu.get_barrier_semaphore()
    partners = place.partners()
    for device in partners:
        pl.semaphore_signal(barrier, inc=1, device_id=device, device_id_type=MESH)
    pl.semaphore_wait(barrier, len(partners))
    load = pltpu.make_async_copy(big_ref, mine, sems[6])
    load.start()
    small_block[0] = small_ref[...]
    small = SumSmall(place, small_block, small_landing, sems[4:6])
    big = SumPieces(place, chunks, mine, landing, big_out, sems[:4])
    load.wait()
    for t in range(len(chunks) + 8 * lag):
        for event in reversed(range(9)):
            c = t - event * lag
            if 0 <= c < len(chunks):
                big.advance(c, event)
        if t % 2 == 0 and t // 2 <= 4:
            if t >= 2:
                small.receive(t // 2 - 1)
            if t // 2 < 4:
                small.send(t // 2)
    small_out[...] = small_block[4]
    big.finish()
    small.finish()


def sum_over_devices(big, small):
    batch_size, seq_size = lax.axis_size("batch"), lax.axis_size("seq")
    rows = big.shape[0]
    chunks = [4096] * (rows // 4096)
    slots = sum_slots(batch_size, seq_size)
    small_rows = small.shape[0]
    members = 2 + 2 * math.isqrt(batch_size) + seq_size // 2
    vmem = pl.BlockSpec(memory_space=pltpu.VMEM)
    return pl.pallas_call(
        functools.partial(sum_kernel, batch_size, seq_size, chunks, 2),
        out_shape=(
            jax.ShapeDtypeStruct(big.shape, half),
            jax.ShapeDtypeStruct(small.shape, full),
        ),
        in_specs=[pl.BlockSpec(memory_space=pl.ANY), vmem],
        out_specs=(vmem, vmem),
        scratch_shapes=[
            pltpu.VMEM(big.shape, half),
            pltpu.VMEM((SumPieces.landing_rows(batch_size, seq_size, chunks), 128), half),
            pltpu.VMEM((5, small_rows, 128), full),
            pltpu.VMEM((members, small_rows, 128), full),
        ]
        + [pltpu.SemaphoreType.DMA((len(chunks), slots))] * 4
        + [pltpu.SemaphoreType.DMA((slots,))] * 2
        + [pltpu.SemaphoreType.DMA],
        compiler_params=pltpu.CompilerParams(
            collective_id=0, has_side_effects=True, vmem_limit_bytes=60 * 1024 * 1024
        ),
        name="sum_over_devices",
    )(big, small)


def sum_grads(grads):
    big_names = [i for i, g in enumerate(grads) if g.ndim == 2]
    small_names = [i for i, g in enumerate(grads) if g.ndim == 1]
    big = jnp.concatenate(
        [
            grads[i][:, j : j + 128].astype(half)
            for i in big_names
            for j in range(0, grads[i].shape[1], 128)
        ],
        axis=0,
    )
    flat = jnp.concatenate([grads[i] for i in small_names])
    small_rows = -(-flat.shape[0] // 1024) * 8
    flat = jnp.pad(flat, (0, small_rows * 128 - flat.shape[0])).reshape(small_rows, 128)
    big, flat = sum_over_devices(big, flat)
    flat = flat.reshape(-1)
    out = list(grads)
    at = 0
    for i in big_names:
        rows, columns = grads[i].shape
        parts = []
        for j in range(columns // 128):
            parts.append(big[at : at + rows].astype(full))
            at += rows
        out[i] = jnp.concatenate(parts, axis=1)
    at = 0
    for i in small_names:
        count = grads[i].shape[0]
        out[i] = flat[at : at + count]
        at += count
    return tuple(out)


def shifted_2(block, axis, distance):
    devices = range(lax.axis_size(axis))
    route = [(i - distance, i) for i in devices if i - distance in devices]
    return lax.ppermute(block, axis, route)


def matmul(left, right):
    return jnp.dot(left, right, preferred_element_type=jnp.float32)


def norm_rows(values_in, norm_gain, norm_shift):
    centre = values_in - jnp.mean(values_in, axis=-1, keepdims=True)
    spread = jnp.mean(centre * centre, axis=-1, keepdims=True)
    return centre * lax.rsqrt(spread + norm_eps) * norm_gain + norm_shift


def exact_gelu(values_in):
    return jax.nn.gelu(values_in, approximate=False)


def masked_scores(query_heads, key_heads, slopes, distance, allowed, score_scale):
    raw_scores = jnp.einsum(
        "rqhd,rkhd->rhqk", query_heads, key_heads, preferred_element_type=jnp.float32
    )
    raw_scores = raw_scores * score_scale - slopes[None, :, None, None] * distance[None, None]
    return jnp.where(allowed[:, None], raw_scores, -1e30)


def local(
    inputs,
    cotangent,
    doc_lengths,
    pool_weight,
    pool_bias,
    gain_one,
    shift_one,
    query_weight,
    key_weight,
    value_weight,
    out_weight,
    slopes,
    gain_two,
    shift_two,
    inner_weight,
    inner_bias,
    outer_weight,
    outer_bias,
    up_weight,
    up_bias,
):
    row_count, block_len, feature_width = inputs.shape
    short_len = block_len // 3
    head_count = slopes.shape[0]
    head_dim = feature_width // head_count
    score_scale = head_dim ** (-0.5)
    total_short = short_len * lax.axis_size("seq")
    offset = lax.axis_index("seq") * short_len
    token_count = row_count * short_len
    left_rim = shifted_2(inputs[:, block_len - 2 :, :], "seq", 1)
    shifted = jnp.concatenate([left_rim, inputs[:, : block_len - 2, :]], axis=1)
    groups = shifted.reshape(token_count, 3 * feature_width)
    pooled = matmul(groups, pool_weight) + pool_bias
    normed_one = norm_rows(pooled, gain_one, shift_one).astype(jnp.bfloat16)
    query = matmul(normed_one, query_weight).astype(jnp.bfloat16)
    key_rows = matmul(normed_one, key_weight).astype(jnp.bfloat16)
    value_rows = matmul(normed_one, value_weight).astype(jnp.bfloat16)
    doc_ends = jnp.cumsum(doc_lengths, axis=1)
    key_places = jnp.arange(total_short, dtype=jnp.int32)
    key_docs = jnp.sum(
        (doc_ends[:, None, :] <= 3 * key_places[None, :, None]).astype(jnp.int32), axis=2
    )
    query_docs = lax.dynamic_slice_in_dim(key_docs, offset, short_len, 1)
    query_places = offset + jnp.arange(short_len, dtype=jnp.int32)
    distance = (query_places[:, None] - key_places[None, :]).astype(jnp.float32)
    allowed = (distance >= 0.0)[None] & (query_docs[:, :, None] == key_docs[:, None, :])
    key_block = key_rows.reshape(row_count, short_len, feature_width)
    value_block = value_rows.reshape(row_count, short_len, feature_width)
    all_keys, all_values = (
        lax.all_gather(key_block, "seq", axis=1, tiled=True),
        lax.all_gather(value_block, "seq", axis=1, tiled=True),
    )
    query_heads = query.reshape(row_count, short_len, head_count, head_dim)
    key_heads = all_keys.reshape(row_count, total_short, head_count, head_dim)
    value_heads = all_values.reshape(row_count, total_short, head_count, head_dim)
    scores = masked_scores(query_heads, key_heads, slopes, distance, allowed, score_scale)
    row_top = jnp.max(scores, axis=-1, keepdims=True)
    exponent = jnp.exp(scores - row_top)
    row_total = jnp.sum(exponent, axis=-1, keepdims=True)
    log_total = row_top + jnp.log(row_total)
    probs_low = (exponent / row_total).astype(jnp.bfloat16)
    attended = jnp.einsum(
        "rhqk,rkhd->rqhd", probs_low, value_heads, preferred_element_type=jnp.float32
    )
    attended = attended.reshape(token_count, feature_width).astype(jnp.bfloat16)
    residual_one = pooled + matmul(attended, out_weight)
    normed_two = norm_rows(residual_one, gain_two, shift_two).astype(jnp.bfloat16)
    inner_sum = matmul(normed_two, inner_weight) + inner_bias
    activated = exact_gelu(inner_sum).astype(jnp.bfloat16)
    residual_two = residual_one + matmul(activated, outer_weight) + outer_bias
    residual_low = residual_two.astype(jnp.bfloat16)
    raised = matmul(residual_low, up_weight) + up_bias
    output = (
        inputs.astype(jnp.float32) + raised.reshape(row_count, block_len, feature_width)
    ).astype(jnp.bfloat16)
    grad_raised = cotangent.reshape(token_count, 3 * feature_width)
    grad_up_weight = matmul(residual_low.T, grad_raised)
    grad_up_bias = jnp.sum(grad_raised.astype(jnp.float32), axis=0)
    grad_resid = matmul(grad_raised, up_weight.T)
    grad_branch = grad_resid.astype(jnp.bfloat16)
    grad_outer_weight = matmul(activated.T, grad_branch)
    grad_outer_bias = jnp.sum(grad_branch.astype(jnp.float32), axis=0)
    grad_active = matmul(grad_branch, outer_weight.T)
    unused_gelu, gelu_back = jax.vjp(exact_gelu, inner_sum)
    grad_inner = gelu_back(grad_active)[0].astype(jnp.bfloat16)
    grad_inner_weight = matmul(normed_two.T, grad_inner)
    grad_inner_bias = jnp.sum(grad_inner.astype(jnp.float32), axis=0)
    grad_normed_two = matmul(grad_inner, inner_weight.T)
    unused_two, norm_back_two = jax.vjp(norm_rows, residual_one, gain_two, shift_two)
    grad_mix_part, grad_gain_two, grad_shift_two = norm_back_two(grad_normed_two)
    grad_mixed = grad_resid + grad_mix_part
    grad_attn = grad_mixed.astype(jnp.bfloat16)
    grad_out_weight = matmul(attended.T, grad_attn)
    grad_attended = matmul(grad_attn, out_weight.T).astype(jnp.bfloat16)
    back_keys, back_values = (all_keys, all_values)
    key_heads = back_keys.reshape(row_count, total_short, head_count, head_dim)
    value_heads = back_values.reshape(row_count, total_short, head_count, head_dim)
    scores = masked_scores(query_heads, key_heads, slopes, distance, allowed, score_scale)
    probs = jnp.exp(scores - log_total)
    grad_heads = grad_attended.reshape(row_count, short_len, head_count, head_dim)
    grad_probs = jnp.einsum(
        "rqhd,rkhd->rhqk", grad_heads, value_heads, preferred_element_type=jnp.float32
    )
    row_term = jnp.sum(probs * grad_probs, axis=-1, keepdims=True)
    grad_scores = (probs * (grad_probs - row_term)).astype(jnp.bfloat16)
    grad_slopes = -jnp.sum(grad_scores.astype(jnp.float32) * distance[None, None], axis=(0, 2, 3))
    grad_query = jnp.einsum(
        "rhqk,rkhd->rqhd", grad_scores, key_heads, preferred_element_type=jnp.float32
    )
    grad_query = (grad_query * score_scale).reshape(token_count, feature_width).astype(jnp.bfloat16)
    grad_value_term = jnp.einsum(
        "rhqk,rqhd->rkhd",
        probs.astype(jnp.bfloat16),
        grad_heads,
        preferred_element_type=jnp.float32,
    ).reshape(row_count, total_short, feature_width)
    grad_key_term = jnp.einsum(
        "rhqk,rqhd->rkhd", grad_scores, query_heads, preferred_element_type=jnp.float32
    )
    grad_key_term = (grad_key_term * score_scale).reshape(row_count, total_short, feature_width)
    grad_keys, grad_values = (
        lax.psum_scatter(
            grad_key_term.astype(jnp.bfloat16), "seq", scatter_dimension=1, tiled=True
        ).astype(jnp.float32),
        lax.psum_scatter(
            grad_value_term.astype(jnp.bfloat16), "seq", scatter_dimension=1, tiled=True
        ).astype(jnp.float32),
    )
    grad_keys = grad_keys.reshape(token_count, feature_width).astype(jnp.bfloat16)
    grad_values = grad_values.reshape(token_count, feature_width).astype(jnp.bfloat16)
    grad_query_weight = matmul(normed_one.T, grad_query)
    grad_key_weight = matmul(normed_one.T, grad_keys)
    grad_value_weight = matmul(normed_one.T, grad_values)
    grad_normed_one = matmul(grad_query, query_weight.T) + matmul(grad_keys, key_weight.T)
    grad_normed_one = grad_normed_one + matmul(grad_values, value_weight.T)
    unused_one, norm_back_one = jax.vjp(norm_rows, pooled, gain_one, shift_one)
    grad_pool_part, grad_gain_one, grad_shift_one = norm_back_one(grad_normed_one)
    grad_pooled = (grad_mixed + grad_pool_part).astype(jnp.bfloat16)
    grad_pool_weight = matmul(groups.T, grad_pooled)
    grad_pool_bias = jnp.sum(grad_pooled.astype(jnp.float32), axis=0)
    grad_groups = matmul(grad_pooled, pool_weight.T).reshape(row_count, block_len, feature_width)
    back_rim = shifted_2(grad_groups[:, :2, :], "seq", -1)
    input_grad = cotangent.astype(jnp.float32) + jnp.concatenate(
        [grad_groups[:, 2:, :], back_rim], axis=1
    )
    local_grads = (
        grad_pool_weight,
        grad_pool_bias,
        grad_gain_one,
        grad_shift_one,
        grad_query_weight,
        grad_key_weight,
        grad_value_weight,
        grad_out_weight,
        grad_slopes,
        grad_gain_two,
        grad_shift_two,
        grad_inner_weight,
        grad_inner_bias,
        grad_outer_weight,
        grad_outer_bias,
        grad_up_weight,
        grad_up_bias,
    )
    summed = sum_grads(local_grads)
    return (output, input_grad) + tuple(summed)


def solution(mesh):
    in_specs = (
        P("batch", "seq", None),
        P("batch", "seq", None),
        P("batch", None),
        P(),
        P(),
        P(),
        P(),
        P(),
        P(),
        P(),
        P(),
        P(),
        P(),
        P(),
        P(),
        P(),
        P(),
        P(),
        P(),
        P(),
    )
    out_specs = (
        P("batch", "seq", None),
        P("batch", "seq", None),
        P(),
        P(),
        P(),
        P(),
        P(),
        P(),
        P(),
        P(),
        P(),
        P(),
        P(),
        P(),
        P(),
        P(),
        P(),
        P(),
        P(),
    )
    return jax.shard_map(local, mesh=mesh, in_specs=in_specs, out_specs=out_specs, check_vma=False)
```

```python
import functools
import math

import jax
import jax.numpy as jnp
from jax import lax
from jax.experimental import pallas as pl
from jax.experimental.pallas import tpu as pltpu
from jax.sharding import PartitionSpec as P

norm_eps = 1e-05
log2_e = math.log2(math.e)

MESH = pl.DeviceIdType.MESH
half = jnp.bfloat16
full = jnp.float32


class Place:
    def __init__(self, batch_size, seq_size):
        side = math.isqrt(batch_size)
        self.depth = seq_size // 2
        self.batch = lax.axis_index("batch")
        self.seq = lax.axis_index("seq")
        self.core = self.seq % 2
        self.level = self.seq // 2
        high, low = self.batch // side, self.batch % side
        self.first = jnp.where(self.core == 0, low, high)
        self.second = jnp.where(self.core == 0, high, low)
        self.side = side
        self.sizes = (2, side, side, self.depth)
        self.where = (self.core, self.first, self.second, self.level)

    def batch_at(self, first, second):
        return jnp.where(
            self.core == 0, second * self.side + first, first * self.side + second
        )

    def partner(self, stage, step):
        member = (self.where[stage] + step) % self.sizes[stage]
        if stage == 0:
            return (self.batch, self.level * 2 + member)
        if stage == 1:
            return (self.batch_at(member, self.second), self.seq)
        if stage == 2:
            return (self.batch_at(self.first, member), self.seq)
        return (self.batch, member * 2 + self.core)

    def partners(self):
        return [
            self.partner(stage, step)
            for stage in range(4)
            for step in range(1, self.sizes[stage])
        ]


def sum_slots(batch_size, seq_size):
    return 1 + 2 * (math.isqrt(batch_size) - 1) + seq_size // 2 - 1


class SumPieces:
    def __init__(self, place, chunks, mine, landing, piece, out, sems, keep):
        self.place, self.chunks = place, chunks
        self.mine, self.landing, self.piece, self.out = mine, landing, piece, out
        self.keep = keep
        self.sent, self.got, self.back_sent, self.back_got = sems
        self.starts = [sum(chunks[:c]) for c in range(len(chunks))]
        sizes = place.sizes
        self.slot = [sum(s - 1 for s in sizes[:stage]) for stage in range(4)]
        self.land = {}
        at = 0
        for c in range(len(chunks)):
            for stage in range(4):
                for step in range(1, sizes[stage]):
                    self.land[c, stage, step] = at
                    at += self.rows(c, stage)

    @staticmethod
    def landing_rows(batch_size, seq_size, chunks):
        side = math.isqrt(batch_size)
        rows, left = 0, sum(chunks)
        for size in (2, side, side, seq_size // 2):
            left //= size
            rows += left * (size - 1)
        return rows

    def rows(self, c, stage):
        count = self.chunks[c]
        for size in self.place.sizes[: stage + 1]:
            count //= size
        return count

    def begin(self, c, stage):
        at = self.starts[c]
        for t in range(stage):
            at = at + self.place.where[t] * self.rows(c, t)
        return at

    def scatter(self, c, stage, step):
        count = self.rows(c, stage)
        member = (self.place.where[stage] + step) % self.place.sizes[stage]
        at = pl.multiple_of(self.begin(c, stage) + member * count, 16)
        slot = self.slot[stage] + step - 1
        return pltpu.make_async_remote_copy(
            src_ref=self.mine.at[pl.ds(at, count), :],
            dst_ref=self.landing.at[pl.ds(self.land[c, stage, step], count), :],
            send_sem=self.sent.at[c, slot],
            recv_sem=self.got.at[c, slot],
            device_id=self.place.partner(stage, step),
            device_id_type=MESH,
        )

    def piece_span(self, c):
        return pl.ds(self.starts[c] * self.rows(c, 3) // self.chunks[c], self.rows(c, 3))

    def keep_copy(self, c):
        at = pl.multiple_of(self.begin(c, 4), 16)
        return pltpu.make_async_copy(
            self.piece.at[self.piece_span(c), :],
            self.out.at[pl.ds(at, self.rows(c, 3)), :],
            self.keep.at[c],
        )

    def gather(self, c, stage, step):
        count = self.rows(c, stage)
        at = pl.multiple_of(self.begin(c, stage + 1), 16)
        slot = self.slot[stage] + step - 1
        source = self.out.at[pl.ds(at, count), :]
        if stage == 3:
            source = self.piece.at[self.piece_span(c), :]
        return pltpu.make_async_remote_copy(
            src_ref=source,
            dst_ref=self.out.at[pl.ds(at, count), :],
            send_sem=self.back_sent.at[c, slot],
            recv_sem=self.back_got.at[c, slot],
            device_id=self.place.partner(stage, step),
            device_id_type=MESH,
        )

    def add(self, c, stage):
        count = self.rows(c, stage)
        at = self.begin(c, stage + 1)
        part = min(count, 128)

        def body(i, carry):
            here = pl.multiple_of(at + i * part, 16)
            total = self.mine[pl.ds(here, part), :].astype(full)
            for step in range(1, self.place.sizes[stage]):
                there = pl.multiple_of(self.land[c, stage, step] + i * part, 16)
                total = total + self.landing[pl.ds(there, part), :].astype(full)
            if stage == 3:
                first = self.piece_span(c).start
                self.piece[pl.ds(pl.multiple_of(first + i * part, 16), part), :] = total.astype(half)
            else:
                self.mine[pl.ds(here, part), :] = total.astype(half)
            return carry

        lax.fori_loop(0, count // part, body, 0)

    def steps(self, stage):
        return range(1, self.place.sizes[stage])

    def advance(self, c, event):
        if 1 <= event <= 4:
            for step in self.steps(event - 1):
                self.scatter(c, event - 1, step).wait_recv()
            self.add(c, event - 1)
        if event <= 3:
            for step in self.steps(event):
                self.scatter(c, event, step).start()
        else:
            stage = 7 - event
            if event == 4:
                self.keep_copy(c).start()
            else:
                for step in self.steps(stage + 1):
                    self.gather(c, stage + 1, step).wait_recv()
            if event == 5:
                self.keep_copy(c).wait()
            if event <= 7:
                for step in self.steps(stage):
                    self.gather(c, stage, step).start()

    def finish(self):
        for c in range(len(self.chunks)):
            for stage in range(4):
                for step in self.steps(stage):
                    self.scatter(c, stage, step).wait_send()
                    self.gather(c, stage, step).wait_send()


class SumSmall:
    def __init__(self, place, block, landing, sems):
        self.place, self.block, self.landing = place, block, landing
        self.sent, self.got = sems
        sizes = place.sizes
        self.slot = [sum(s - 1 for s in sizes[:stage]) for stage in range(4)]
        self.base = [sum(sizes[:stage]) for stage in range(4)]

    def copy(self, stage, step):
        slot = self.slot[stage] + step - 1
        return pltpu.make_async_remote_copy(
            src_ref=self.block.at[stage],
            dst_ref=self.landing.at[self.base[stage] + self.place.where[stage]],
            send_sem=self.sent.at[slot],
            recv_sem=self.got.at[slot],
            device_id=self.place.partner(stage, step),
            device_id_type=MESH,
        )

    def send(self, stage):
        self.landing[self.base[stage] + self.place.where[stage]] = self.block[stage]
        for step in range(1, self.place.sizes[stage]):
            self.copy(stage, step).start()

    def receive(self, stage):
        for step in range(1, self.place.sizes[stage]):
            self.copy(stage, step).wait_recv()
        total = self.landing[self.base[stage]]
        for member in range(1, self.place.sizes[stage]):
            total = total + self.landing[self.base[stage] + member]
        self.block[stage + 1] = total

    def finish(self):
        for stage in range(4):
            for step in range(1, self.place.sizes[stage]):
                self.copy(stage, step).wait_send()


def dot_nn(left, right):
    return lax.dot_general(
        left, right, (((1,), (0,)), ((), ())), preferred_element_type=full
    )


def dot_nt(left, right):
    return lax.dot_general(
        left, right, (((1,), (1,)), ((), ())), preferred_element_type=full
    )


def dot_tn(left, right):
    return lax.dot_general(
        left, right, (((0,), (0,)), ((), ())), preferred_element_type=full
    )


def centred_rows(values_in):
    centre = values_in - jnp.mean(values_in, axis=-1, keepdims=True)
    spread = jnp.mean(centre * centre, axis=-1, keepdims=True)
    inverse = lax.rsqrt(spread + norm_eps)
    return centre * inverse, inverse


def norm_back(grad_normed, scaled, inverse, gain):
    inner = grad_normed * gain
    first = jnp.mean(inner, axis=-1, keepdims=True)
    second = jnp.mean(inner * scaled, axis=-1, keepdims=True)
    return inverse * (inner - first - scaled * second)


class Sizes:
    def __init__(self, batch_size, seq_size, rows, block, width, hidden, heads):
        self.batch, self.seq = batch_size, seq_size
        self.rows, self.block, self.width, self.hidden = rows, block, width, hidden
        self.heads = heads
        self.tokens = rows * block
        self.length = seq_size * block
        self.depth = seq_size // 2
        self.per_row = seq_size // rows
        self.chips_per_row = self.per_row // 2
        self.own_width = width // self.per_row
        self.own_heads = heads // self.per_row
        self.pairs = self.own_heads // 2
        self.head_dim = width // heads
        self.span = 2 * block
        self.query_blocks = self.length // self.span
        self.reach = self.query_blocks // 2
        self.tiles = []
        for i in range(self.query_blocks):
            for j in range(max(0, i - self.reach), i + 1):
                self.tiles.append((i, j))
        self.lanes = width // 128
        self.parts = hidden // width


def product_list(parts):
    order = []
    for j in range(parts):
        order += [("inner", j), ("outer", j)]
    order += [("up", 0), ("up", 1), ("up", 2), ("out", 0)]
    order += [("query", 0), ("key", 0), ("value", 0)]
    order += [("pool", 0), ("pool", 1), ("pool", 2)]
    return order


small_places = (
    ("pool_bias", 0), ("gain_one", 4), ("shift_one", 8), ("slopes", 12),
    ("gain_two", 13), ("shift_two", 17), ("inner_bias", 21), ("outer_bias", 37),
    ("up_bias", 41),
)
small_rows = 56


def layer_kernel(size, chunks, lag, docs, slopes, pool_bias, gain_one, shift_one,
                 gain_two, shift_two, inner_bias, outer_bias, up_bias,
                 inputs_hbm, cotangent_hbm, pool_hbm, query_hbm, key_hbm, value_hbm,
                 out_hbm, inner_hbm, outer_hbm, up_hbm,
                 output_hbm, shift_hbm, sums_hbm, small_out,
                 *scratch_refs):
    names = [name for name, _ in scratch_plan(size, chunks)]
    s = dict(zip(names, scratch_refs))
    place = Place(size.batch, size.seq)
    me, core, level = place.seq, place.core, place.level
    rows, block, width, hidden = size.rows, size.block, size.width, size.hidden
    tokens, length, depth = size.tokens, size.length, size.depth
    per_row, chips = size.per_row, size.chips_per_row
    own_width, pairs = size.own_width, size.pairs
    my_row, my_group = me // per_row, me % per_row
    lanes, parts, span = size.lanes, size.parts, size.span
    products = product_list(parts)
    product_rows = width * lanes

    def tile_at(name, part, lane):
        return products.index((name, part)) * product_rows + lane * width

    loads = {}

    def load(name, source, target):
        copy = pltpu.make_async_copy(source, target, s["load_sem"].at[len(loads)])
        copy.start()
        loads[name] = copy

    first_column = pl.multiple_of(my_group * own_width, own_width)

    def x_load(step):
        return pltpu.make_async_copy(
            inputs_hbm.at[(my_row + 1 + step) % rows], s["x"].at[step % 2],
            s["x_sem"].at[step % 2],
        )

    x_load(0).start()
    load("pool", pool_hbm, s["pool_w"])
    load("dy", cotangent_hbm, s["raised"])
    load("up", up_hbm, s["up_w"])
    load("query", query_hbm.at[:, pl.ds(first_column, own_width)], s["query_w"])
    load("key", key_hbm.at[:, pl.ds(first_column, own_width)], s["key_w"])
    load("value", value_hbm.at[:, pl.ds(first_column, own_width)], s["value_w"])
    load("outer", outer_hbm, s["outer_w"])
    load("out", out_hbm, s["out_w"])
    load("inner", inner_hbm, s["inner_w"])

    barrier = pltpu.get_barrier_semaphore()
    greeted = [(place.batch, (me + k) % size.seq) for k in range(1, size.seq)]
    for stage in (1, 2):
        greeted += [place.partner(stage, k) for k in range(1, place.sizes[stage])]
    for device in greeted:
        pl.semaphore_signal(barrier, inc=1, device_id=device, device_id_type=MESH)
    pl.semaphore_wait(barrier, len(greeted))

    def remote(source, target, sent, got, device):
        return pltpu.make_async_remote_copy(
            src_ref=source, dst_ref=target, send_sem=sent, recv_sem=got,
            device_id=device, device_id_type=MESH,
        )

    rim_copy = remote(
        inputs_hbm.at[:, pl.ds(3 * block - 16, 16), :], s["rim"],
        s["rim_sem"].at[0], s["rim_sem"].at[1], (place.batch, (me + 1) % size.seq),
    )

    @pl.when(me < size.seq - 1)
    def _():
        rim_copy.start()

    small_block = s["small_block"]
    small_block[0] = jnp.zeros((small_rows, 128), full)
    small_at = dict(small_places)

    def put_small(name, at, values):
        for c in range(values.shape[1] // 128):
            small_block[0, pl.ds(small_at[name] + at // 128 + c, 1), :] = values[
                :, c * 128 : (c + 1) * 128
            ]

    stage = s["stage"]

    def spread_rows(at, values):
        for c in range(lanes):
            stage[c, pl.ds(at, values.shape[0]), :] = values[:, c * 128 : (c + 1) * 128]

    def every_third(at):
        return jnp.concatenate(
            [stage[c, pl.ds(at, block, stride=3), :] for c in range(lanes)], axis=1
        )

    def put_third(at, values):
        for c in range(lanes):
            stage[c, pl.ds(at, block, stride=3), :] = values[:, c * 128 : (c + 1) * 128]

    def row_span(r):
        return pl.ds(pl.multiple_of(r * block, block), block)

    loads["dy"].wait()
    loads["up"].wait()
    up_sum = jnp.zeros((1, width), full)

    def split_cotangent(r, carry):
        spread_rows(8, s["raised"][r].astype(full))
        totals = []
        grad = jnp.zeros((block, width), full)
        for k in range(3):
            part = every_third(8 + k)
            totals.append(carry[k] + jnp.sum(part, axis=0, keepdims=True))
            low = part.astype(half)
            s["dy"][row_span(r), k * width : (k + 1) * width] = low
            grad = grad + dot_nt(low, s["up_w"][:, k * width : (k + 1) * width])
        s["grad_resid"][row_span(r), :] = grad
        low = grad.astype(half)
        s["grad_branch"][row_span(r), :] = low
        totals.append(carry[3] + jnp.sum(low.astype(full), axis=0, keepdims=True))
        return tuple(totals)

    sums = lax.fori_loop(0, rows, split_cotangent, (up_sum,) * 4)
    load("x", inputs_hbm, s["raised"])
    for k in range(3):
        put_small("up_bias", k * width, sums[k])
    put_small("outer_bias", 0, sums[3])

    @pl.when(me > 0)
    def _():
        rim_copy.wait_recv()

    loads["pool"].wait()
    nr = s["nr"]

    def nr_rows(owner):
        return pl.ds(pl.multiple_of(owner * block, block), block)

    def row_copy(r, target_level):
        return remote(
            s["normed"].at[row_span(r), :], nr.at[nr_rows(me), :],
            s["row_sent"].at[target_level], s["row_got"].at[level],
            (place.batch, target_level * 2 + core),
        )

    def row_from(source_level):
        return remote(
            s["normed"].at[row_span(0), :], nr.at[nr_rows(source_level * 2 + core), :],
            s["row_sent"].at[source_level], s["row_got"].at[source_level],
            (place.batch, source_level * 2 + core),
        )

    for step in range(rows):
        r = (my_row + 1 + step) % rows
        rim_rows = s["rim"][r].astype(full)[8:16, :]
        rim_rows = jnp.where(me > 0, rim_rows, 0.0)
        spread_rows(0, rim_rows)
        x_load(step).wait()
        if step + 1 < rows:
            x_load(step + 1).start()
        spread_rows(8, s["x"][step % 2].astype(full))
        pooled = jnp.zeros((block, width), full) + pool_bias[...]
        for k in range(3):
            part = every_third(6 + k).astype(half)
            s["groups"][row_span(r), k * width : (k + 1) * width] = part
            pooled = pooled + dot_nn(part, s["pool_w"][k * width : (k + 1) * width, :])
        s["pooled"][row_span(r), :] = pooled
        scaled, _ = centred_rows(pooled)
        s["normed"][row_span(r), :] = (scaled * gain_one[...] + shift_one[...]).astype(half)
        if step < rows - 1:
            for i in range(chips):
                row_copy(r, r * chips + i).start()
        else:
            for i in range(1, chips):
                row_copy(r, r * chips + (level % chips + i) % chips).start()
            own_copy = pltpu.make_async_copy(
                s["normed"].at[row_span(r), :], nr.at[nr_rows(me), :], s["own_sem"].at[0]
            )
            own_copy.start()

    loads["outer"].wait()

    def before_activation(j, carry):
        at = pl.ds(pl.multiple_of(j * width, width), width)
        grad = dot_nt(s["grad_branch"][...], s["outer_w"][at, :])
        s["grad_inner"][:, at] = grad.astype(half)
        return carry

    lax.fori_loop(0, parts, before_activation, 0)

    def across(source_level, owner_core):
        owner = source_level * 2 + owner_core
        return remote(
            nr.at[nr_rows(owner), :], nr.at[nr_rows(owner), :],
            s["across_sent"].at[source_level], s["across_got"].at[source_level],
            (place.batch, level * 2 + 1 - core),
        )

    loads["query"].wait()
    loads["key"].wait()
    loads["value"].wait()

    def project(owner):
        at = nr_rows(owner)
        source = nr[at, :]
        q = dot_nn(source, s["query_w"][...])
        k = dot_nn(source, s["key_w"][...])
        v = dot_nn(source, s["value_w"][...])
        qt, kt, vt = q.T, k.T, v.T
        s["vt"][:, at] = vt.astype(half)
        zeros = jnp.zeros((64, block), half)
        line = lax.broadcasted_iota(jnp.int32, (16, block), 0)
        key_at = owner * block + lax.broadcasted_iota(jnp.int32, (16, block), 1)
        fine = (key_at % 128).astype(full)
        coarse = (key_at - key_at % 128).astype(full)
        extra = jnp.where(line == 0, 1.0, jnp.where(line == 1, fine, coarse))
        extra = jnp.where(line < 3, extra, 0.0).astype(half)
        for p in range(pairs):
            s["k"][p, at, :] = k[:, p * 128 : (p + 1) * 128].astype(half)
            s["v"][p, at, :] = v[:, p * 128 : (p + 1) * 128].astype(half)
            for side in range(2):
                h = 2 * p + side
                piece = qt[h * 64 : (h + 1) * 64, :].astype(half)
                s["qt"][h, :, at] = jnp.concatenate(
                    [piece, zeros] if side == 0 else [zeros, piece], axis=0
                )
                piece = kt[h * 64 : (h + 1) * 64, :].astype(half)
                s["kt"][h, :, at] = jnp.concatenate([piece, extra], axis=0)

    order = [0]
    for k in range(1, depth):
        order.append((k + 1) // 2 if k % 2 else depth - k // 2)
    for k in order:
        source_level = (level + k) % depth
        if k == 0:
            own_copy.wait()
        else:
            row_from(source_level).wait_recv()
        across(source_level, core).start()
    for k in order:
        source_level = (level + k) % depth
        project(source_level * 2 + core)
        across(source_level, 1 - core).wait_recv()
        project(source_level * 2 + 1 - core)

    ends = []
    total = 0
    for d in range(docs.shape[1]):
        total = total + docs[my_row, d]
        ends.append(total)
    key_line = lax.broadcasted_iota(jnp.int32, (span, span), 0)
    query_line = lax.broadcasted_iota(jnp.int32, (span, span), 1)
    scale_two = size.head_dim ** -0.5 * log2_e

    def tile_of(i, j):
        return size.tiles.index((i, j))

    def near(i):
        return range(max(0, i - size.reach), i + 1)

    def att_copy(owner, at_row, at_group, slot):
        return remote(
            s["att_out"].at[nr_rows(owner), :],
            s["att"].at[row_span(at_row), pl.ds(pl.multiple_of(at_group * own_width, own_width), own_width)],
            s["att_sent"].at[owner], s["att_got"].at[slot], (place.batch, owner),
        )

    def head_slope(h):
        return slopes[my_group * size.own_heads + h]

    for i in range(size.query_blocks):
        cols = slice(i * span, (i + 1) * span)
        place_q = 3 * (i * span + lax.broadcasted_iota(jnp.int32, (1, span), 1))
        start = jnp.zeros((1, span), jnp.int32)
        for end in ends:
            start = jnp.where(end <= place_q, jnp.maximum(start, end), start)
        for w, j in enumerate(near(i)):
            allowed = 3 * (j * span + key_line) >= start
            if j == i:
                allowed = allowed & (key_line <= query_line)
            s["work"][size.reach + 1 + w] = jnp.where(allowed, 0.0, -1e30)

        def forward_pair(p, carry):
            for side in range(2):
                h = 2 * p + side
                slope_two = head_slope(h) * log2_e
                top = None
                for w, j in enumerate(near(i)):
                    score = dot_nn(s["k"][p, j * span : (j + 1) * span, :], s["qt"][h, :, cols])
                    away = (key_line + (j - i) * span).astype(full)
                    score = score * scale_two + (away * slope_two + s["work"][size.reach + 1 + w])
                    s["work"][w] = score
                    best = jnp.max(score, axis=0, keepdims=True)
                    top = best if top is None else jnp.maximum(top, best)
                total = jnp.zeros((1, span), full)
                mixed = jnp.zeros((64, span), full)
                for w, j in enumerate(near(i)):
                    expo = jnp.exp2(s["work"][w] - top)
                    total = total + jnp.sum(expo, axis=0, keepdims=True)
                    low = expo.astype(half)
                    s["expo"][h, tile_of(i, j)] = low
                    at = pl.multiple_of(h * 64, 64)
                    mixed = mixed + dot_nn(
                        s["vt"][pl.ds(at, 64), j * span : (j + 1) * span], low
                    )
                inverse = 1.0 / total
                s["inverse"][h, :, cols] = jnp.broadcast_to(inverse, (8, span))
                s["mixed"][pl.ds(pl.multiple_of(h * 64, 64), 64), cols] = mixed * inverse
            return carry

        lax.fori_loop(0, pairs, forward_pair, 0)
        s["att_out"][cols, :] = s["mixed"][:, cols].T.astype(half)
        for owner in (2 * i, 2 * i + 1):

            @pl.when(me == owner)
            def _():
                copy = pltpu.make_async_copy(
                    s["att_out"].at[nr_rows(owner), :],
                    s["att"].at[row_span(my_row), pl.ds(first_column, own_width)],
                    s["own_sem"].at[1],
                )
                copy.start()

            @pl.when(me != owner)
            def _():
                att_copy(owner, my_row, my_group, me).start()

    loads["out"].wait()
    loads["inner"].wait()
    pltpu.make_async_copy(
        s["att_out"].at[nr_rows(0), :],
        s["att"].at[row_span(my_row), pl.ds(first_column, own_width)],
        s["own_sem"].at[1],
    ).wait()
    for k in range(1, size.seq):
        source = (me + k) % size.seq
        att_copy(source, source // per_row, source % per_row, source).wait_recv()

    def second_norm(r, carry):
        at = row_span(r)
        residual = s["pooled"][at, :] + dot_nn(s["att"][at, :], s["out_w"][...])
        s["residual"][at, :] = residual
        scaled, _ = centred_rows(residual)
        s["normed_two"][at, :] = (scaled * gain_two[...] + shift_two[...]).astype(half)
        return carry

    lax.fori_loop(0, rows, second_norm, 0)

    for j in range(parts):
        at = slice(j * width, (j + 1) * width)

        def feed(r, carry):
            here = row_span(r)
            value = dot_nn(s["normed_two"][here, :], s["inner_w"][:, at]) + inner_bias[:, at]
            share = 0.5 + 0.5 * lax.erf(value * (0.5 ** 0.5))
            density = jnp.exp(-0.5 * value * value) * (0.5 / math.pi) ** 0.5
            s["activated"][here, at] = (value * share).astype(half)
            grad = s["grad_inner"][here, at].astype(full) * (share + value * density)
            low = grad.astype(half)
            s["grad_inner"][here, at] = low
            return carry + jnp.sum(low.astype(full), axis=0, keepdims=True)

        total = lax.fori_loop(0, rows, feed, jnp.zeros((1, width), full))
        put_small("inner_bias", j * width, total)

    def grad_copy(owner, slot):
        row, group = owner // per_row, owner % per_row
        column = pl.ds(pl.multiple_of(group * own_width, own_width), own_width)
        return remote(
            s["grad_att"].at[row_span(row), column], s["grad_heads"].at[nr_rows(slot), :],
            s["grad_sent"].at[owner], s["grad_got"].at[slot], (place.batch, owner),
        )

    gain_sum = jnp.zeros((1, width), full)
    shift_sum = jnp.zeros((1, width), full)
    for step in range(rows):
        r = (my_row + 1 + step) % rows
        at = row_span(r)
        grad = dot_nt(s["grad_inner"][at, :], s["inner_w"][...])
        scaled, inverse = centred_rows(s["residual"][at, :])
        gain_sum = gain_sum + jnp.sum(grad * scaled, axis=0, keepdims=True)
        shift_sum = shift_sum + jnp.sum(grad, axis=0, keepdims=True)
        mixed = s["grad_resid"][at, :] + norm_back(grad, scaled, inverse, gain_two[...])
        s["grad_resid"][at, :] = mixed
        s["grad_att"][at, :] = dot_nt(mixed.astype(half), s["out_w"][...]).astype(half)
        for g in range(per_row):
            owner = r * per_row + g
            if step < rows - 1:
                grad_copy(owner, me).start()
            else:

                @pl.when(owner != me)
                def _():
                    grad_copy(owner, me).start()

                @pl.when(owner == me)
                def _():
                    pltpu.make_async_copy(
                        s["grad_att"].at[row_span(my_row), pl.ds(first_column, own_width)],
                        s["grad_heads"].at[nr_rows(me), :], s["own_sem"].at[2],
                    ).start()
    put_small("gain_two", 0, gain_sum)
    put_small("shift_two", 0, shift_sum)

    big = SumPieces(place, chunks, s["mine"], s["landing"], s["piece"], sums_hbm,
                    [s["sum_sem"].at[k] for k in range(4)], s["keep_sem"])
    clock = [0]
    begun = {}

    def tick():
        for c in sorted(begun):
            event, off = divmod(clock[0] - begun[c], lag)
            if off == 0 and 0 <= event <= 8:
                big.advance(c, event)
        clock[0] += 1

    def begin(c):
        begun[c] = clock[0]

    def put_product(at, value):
        for c in range(value.shape[1] // 128):
            s["mine"][pl.ds(at + c * width, width), :] = value[
                :, c * 128 : (c + 1) * 128
            ].astype(half)

    for j in range(parts):
        at = slice(j * width, (j + 1) * width)
        put_product(tile_at("inner", j, 0), dot_tn(s["normed_two"][...], s["grad_inner"][:, at]))
        put_product(tile_at("outer", j, 0), dot_tn(s["activated"][:, at], s["grad_branch"][...]))
        begin(j)
        tick()

    def second_residual(r, carry):
        at = row_span(r)
        value = s["residual"][at, :] + dot_nn(s["activated"][at, :], s["outer_w"][...])
        s["normed_two"][at, :] = (value + outer_bias[...]).astype(half)
        return carry

    lax.fori_loop(0, rows, second_residual, 0)
    for k in range(3):
        at = slice(k * width, (k + 1) * width)
        put_product(tile_at("up", k, 0), dot_tn(s["normed_two"][...], s["dy"][:, at]))
        if k == 1:
            begin(parts)
            tick()
    put_product(tile_at("out", 0, 0), dot_tn(s["att"][...], s["grad_resid"][...].astype(half)))
    begin(parts + 1)
    tick()

    def raise_row(r, carry):
        for k in range(3):
            at = slice(k * width, (k + 1) * width)
            raised = dot_nn(s["normed_two"][row_span(r), :], s["up_w"][:, at])
            put_third(8 + k, raised + up_bias[:, at])
        whole = jnp.concatenate([stage[c, 8 : 8 + 3 * block, :] for c in range(lanes)], axis=1)
        s["raised"][r] = (s["raised"][r].astype(full) + whole).astype(half)
        return carry

    loads["x"].wait()
    lax.fori_loop(0, rows, raise_row, 0)
    output_copy = pltpu.make_async_copy(s["raised"], output_hbm, s["own_sem"].at[3])
    output_copy.start()

    blank = jnp.zeros((width, 128), half)
    for name in ("query", "key", "value"):
        for c in range(lanes):
            s["mine"][pl.ds(tile_at(name, 0, c), width), :] = blank

    pltpu.make_async_copy(
        s["grad_att"].at[row_span(my_row), pl.ds(first_column, own_width)],
        s["grad_heads"].at[nr_rows(me), :], s["own_sem"].at[2],
    ).wait()
    for k in range(1, size.seq):
        grad_copy((me + k) % size.seq, (me + k) % size.seq).wait_recv()

    half_blocks = size.query_blocks // 2

    def value_tile(p, j):
        lane = pl.multiple_of((p * half_blocks + j // 2) * 128, 128)
        return s["residual"].at[(j % 2) * span : (j % 2 + 1) * span, pl.ds(lane, 128)]

    def value_block(p, b):
        lane = pl.multiple_of((p * half_blocks + b // 4) * 128, 128)
        return s["residual"].at[row_span(b % 4), pl.ds(lane, 128)]

    def key_tile(p, j):
        at = p * half_blocks + j // 2
        return s["work"].at[at, :, (j % 2) * 128 : (j % 2 + 1) * 128]

    def key_block(p, b):
        lane = pl.multiple_of(b // 2 % 2 * 128, 128)
        return s["work"].at[p * half_blocks + b // 4, row_span(b % 2), pl.ds(lane, 128)]

    turned = s["work"].at[2 * size.reach + 1, 0:own_width, :]

    for i in range(size.query_blocks):
        cols = slice(i * span, (i + 1) * span)
        turned[...] = s["grad_heads"][cols, :].astype(full).T
        query_at = (i * span + lax.broadcasted_iota(jnp.int32, (1, span), 1)).astype(full)

        def backward_pair(p, carry):
            for side in range(2):
                h = 2 * p + side
                head = pl.ds(pl.multiple_of(h * 64, 64), 64)
                inverse = s["inverse"][h, 0:1, cols]
                grad = turned[head, :] * inverse
                term = jnp.sum(grad * s["mixed"][head, cols], axis=0, keepdims=True)
                low = grad.astype(half)
                zeros = jnp.zeros((64, span), half)
                low = jnp.concatenate([low, zeros] if side == 0 else [zeros, low], axis=0)
                query_grad = jnp.zeros((80, span), full)
                for j in near(i):
                    keys = slice(j * span, (j + 1) * span)
                    expo = s["expo"][h, tile_of(i, j)]
                    grad_probs = dot_nn(s["v"][p, keys, :], low)
                    grad_scores = (expo.astype(full) * (grad_probs - term)).astype(half)
                    to_value = dot_nt(expo, low)
                    to_key = dot_nt(grad_scores, s["qt"][h, :, cols])
                    if j == i and side == 0:
                        value_tile(p, j)[...] = to_value
                        key_tile(p, j)[...] = to_key
                    else:
                        value_tile(p, j)[...] += to_value
                        key_tile(p, j)[...] += to_key
                    query_grad = query_grad + dot_nn(s["kt"][h, :, keys], grad_scores)
                s["mixed"][head, cols] = query_grad[:64, :]
                slope = (
                    query_grad[65:66, :] + query_grad[66:67, :] - query_at * query_grad[64:65, :]
                )
                slope = jnp.broadcast_to(slope, (8, span))
                if i == 0:
                    s["slope_sum"][h] = slope
                else:
                    s["slope_sum"][h] += slope
            return carry

        lax.fori_loop(0, pairs, backward_pair, 0)
        tick()

    head_lane = lax.broadcasted_iota(jnp.int32, (1, 128), 1)
    slope_row = jnp.zeros((1, 128), full)
    for h in range(size.own_heads):
        total = jnp.sum(s["slope_sum"][h][0:1, :], axis=1, keepdims=True)
        slope_row = slope_row + jnp.where(head_lane == my_group * size.own_heads + h, total, 0.0)
    small_block[0, pl.ds(small_at["slopes"], 1), :] = slope_row

    scale = size.head_dim ** -0.5

    fit = width // own_width

    def grads_at(which, at=None):
        down = which // fit * length
        if at is None:
            at = pl.ds(down, length)
        else:
            at = pl.ds(pl.multiple_of(at + down, block), block)
        return s["outer_w"].at[at, which % fit * own_width : (which % fit + 1) * own_width]

    def settle(b, carry):
        at = nr_rows(b)
        for which in range(3):
            target = grads_at(which, b * block)
            if which == 0:
                target[...] = (s["mixed"][:, at].T * scale).astype(half)
                continue
            for p in range(pairs):
                lane = slice(p * 128, (p + 1) * 128)
                if which == 1:
                    target[:, lane] = (key_block(p, b)[...] * scale).astype(half)
                else:
                    target[:, lane] = value_block(p, b)[...].astype(half)
        return carry

    lax.fori_loop(0, size.seq, settle, 0)

    def normed_grad(owner):
        return (
            dot_nt(grads_at(0, owner * block)[...], s["query_w"][...])
            + dot_nt(grads_at(1, owner * block)[...], s["key_w"][...])
            + dot_nt(grads_at(2, owner * block)[...], s["value_w"][...])
        )

    def held(first, owner_level):
        across_at = (first + owner_level // rows) * width
        return s["activated"].at[
            row_span(owner_level % rows), pl.ds(pl.multiple_of(across_at, width), width)
        ]

    held_parts = -(-depth // rows)

    def pair_copy(owner_level):
        return remote(
            held(0, owner_level), s["pair_in"].at[row_span(owner_level), :],
            s["pair_sent"].at[owner_level], s["pair_got"].at[owner_level],
            (place.batch, level * 2 + 1 - core),
        )

    def back_copy(owner_level, source_level):
        row, part = source_level // chips, source_level % chips
        return remote(
            held(held_parts, owner_level),
            s["back"].at[part, row_span(row), :],
            s["back_sent"].at[owner_level], s["back_got"].at[source_level],
            (place.batch, owner_level * 2 + core),
        )

    for k in range(depth):
        owner_level = (level + 1 + k) % depth
        held(0, owner_level)[...] = normed_grad(owner_level * 2 + 1 - core).astype(half)
        pair_copy(owner_level).start()
    for k in range(depth):
        owner_level = (level + 1 + k) % depth
        grad = normed_grad(owner_level * 2 + core)
        pair_copy(owner_level).wait_recv()
        grad = grad + s["pair_in"][row_span(owner_level), :].astype(full)
        held(held_parts, owner_level)[...] = grad.astype(half)
        if k < depth - 1:
            back_copy(owner_level, level).start()
        else:
            back_own = pltpu.make_async_copy(
                held(held_parts, level),
                s["back"].at[level % chips, row_span(level // chips), :],
                s["own_sem"].at[4],
            )
            back_own.start()
    tick()

    for which, name in enumerate(("query", "key", "value")):
        value = dot_tn(nr[...], grads_at(which)[...])
        base = products.index((name, 0)) * product_rows
        for c in range(own_width // 128):
            at = pl.multiple_of(base + (my_group * (own_width // 128) + c) * width, width)
            s["mine"][pl.ds(at, width), :] = value[:, c * 128 : (c + 1) * 128].astype(half)
        if name == "key":
            begin(parts + 2)
            tick()

    back_own.wait()
    for k in range(1, depth):
        source_level = (level + k) % depth
        back_copy(source_level, source_level).wait_recv()

    def first_norm(r, carry):
        at = row_span(r)
        grad = s["back"][0, at, :].astype(full)
        for part in range(1, chips):
            grad = grad + s["back"][part, at, :].astype(full)
        scaled, inverse = centred_rows(s["pooled"][at, :])
        low = s["grad_resid"][at, :] + norm_back(grad, scaled, inverse, gain_one[...])
        low = low.astype(half)
        s["normed"][at, :] = low
        for k in range(3):
            put_third(6 + k, dot_nt(low, s["pool_w"][k * width : (k + 1) * width, :]))
        for c in range(lanes):
            lane = slice(c * 128, (c + 1) * 128)
            s["edge_out"][r, :, lane] = stage[c, 0:8, :]
            s["edge_end"][r, :, lane] = stage[c, 3 * block - 8 : 3 * block + 8, :]
            s["raised"][r, :, lane] = stage[c, 8 : 8 + 3 * block, :].astype(half)
        return (
            carry[0] + jnp.sum(grad * scaled, axis=0, keepdims=True),
            carry[1] + jnp.sum(grad, axis=0, keepdims=True),
            carry[2] + jnp.sum(low.astype(full), axis=0, keepdims=True),
        )

    output_copy.wait()
    for k in range(1, depth):
        row_from((level + k) % depth).wait_send()
    nothing = jnp.zeros((1, width), full)
    totals = lax.fori_loop(0, rows, first_norm, (nothing,) * 3)
    put_small("gain_one", 0, totals[0])
    put_small("shift_one", 0, totals[1])
    put_small("pool_bias", 0, totals[2])
    edge_copy = remote(
        s["edge_out"], s["edge_in"], s["rim_sem"].at[2], s["rim_sem"].at[3],
        (place.batch, (me + size.seq - 1) % size.seq),
    )

    @pl.when(me > 0)
    def _():
        edge_copy.start()

    small = SumSmall(place, small_block, s["small_landing"],
                     [s["small_sem"].at[0], s["small_sem"].at[1]])
    small.send(0)
    for k in range(3):
        at = slice(k * width, (k + 1) * width)
        put_product(tile_at("pool", k, 0), dot_tn(s["groups"][:, at], s["normed"][...]))
        if k == 0:
            begin(parts + 3)
            tick()
    begin(parts + 4)
    tick()
    small.receive(0)
    small.send(1)

    @pl.when(me < size.seq - 1)
    def _():
        edge_copy.wait_recv()

    edge_row = lax.broadcasted_iota(jnp.int32, (16, width), 0)
    for r in range(rows):
        edge = jnp.where(me < size.seq - 1, s["edge_in"][r], 0.0)
        edge = jnp.concatenate([edge, edge], axis=0)
        edge = jnp.where(edge_row >= 14, edge, s["edge_end"][r])
        s["raised"][r, 3 * block - 16 : 3 * block, :] = edge.astype(half)
    shift_copy = pltpu.make_async_copy(s["raised"], shift_hbm, s["own_sem"].at[5])
    shift_copy.start()

    stages_done = 1
    last = begun[parts + 4] + 8 * lag
    while clock[0] <= last:
        tick()
        if stages_done < 4 and clock[0] % 2 == 0:
            small.receive(stages_done)
            stages_done += 1
            if stages_done < 4:
                small.send(stages_done)
    while stages_done < 4:
        small.receive(stages_done)
        stages_done += 1
        if stages_done < 4:
            small.send(stages_done)
    small_out[...] = small_block[4]

    shift_copy.wait()

    @pl.when(me < size.seq - 1)
    def _():
        rim_copy.wait_send()

    @pl.when(me > 0)
    def _():
        edge_copy.wait_send()

    for k in range(1, depth):
        other = (level + k) % depth
        back_copy(other, other).wait_send()
    for k in range(depth):
        across(k, core).wait_send()
        pair_copy(k).wait_send()
    for k in range(1, size.seq):
        other = (me + k) % size.seq
        att_copy(other, other // per_row, other % per_row, other).wait_send()
        grad_copy(other, other).wait_send()
    big.finish()
    small.finish()


def scratch_plan(size, chunks):
    tokens, length, width, hidden = size.tokens, size.length, size.width, size.hidden
    rows, block, depth = size.rows, size.block, size.depth
    own, pairs, heads = size.own_width, size.pairs, size.own_heads
    near = size.reach + 1
    members = 2 + 2 * math.isqrt(size.batch) + depth
    slots = sum_slots(size.batch, size.seq)
    dma = pltpu.SemaphoreType.DMA
    total = sum(chunks)
    return [
        ("x", pltpu.VMEM((2, 3 * block, width), half)),
        ("raised", pltpu.VMEM((rows, 3 * block, width), half)),
        ("pool_w", pltpu.VMEM((3 * width, width), half)),
        ("up_w", pltpu.VMEM((width, 3 * width), half)),
        ("query_w", pltpu.VMEM((width, own), half)),
        ("key_w", pltpu.VMEM((width, own), half)),
        ("value_w", pltpu.VMEM((width, own), half)),
        ("outer_w", pltpu.VMEM((hidden, width), half)),
        ("inner_w", pltpu.VMEM((width, hidden), half)),
        ("out_w", pltpu.VMEM((width, width), half)),
        ("rim", pltpu.VMEM((rows, 16, width), half)),
        ("stage", pltpu.VMEM((size.lanes, 3 * block + 8, 128), full)),
        ("groups", pltpu.VMEM((tokens, 3 * width), half)),
        ("dy", pltpu.VMEM((tokens, 3 * width), half)),
        ("grad_resid", pltpu.VMEM((tokens, width), full)),
        ("grad_branch", pltpu.VMEM((tokens, width), half)),
        ("pooled", pltpu.VMEM((tokens, width), full)),
        ("normed", pltpu.VMEM((tokens, width), half)),
        ("nr", pltpu.VMEM((length, width), half)),
        ("grad_inner", pltpu.VMEM((tokens, hidden), half)),
        ("activated", pltpu.VMEM((tokens, hidden), half)),
        ("qt", pltpu.VMEM((heads, 128, length), half)),
        ("kt", pltpu.VMEM((heads, 80, length), half)),
        ("vt", pltpu.VMEM((own, length), half)),
        ("k", pltpu.VMEM((pairs, length, 128), half)),
        ("v", pltpu.VMEM((pairs, length, 128), half)),
        ("work", pltpu.VMEM((2 * near, size.span, size.span), full)),
        ("expo", pltpu.VMEM((heads, len(size.tiles), size.span, size.span), half)),
        ("inverse", pltpu.VMEM((heads, 8, length), full)),
        ("mixed", pltpu.VMEM((own, length), full)),
        ("att_out", pltpu.VMEM((length, own), half)),
        ("att", pltpu.VMEM((tokens, width), half)),
        ("residual", pltpu.VMEM((tokens, width), full)),
        ("normed_two", pltpu.VMEM((tokens, width), half)),
        ("grad_att", pltpu.VMEM((tokens, width), half)),
        ("grad_heads", pltpu.VMEM((length, own), half)),
        ("slope_sum", pltpu.VMEM((heads, 8, size.span), full)),
        ("pair_in", pltpu.VMEM((depth * block, width), half)),
        ("back", pltpu.VMEM((size.chips_per_row, tokens, width), half)),
        ("edge_out", pltpu.VMEM((rows, 8, width), full)),
        ("edge_in", pltpu.VMEM((rows, 8, width), full)),
        ("edge_end", pltpu.VMEM((rows, 16, width), full)),
        ("mine", pltpu.VMEM((total, 128), half)),
        ("landing", pltpu.VMEM((SumPieces.landing_rows(size.batch, size.seq, chunks), 128), half)),
        ("piece", pltpu.VMEM((total // (size.batch * size.seq), 128), half)),
        ("small_block", pltpu.VMEM((5, small_rows, 128), full)),
        ("small_landing", pltpu.VMEM((members, small_rows, 128), full)),
        ("load_sem", dma((10,))),
        ("x_sem", dma((2,))),
        ("rim_sem", dma((4,))),
        ("own_sem", dma((6,))),
        ("row_sent", dma((depth,))),
        ("row_got", dma((depth,))),
        ("across_sent", dma((depth,))),
        ("across_got", dma((depth,))),
        ("att_sent", dma((size.seq,))),
        ("att_got", dma((size.seq,))),
        ("grad_sent", dma((size.seq,))),
        ("grad_got", dma((size.seq,))),
        ("pair_sent", dma((depth,))),
        ("pair_got", dma((depth,))),
        ("back_sent", dma((depth,))),
        ("back_got", dma((depth,))),
        ("sum_sem", dma((4, len(chunks), slots))),
        ("keep_sem", dma((len(chunks),))),
        ("small_sem", dma((2, slots))),
    ]


def widen_kernel(plan, steps, sums, shift, cotangent, *refs):
    outs = dict(zip(plan, refs[: len(plan)]))
    grad_inputs = refs[len(plan)]
    source, target, moved, kept, result, load_sem, store_sem, row_sem = refs[len(plan) + 1 :]
    rows = shift.shape[0]
    deep = source.shape[0]
    product_rows = source.shape[1]
    width = target.shape[1]

    def load(i):
        return pltpu.make_async_copy(
            sums.at[pl.ds(i * product_rows, product_rows), :], source.at[i % deep],
            load_sem.at[i % deep],
        )

    def store(i):
        name, part = steps[i]
        out = outs[name]
        if out.shape[0] > width:
            out = out.at[pl.ds(part * width, width), :]
        elif out.shape[1] > width:
            out = out.at[:, pl.ds(part * width, width)]
        return pltpu.make_async_copy(target.at[i % deep], out, store_sem.at[i % deep])

    def row_loads(r):
        return (
            pltpu.make_async_copy(shift.at[r], moved.at[r % 2], row_sem.at[0, r % 2]),
            pltpu.make_async_copy(cotangent.at[r], kept.at[r % 2], row_sem.at[1, r % 2]),
        )

    def row_store(r):
        return pltpu.make_async_copy(result.at[r % 2], grad_inputs.at[r], row_sem.at[2, r % 2])

    for i in range(deep - 1):
        load(i).start()
    for copy in row_loads(0):
        copy.start()
    for r in range(rows):
        if r + 1 < rows:
            for copy in row_loads(r + 1):
                copy.start()
        for copy in row_loads(r):
            copy.wait()
        if r >= 2:
            row_store(r - 2).wait()

        def add_rows(b, carry):
            at = pl.ds(pl.multiple_of(b * 64, 64), 64)
            result[r % 2, at, :] = moved[r % 2, at, :].astype(full) + kept[
                r % 2, at, :
            ].astype(full)
            return carry

        lax.fori_loop(0, result.shape[1] // 64, add_rows, 0)
        row_store(r).start()
    for i in range(len(steps)):
        if i + deep - 1 < len(steps):
            load(i + deep - 1).start()
        load(i).wait()
        if i >= deep:
            store(i - deep).wait()

        def convert(b, carry):
            at = pl.multiple_of(b * 64, 64)
            for c in range(product_rows // width):
                target[i % deep, pl.ds(at, 64), c * 128 : (c + 1) * 128] = source[
                    i % deep, pl.ds(c * width + at, 64), :
                ].astype(full)
            return carry

        lax.fori_loop(0, width // 64, convert, 0)
        store(i).start()
    for r in range(max(0, rows - 2), rows):
        row_store(r).wait()
    for i in range(max(0, len(steps) - deep), len(steps)):
        store(i).wait()


def widen(sums, shift, cotangent, shapes, steps):
    any_space = pl.BlockSpec(memory_space=pl.ANY)
    names = tuple(shapes)
    width = shift.shape[2]
    deep = 3
    outs = [jax.ShapeDtypeStruct(shapes[name], full) for name in names]
    outs.append(jax.ShapeDtypeStruct(shift.shape, full))
    row = shift.shape[1:]
    product_rows = sums.shape[0] // len(steps)
    results = pl.pallas_call(
        functools.partial(widen_kernel, names, steps),
        out_shape=outs,
        in_specs=[any_space] * 3,
        out_specs=[any_space] * len(outs),
        scratch_shapes=[
            pltpu.VMEM((deep, product_rows, 128), half),
            pltpu.VMEM((deep, width, width), full),
            pltpu.VMEM((2,) + row, half),
            pltpu.VMEM((2,) + row, half),
            pltpu.VMEM((2,) + row, full),
            pltpu.SemaphoreType.DMA((deep,)),
            pltpu.SemaphoreType.DMA((deep,)),
            pltpu.SemaphoreType.DMA((3, 2)),
        ],
        name="widen",
    )(sums, shift, cotangent)
    return dict(zip(names, results[:-1])), results[-1]


def local(
    inputs,
    cotangent,
    doc_lengths,
    pool_weight,
    pool_bias,
    gain_one,
    shift_one,
    query_weight,
    key_weight,
    value_weight,
    out_weight,
    slopes,
    gain_two,
    shift_two,
    inner_weight,
    inner_bias,
    outer_weight,
    outer_bias,
    up_weight,
    up_bias,
):
    rows, block_len, width = inputs.shape
    hidden = inner_weight.shape[1]
    size = Sizes(
        lax.axis_size("batch"), lax.axis_size("seq"), rows, block_len // 3, width,
        hidden, slopes.shape[0],
    )
    steps = product_list(size.parts)
    product_rows = width * size.lanes
    chunks = [2 * product_rows] * (len(steps) // 2)
    total = len(steps) * product_rows
    vmem = pl.BlockSpec(memory_space=pltpu.VMEM)
    smem = pl.BlockSpec(memory_space=pltpu.SMEM)
    any_space = pl.BlockSpec(memory_space=pl.ANY)
    plan = scratch_plan(size, chunks)
    vectors = (
        pool_bias, gain_one, shift_one, gain_two, shift_two, inner_bias, outer_bias, up_bias,
    )
    output, shift, sums, small = pl.pallas_call(
        functools.partial(layer_kernel, size, chunks, 2),
        out_shape=(
            jax.ShapeDtypeStruct(inputs.shape, half),
            jax.ShapeDtypeStruct(inputs.shape, half),
            jax.ShapeDtypeStruct((total, 128), half),
            jax.ShapeDtypeStruct((small_rows, 128), full),
        ),
        in_specs=[smem, smem] + [vmem] * 8 + [any_space] * 10,
        out_specs=(any_space, any_space, any_space, vmem),
        scratch_shapes=[kind for _, kind in plan],
        compiler_params=pltpu.CompilerParams(
            collective_id=0, has_side_effects=True, vmem_limit_bytes=67043328
        ),
        name="layer",
    )(
        doc_lengths, slopes, *(v.reshape(1, -1) for v in vectors),
        inputs, cotangent, pool_weight, query_weight, key_weight, value_weight,
        out_weight, inner_weight, outer_weight, up_weight,
    )
    shapes = {
        "inner": inner_weight.shape, "outer": outer_weight.shape, "up": up_weight.shape,
        "out": out_weight.shape, "query": query_weight.shape, "key": key_weight.shape,
        "value": value_weight.shape, "pool": pool_weight.shape,
    }
    grads, input_grad = widen(sums, shift, cotangent, shapes, steps)
    places = dict(small_places)

    def vector(name, count):
        at = places[name]
        if count < 128:
            return small[at, :count]
        return small[at : at + count // 128].reshape(count)

    return (
        output,
        input_grad,
        grads["pool"],
        vector("pool_bias", width),
        vector("gain_one", width),
        vector("shift_one", width),
        grads["query"],
        grads["key"],
        grads["value"],
        grads["out"],
        vector("slopes", slopes.shape[0]),
        vector("gain_two", width),
        vector("shift_two", width),
        grads["inner"],
        vector("inner_bias", hidden),
        grads["outer"],
        vector("outer_bias", width),
        grads["up"],
        vector("up_bias", 3 * width),
    )


def solution(mesh):
    blocks = P("batch", "seq", None)
    in_specs = (blocks, blocks, P("batch", None)) + (P(),) * 17
    out_specs = (blocks, blocks) + (P(),) * 17
    return jax.shard_map(local, mesh=mesh, in_specs=in_specs, out_specs=out_specs, check_vma=False)
```

```python
import functools
import math
from types import SimpleNamespace

import jax
import jax.numpy as jnp
from jax import lax
from jax.experimental import pallas as pl
from jax.experimental.pallas import tpu as pltpu
from jax.sharding import PartitionSpec as P

norm_eps = 1e-05
log2_e = math.log2(math.e)

MESH = pl.DeviceIdType.MESH
half = jnp.bfloat16
full = jnp.float32


class Place:
    def __init__(self, batch_size, seq_size):
        side = math.isqrt(batch_size)
        self.depth = seq_size // 2
        self.batch = lax.axis_index("batch")
        self.seq = lax.axis_index("seq")
        self.core = self.seq % 2
        self.level = self.seq // 2
        high, low = self.batch // side, self.batch % side
        self.first = jnp.where(self.core == 0, low, high)
        self.second = jnp.where(self.core == 0, high, low)
        self.side = side
        self.sizes = stage_sizes(batch_size, seq_size)
        bits = [self.level // 2**b % 2 for b in range(len(self.sizes) - 3)]
        self.where = (self.core, self.first, self.second, *bits)

    def batch_at(self, first, second):
        return jnp.where(
            self.core == 0, second * self.side + first, first * self.side + second
        )

    def partner(self, stage, step):
        member = (self.where[stage] + step) % self.sizes[stage]
        if stage == 0:
            return (self.batch, self.level * 2 + member)
        if stage == 1:
            return (self.batch_at(member, self.second), self.seq)
        if stage == 2:
            return (self.batch_at(self.first, member), self.seq)
        other = self.level + (member - self.where[stage]) * 2 ** (stage - 3)
        return (self.batch, other * 2 + self.core)


def stage_sizes(batch_size, seq_size):
    side = math.isqrt(batch_size)
    bits = (seq_size // 2).bit_length() - 1
    return (2, side, side) + (2,) * bits


def sum_slots(batch_size, seq_size):
    return sum(size - 1 for size in stage_sizes(batch_size, seq_size))


class SumPieces:
    def __init__(self, place, chunks, orders, mine, landing, piece, out, sems, keep):
        self.place, self.chunks, self.orders = place, chunks, orders
        self.mine, self.landing, self.piece, self.out = mine, landing, piece, out
        self.keep = keep
        self.sent, self.got, self.back_sent, self.back_got = sems
        self.starts = [sum(chunks[:c]) for c in range(len(chunks))]
        sizes = place.sizes
        self.last = len(sizes) - 1
        self.events = 2 * len(sizes) + 1
        self.land = {}
        at = 0
        for c in range(len(chunks)):
            for stage in range(len(sizes)):
                for step in self.steps(c, stage):
                    self.land[c, stage, step] = at
                    at += self.rows(c, stage)

    @staticmethod
    def landing_rows(batch_size, seq_size, chunks, orders):
        sizes, rows = stage_sizes(batch_size, seq_size), 0
        for left, order in zip(chunks, orders):
            for axis in order:
                left //= sizes[axis]
                rows += left * (sizes[axis] - 1)
        return rows

    def size_at(self, c, stage):
        return self.place.sizes[self.orders[c][stage]]

    def where_at(self, c, stage):
        return self.place.where[self.orders[c][stage]]

    def slot(self, c, stage):
        return sum(self.size_at(c, t) - 1 for t in range(stage))

    def rows(self, c, stage):
        count = self.chunks[c]
        for t in range(stage + 1):
            count //= self.size_at(c, t)
        return count

    def begin(self, c, stage):
        at = self.starts[c]
        for t in range(stage):
            at = at + self.where_at(c, t) * self.rows(c, t)
        return at

    def scatter(self, c, stage, step):
        count = self.rows(c, stage)
        member = (self.where_at(c, stage) + step) % self.size_at(c, stage)
        at = pl.multiple_of(self.begin(c, stage) + member * count, 16)
        slot = self.slot(c, stage) + step - 1
        return pltpu.make_async_remote_copy(
            src_ref=self.mine.at[pl.ds(at, count), :],
            dst_ref=self.landing.at[pl.ds(self.land[c, stage, step], count), :],
            send_sem=self.sent.at[c, slot],
            recv_sem=self.got.at[c, slot],
            device_id=self.place.partner(self.orders[c][stage], step),
            device_id_type=MESH,
        )

    def piece_span(self, c):
        count = self.rows(c, self.last)
        return pl.ds(self.starts[c] * count // self.chunks[c], count)

    def keep_copy(self, c):
        at = pl.multiple_of(self.begin(c, self.last + 1), 16)
        return pltpu.make_async_copy(
            self.piece.at[self.piece_span(c), :],
            self.out.at[pl.ds(at, self.rows(c, self.last)), :],
            self.keep.at[c],
        )

    def gather(self, c, stage, step):
        count = self.rows(c, stage)
        at = pl.multiple_of(self.begin(c, stage + 1), 16)
        slot = self.slot(c, stage) + step - 1
        source = self.out.at[pl.ds(at, count), :]
        if stage == self.last:
            source = self.piece.at[self.piece_span(c), :]
        return pltpu.make_async_remote_copy(
            src_ref=source,
            dst_ref=self.out.at[pl.ds(at, count), :],
            send_sem=self.back_sent.at[c, slot],
            recv_sem=self.back_got.at[c, slot],
            device_id=self.place.partner(self.orders[c][stage], step),
            device_id_type=MESH,
        )

    def add(self, c, stage):
        count = self.rows(c, stage)
        at = self.begin(c, stage + 1)
        part = min(count, 512)

        def body(i, carry):
            here = pl.ds(pl.multiple_of(at + i * part, 16), part)
            if self.size_at(c, stage) == 2:
                there = pl.multiple_of(self.land[c, stage, 1] + i * part, 16)
                total = self.mine[here, :] + self.landing[pl.ds(there, part), :]
            else:
                total = self.mine[here, :].astype(full)
                for step in self.steps(c, stage):
                    there = pl.multiple_of(self.land[c, stage, step] + i * part, 16)
                    total = total + self.landing[pl.ds(there, part), :].astype(full)
                total = total.astype(half)
            if stage == self.last:
                first = self.piece_span(c).start
                self.piece[pl.ds(pl.multiple_of(first + i * part, 16), part), :] = total
            else:
                self.mine[here, :] = total
            return carry

        lax.fori_loop(0, count // part, body, 0)

    def steps(self, c, stage):
        return range(1, self.size_at(c, stage))

    def advance(self, c, event):
        count = self.last + 1
        if 1 <= event <= count:
            for step in self.steps(c, event - 1):
                self.scatter(c, event - 1, step).wait_recv()
            self.add(c, event - 1)
        if event < count:
            for step in self.steps(c, event):
                self.scatter(c, event, step).start()
            return
        stage = 2 * count - 1 - event
        if event == count:
            self.keep_copy(c).start()
        else:
            for step in self.steps(c, stage + 1):
                self.gather(c, stage + 1, step).wait_recv()
        if event == count + 1:
            self.keep_copy(c).wait()
        if stage >= 0:
            for step in self.steps(c, stage):
                self.gather(c, stage, step).start()

    def finish(self):
        for c in range(len(self.chunks)):
            for stage in range(self.last + 1):
                for step in self.steps(c, stage):
                    self.scatter(c, stage, step).wait_send()
                    self.gather(c, stage, step).wait_send()


class SumSmall:
    def __init__(self, place, block, landing, sems):
        self.place, self.block, self.landing = place, block, landing
        self.sent, self.got = sems
        sizes = place.sizes
        self.slot = [sum(s - 1 for s in sizes[:stage]) for stage in range(len(sizes))]
        self.base = [sum(sizes[:stage]) for stage in range(len(sizes))]

    def copy(self, stage, step):
        slot = self.slot[stage] + step - 1
        return pltpu.make_async_remote_copy(
            src_ref=self.block.at[stage],
            dst_ref=self.landing.at[self.base[stage] + self.place.where[stage]],
            send_sem=self.sent.at[slot],
            recv_sem=self.got.at[slot],
            device_id=self.place.partner(stage, step),
            device_id_type=MESH,
        )

    def send(self, stage):
        self.landing[self.base[stage] + self.place.where[stage]] = self.block[stage]
        for step in range(1, self.place.sizes[stage]):
            self.copy(stage, step).start()

    def receive(self, stage):
        for step in range(1, self.place.sizes[stage]):
            self.copy(stage, step).wait_recv()
        total = self.landing[self.base[stage]]
        for member in range(1, self.place.sizes[stage]):
            total = total + self.landing[self.base[stage] + member]
        self.block[stage + 1] = total

    def finish(self):
        for stage in range(len(self.place.sizes)):
            for step in range(1, self.place.sizes[stage]):
                self.copy(stage, step).wait_send()


def dot_nn(left, right):
    return lax.dot_general(
        left, right, (((1,), (0,)), ((), ())), preferred_element_type=full
    )


def dot_nt(left, right):
    return lax.dot_general(
        left, right, (((1,), (1,)), ((), ())), preferred_element_type=full
    )


def dot_tn(left, right):
    return lax.dot_general(
        left, right, (((0,), (0,)), ((), ())), preferred_element_type=full
    )


def centred_rows(values_in):
    centre = values_in - jnp.mean(values_in, axis=-1, keepdims=True)
    spread = jnp.mean(centre * centre, axis=-1, keepdims=True)
    inverse = lax.rsqrt(spread + norm_eps)
    return centre * inverse, inverse


def norm_back(grad_normed, scaled, inverse, gain):
    inner = grad_normed * gain
    first = jnp.mean(inner, axis=-1, keepdims=True)
    second = jnp.mean(inner * scaled, axis=-1, keepdims=True)
    return inverse * (inner - first - scaled * second)


class Sizes:
    def __init__(self, batch_size, seq_size, rows, block, width, hidden, heads):
        self.batch, self.seq = batch_size, seq_size
        self.rows, self.block, self.width, self.hidden = rows, block, width, hidden
        self.heads = heads
        self.tokens = rows * block
        self.length = seq_size * block
        self.depth = seq_size // 2
        self.per_row = seq_size // rows
        self.chips_per_row = self.per_row // 2
        self.own_width = width // self.per_row
        self.own_heads = heads // self.per_row
        self.pairs = self.own_heads // 2
        self.head_dim = width // heads
        self.span = 2 * block
        self.query_blocks = self.length // self.span
        self.reach = self.query_blocks // 2
        self.tiles = []
        for i in range(self.query_blocks):
            for j in range(max(0, i - self.reach), i + 1):
                self.tiles.append((i, j))
        self.lanes = width // 128
        self.parts = hidden // width


def product_list(parts):
    order = []
    for j in range(parts):
        order += [(Product.inner, j), (Product.outer, j)]
    order += [(Product.up, 0), (Product.up, 1), (Product.up, 2), (Product.out, 0)]
    order += [(Product.query, 0), (Product.key, 0), (Product.value, 0)]
    order += [(Product.pool, 0), (Product.pool, 1), (Product.pool, 2)]
    return order


class Product:
    inner, outer, up, out, query, key, value, pool = range(8)


class Small:
    pool_bias, gain_one, shift_one, slopes = 0, 4, 8, 12
    gain_two, shift_two, inner_bias, outer_bias, up_bias = 13, 17, 21, 37, 41


class Site:
    feed, norm_two, second, up, out, rise, heads, back, settle = range(9)
    pair, give, weights, rows, norm_one, pool = range(9, 15)


small_rows = 56


pace = {
    (Site.feed, 0): (0,),
    (Site.feed, 1): (1,),
    (Site.feed, 2): (0, 2,),
    (Site.feed, 3): (1, 3,),
    (Site.norm_two, 0): (2,),
    (Site.norm_two, 1): (0,),
    (Site.norm_two, 2): (3,),
    (Site.second, 0): (1,),
    (Site.up, 1): (4,),
    (Site.up, 2): (2,),
    (Site.out, 0): (5,),
    (Site.rise, 0): (0,),
    (Site.rise, 3): (4,),
    (Site.heads, 0): (3, 5, 1, 2, 0,),
    (Site.back, 3): (1,),
    (Site.back, 4): (4, 2, 3, 0,),
    (Site.back, 6): (1, 5,),
    (Site.back, 7): (2, 4, 3,),
    (Site.settle, 0): (0,),
    (Site.pair, 0): (1, 5,),
    (Site.pair, 3): (2,),
    (Site.give, 0): (4,),
    (Site.give, 2): (3, 0,),
    (Site.weights, 0): (1,),
    (Site.weights, 1): (6,),
    (Site.weights, 2): (5,),
    (Site.rows, 0): (2, 0, 1, 6, 2, 0,),
    (Site.norm_one, 1): (0,),
    (Site.norm_one, 2): (1,),
    (Site.pool, 0): (7,),
    (Site.pool, 1): (6, 8,),
    (Site.pool, 2): (4, 1, 3, 9,),
}
finish_order = (
    5, 7, 2, 8, 6, 9, 4, 2, 3, 5, 7, 6, 8, 4, 9, 5,
    3, 6, 7, 8, 6, 4, 7, 9, 8, 5, 6, 9, 7, 3, 8, 9,
    3, 7, 8, 4, 9, 4, 7, 8, 5, 9, 6, 5, 7, 8, 9, 6,
    6, 7, 8, 7, 8, 9, 9,
)
level_first = ()


def axis_orders(size, count):
    axes = tuple(range(len(stage_sizes(size.batch, size.seq))))
    return [
        axes[:2] + axes[3:] + axes[2:3] if c in level_first else axes for c in range(count)
    ]


def layer_kernel(size, chunks, docs, slopes, pool_bias, gain_one, shift_one,
                 gain_two, shift_two, inner_bias, outer_bias, up_bias,
                 inputs_hbm, cotangent_hbm, pool_hbm, query_hbm, key_hbm, value_hbm,
                 out_hbm, inner_hbm, outer_hbm, up_hbm,
                 output_hbm, shift_hbm, sums_hbm, small_out,
                 *scratch_refs):
    s = SimpleNamespace(**dict(zip(scratch_plan(size, chunks), scratch_refs)))
    place = Place(size.batch, size.seq)
    me, core, level = place.seq, place.core, place.level
    rows, block, width, hidden = size.rows, size.block, size.width, size.hidden
    tokens, length, depth = size.tokens, size.length, size.depth
    per_row, chips = size.per_row, size.chips_per_row
    own_width, pairs = size.own_width, size.pairs
    my_row, my_group = me // per_row, me % per_row
    lanes, parts, span = size.lanes, size.parts, size.span
    products = product_list(parts)
    product_rows = width * lanes

    def tile_at(name, part, lane):
        return products.index((name, part)) * product_rows + lane * width

    loads = SimpleNamespace()

    def load(source, target):
        copy = pltpu.make_async_copy(source, target, s.load_sem.at[len(vars(loads))])
        copy.start()
        return copy

    first_column = pl.multiple_of(my_group * own_width, own_width)

    def x_load(step):
        return pltpu.make_async_copy(
            inputs_hbm.at[(my_row + 1 + step) % rows], s.x.at[step % 2],
            s.x_sem.at[step % 2],
        )

    x_load(0).start()
    loads.pool = load(pool_hbm, s.pool_w)
    loads.dy = load(cotangent_hbm, s.raised)
    loads.up = load(up_hbm, s.up_w)
    loads.query = load(query_hbm.at[:, pl.ds(first_column, own_width)], s.query_w)
    loads.key = load(key_hbm.at[:, pl.ds(first_column, own_width)], s.key_w)
    loads.value = load(value_hbm.at[:, pl.ds(first_column, own_width)], s.value_w)
    loads.outer = load(outer_hbm, s.outer_w)
    loads.out = load(out_hbm, s.out_w)
    loads.inner = load(inner_hbm, s.inner_w)

    barrier = pltpu.get_barrier_semaphore()
    greeted = [(place.batch, (me + k) % size.seq) for k in range(1, size.seq)]
    for stage in (1, 2):
        greeted += [place.partner(stage, k) for k in range(1, place.sizes[stage])]
    for device in greeted:
        pl.semaphore_signal(barrier, inc=1, device_id=device, device_id_type=MESH)
    pl.semaphore_wait(barrier, len(greeted))

    def remote(source, target, sent, got, device):
        return pltpu.make_async_remote_copy(
            src_ref=source, dst_ref=target, send_sem=sent, recv_sem=got,
            device_id=device, device_id_type=MESH,
        )

    rim_copy = remote(
        inputs_hbm.at[:, pl.ds(3 * block - 16, 16), :], s.rim,
        s.rim_sem.at[0], s.rim_sem.at[1], (place.batch, (me + 1) % size.seq),
    )

    @pl.when(me < size.seq - 1)
    def _():
        rim_copy.start()

    small_block = s.small_block
    small_block[0] = jnp.zeros((small_rows, 128), full)

    def put_small(name, at, values):
        for c in range(values.shape[1] // 128):
            small_block[0, pl.ds(name + at // 128 + c, 1), :] = values[
                :, c * 128 : (c + 1) * 128
            ]

    stage = s.stage

    def spread_rows(at, values):
        for c in range(lanes):
            stage[c, pl.ds(at, values.shape[0]), :] = values[:, c * 128 : (c + 1) * 128]

    def every_third(at):
        return jnp.concatenate(
            [stage[c, pl.ds(at, block, stride=3), :] for c in range(lanes)], axis=1
        )

    def put_third(at, values):
        for c in range(lanes):
            stage[c, pl.ds(at, block, stride=3), :] = values[:, c * 128 : (c + 1) * 128]

    def row_span(r):
        return pl.ds(pl.multiple_of(r * block, block), block)

    loads.dy.wait()
    loads.up.wait()
    up_sum = jnp.zeros((1, width), full)

    def split_cotangent(r, carry):
        spread_rows(8, s.raised[r].astype(full))
        totals = []
        grad = jnp.zeros((block, width), full)
        for k in range(3):
            part = every_third(8 + k)
            totals.append(carry[k] + jnp.sum(part, axis=0, keepdims=True))
            low = part.astype(half)
            s.dy[row_span(r), k * width : (k + 1) * width] = low
            grad = grad + dot_nt(low, s.up_w[:, k * width : (k + 1) * width])
        s.grad_resid[row_span(r), :] = grad
        low = grad.astype(half)
        s.grad_branch[row_span(r), :] = low
        totals.append(carry[3] + jnp.sum(low.astype(full), axis=0, keepdims=True))
        return tuple(totals)

    sums = lax.fori_loop(0, rows, split_cotangent, (up_sum,) * 4)
    loads.x = load(inputs_hbm, s.raised)
    for k in range(3):
        put_small(Small.up_bias, k * width, sums[k])
    put_small(Small.outer_bias, 0, sums[3])

    @pl.when(me > 0)
    def _():
        rim_copy.wait_recv()

    loads.pool.wait()
    nr = s.nr

    def nr_rows(owner):
        return pl.ds(pl.multiple_of(owner * block, block), block)

    def row_copy(r, target_level):
        return remote(
            s.normed.at[row_span(r), :], nr.at[nr_rows(me), :],
            s.row_sent.at[target_level], s.row_got.at[level],
            (place.batch, target_level * 2 + core),
        )

    def row_from(source_level):
        return remote(
            s.normed.at[row_span(0), :], nr.at[nr_rows(source_level * 2 + core), :],
            s.row_sent.at[source_level], s.row_got.at[source_level],
            (place.batch, source_level * 2 + core),
        )

    for step in range(rows):
        r = (my_row + 1 + step) % rows
        rim_rows = s.rim[r].astype(full)[8:16, :]
        rim_rows = jnp.where(me > 0, rim_rows, 0.0)
        spread_rows(0, rim_rows)
        x_load(step).wait()
        if step + 1 < rows:
            x_load(step + 1).start()
        spread_rows(8, s.x[step % 2].astype(full))
        pooled = jnp.zeros((block, width), full) + pool_bias[...]
        for k in range(3):
            part = every_third(6 + k).astype(half)
            s.groups[row_span(r), k * width : (k + 1) * width] = part
            pooled = pooled + dot_nn(part, s.pool_w[k * width : (k + 1) * width, :])
        s.pooled[row_span(r), :] = pooled
        scaled, _ = centred_rows(pooled)
        s.normed[row_span(r), :] = (scaled * gain_one[...] + shift_one[...]).astype(half)
        if step < rows - 1:
            for i in range(chips):
                row_copy(r, r * chips + i).start()
        else:
            for i in range(1, chips):
                row_copy(r, r * chips + (level % chips + i) % chips).start()
            own_copy = pltpu.make_async_copy(
                s.normed.at[row_span(r), :], nr.at[nr_rows(me), :], s.own_sem.at[0]
            )
            own_copy.start()

    loads.outer.wait()

    def before_activation(j, carry):
        at = pl.ds(pl.multiple_of(j * width, width), width)
        grad = dot_nt(s.grad_branch[...], s.outer_w[at, :])
        s.grad_inner[:, at] = grad.astype(half)
        return carry

    lax.fori_loop(0, parts, before_activation, 0)

    def across(source_level, owner_core):
        owner = source_level * 2 + owner_core
        return remote(
            nr.at[nr_rows(owner), :], nr.at[nr_rows(owner), :],
            s.across_sent.at[source_level], s.across_got.at[source_level],
            (place.batch, level * 2 + 1 - core),
        )

    loads.query.wait()
    loads.key.wait()
    loads.value.wait()

    def project(owner):
        at = nr_rows(owner)
        source = nr[at, :]
        q = dot_nn(source, s.query_w[...])
        k = dot_nn(source, s.key_w[...])
        v = dot_nn(source, s.value_w[...])
        qt, kt, vt = q.T, k.T, v.T
        s.vt[:, at] = vt.astype(half)
        zeros = jnp.zeros((64, block), half)
        line = lax.broadcasted_iota(jnp.int32, (16, block), 0)
        key_at = owner * block + lax.broadcasted_iota(jnp.int32, (16, block), 1)
        fine = (key_at % 128).astype(full)
        coarse = (key_at - key_at % 128).astype(full)
        extra = jnp.where(line == 0, 1.0, jnp.where(line == 1, fine, coarse))
        extra = jnp.where(line < 3, extra, 0.0).astype(half)
        for p in range(pairs):
            s.k[p, at, :] = k[:, p * 128 : (p + 1) * 128].astype(half)
            s.v[p, at, :] = v[:, p * 128 : (p + 1) * 128].astype(half)
            for side in range(2):
                h = 2 * p + side
                piece = qt[h * 64 : (h + 1) * 64, :].astype(half)
                s.qt[h, :, at] = jnp.concatenate(
                    [piece, zeros] if side == 0 else [zeros, piece], axis=0
                )
                piece = kt[h * 64 : (h + 1) * 64, :].astype(half)
                s.kt[h, :, at] = jnp.concatenate([piece, extra], axis=0)

    order = [0]
    for k in range(1, depth):
        order.append((k + 1) // 2 if k % 2 else depth - k // 2)
    for k in order:
        source_level = (level + k) % depth
        if k == 0:
            own_copy.wait()
        else:
            row_from(source_level).wait_recv()
        across(source_level, core).start()
    for k in order:
        source_level = (level + k) % depth
        project(source_level * 2 + core)
        across(source_level, 1 - core).wait_recv()
        project(source_level * 2 + 1 - core)

    ends = []
    total = 0
    for d in range(docs.shape[1]):
        total = total + docs[my_row, d]
        ends.append(total)
    key_line = lax.broadcasted_iota(jnp.int32, (span, span), 0)
    query_line = lax.broadcasted_iota(jnp.int32, (span, span), 1)
    scale_two = size.head_dim ** -0.5 * log2_e

    def tile_of(i, j):
        return size.tiles.index((i, j))

    def near(i):
        return range(max(0, i - size.reach), i + 1)

    def att_copy(owner, at_row, at_group, slot):
        return remote(
            s.att_out.at[nr_rows(owner), :],
            s.att.at[row_span(at_row), pl.ds(pl.multiple_of(at_group * own_width, own_width), own_width)],
            s.att_sent.at[owner], s.att_got.at[slot], (place.batch, owner),
        )

    def head_slope(h):
        return slopes[my_group * size.own_heads + h]

    for i in range(size.query_blocks):
        cols = slice(i * span, (i + 1) * span)
        place_q = 3 * (i * span + lax.broadcasted_iota(jnp.int32, (1, span), 1))
        start = jnp.zeros((1, span), jnp.int32)
        for end in ends:
            start = jnp.where(end <= place_q, jnp.maximum(start, end), start)
        for w, j in enumerate(near(i)):
            allowed = 3 * (j * span + key_line) >= start
            if j == i:
                allowed = allowed & (key_line <= query_line)
            s.work[size.reach + 1 + w] = jnp.where(allowed, 0.0, -1e30)

        def forward_pair(p, carry):
            for side in range(2):
                h = 2 * p + side
                slope_two = head_slope(h) * log2_e
                top = None
                for w, j in enumerate(near(i)):
                    score = dot_nn(s.k[p, j * span : (j + 1) * span, :], s.qt[h, :, cols])
                    away = (key_line + (j - i) * span).astype(full)
                    score = score * scale_two + (away * slope_two + s.work[size.reach + 1 + w])
                    s.work[w] = score
                    best = jnp.max(score, axis=0, keepdims=True)
                    top = best if top is None else jnp.maximum(top, best)
                total = jnp.zeros((1, span), full)
                mixed = jnp.zeros((64, span), full)
                for w, j in enumerate(near(i)):
                    expo = jnp.exp2(s.work[w] - top)
                    total = total + jnp.sum(expo, axis=0, keepdims=True)
                    low = expo.astype(half)
                    s.expo[h, tile_of(i, j)] = low
                    at = pl.multiple_of(h * 64, 64)
                    mixed = mixed + dot_nn(
                        s.vt[pl.ds(at, 64), j * span : (j + 1) * span], low
                    )
                inverse = 1.0 / total
                s.inverse[h, :, cols] = jnp.broadcast_to(inverse, (8, span))
                s.mixed[pl.ds(pl.multiple_of(h * 64, 64), 64), cols] = mixed * inverse
            return carry

        lax.fori_loop(0, pairs, forward_pair, 0)
        s.att_out[cols, :] = s.mixed[:, cols].T.astype(half)
        for owner in (2 * i, 2 * i + 1):

            @pl.when(me == owner)
            def _():
                copy = pltpu.make_async_copy(
                    s.att_out.at[nr_rows(owner), :],
                    s.att.at[row_span(my_row), pl.ds(first_column, own_width)],
                    s.own_sem.at[1],
                )
                copy.start()

            @pl.when(me != owner)
            def _():
                att_copy(owner, my_row, my_group, me).start()

    loads.out.wait()
    loads.inner.wait()
    pltpu.make_async_copy(
        s.att_out.at[nr_rows(0), :],
        s.att.at[row_span(my_row), pl.ds(first_column, own_width)],
        s.own_sem.at[1],
    ).wait()
    for k in range(1, size.seq):
        source = (me + k) % size.seq
        att_copy(source, source // per_row, source % per_row, source).wait_recv()

    def second_norm(r, carry):
        at = row_span(r)
        residual = s.pooled[at, :] + dot_nn(s.att[at, :], s.out_w[...])
        s.residual[at, :] = residual
        scaled, _ = centred_rows(residual)
        s.normed_two[at, :] = (scaled * gain_two[...] + shift_two[...]).astype(half)
        return carry

    lax.fori_loop(0, rows, second_norm, 0)

    big = SumPieces(place, chunks, axis_orders(size, len(chunks)), s.mine, s.landing, s.piece, sums_hbm,
                    [s.sum_sem.at[k] for k in range(4)], s.keep_sem)
    reached = [0] * len(chunks)
    visits = {}
    split = len(chunks) * 2 * product_rows > sum(chunks)
    chunk_of = {name: name for name in range(len(chunks))}
    if not split:
        del chunk_of[len(chunks) - 1]
        chunk_of[len(chunks)] = len(chunks) - 1

    def sum_step(c):
        big.advance(c, reached[c])
        reached[c] += 1

    def ticks(where):
        visit = visits.get(where, 0)
        visits[where] = visit + 1
        for name in pace.get((where, visit), ()):
            if name in chunk_of:
                sum_step(chunk_of[name])

    def put_product(at, value):
        for c in range(value.shape[1] // 128):
            s.mine[pl.ds(at + c * width, width), :] = value[
                :, c * 128 : (c + 1) * 128
            ].astype(half)

    for j in range(parts):
        at = slice(j * width, (j + 1) * width)

        def feed(r, carry):
            here = row_span(r)
            value = dot_nn(s.normed_two[here, :], s.inner_w[:, at]) + inner_bias[:, at]
            share = 0.5 + 0.5 * lax.erf(value * (0.5 ** 0.5))
            density = jnp.exp(-0.5 * value * value) * (0.5 / math.pi) ** 0.5
            s.activated[here, at] = (value * share).astype(half)
            grad = s.grad_inner[here, at].astype(full) * (share + value * density)
            low = grad.astype(half)
            s.grad_inner[here, at] = low
            return carry + jnp.sum(low.astype(full), axis=0, keepdims=True)

        total = lax.fori_loop(0, rows, feed, jnp.zeros((1, width), full))
        put_small(Small.inner_bias, j * width, total)
        put_product(tile_at(Product.inner, j, 0), dot_tn(s.normed_two[...], s.grad_inner[:, at]))
        put_product(tile_at(Product.outer, j, 0), dot_tn(s.activated[:, at], s.grad_branch[...]))
        ticks(Site.feed)

    def grad_copy(owner, slot):
        row, group = owner // per_row, owner % per_row
        column = pl.ds(pl.multiple_of(group * own_width, own_width), own_width)
        return remote(
            s.grad_att.at[row_span(row), column], s.grad_heads.at[nr_rows(slot), :],
            s.grad_sent.at[owner], s.grad_got.at[slot], (place.batch, owner),
        )

    gain_sum = jnp.zeros((1, width), full)
    shift_sum = jnp.zeros((1, width), full)
    for step in range(rows):
        r = (my_row + 1 + step) % rows
        at = row_span(r)
        grad = dot_nt(s.grad_inner[at, :], s.inner_w[...])
        scaled, inverse = centred_rows(s.residual[at, :])
        gain_sum = gain_sum + jnp.sum(grad * scaled, axis=0, keepdims=True)
        shift_sum = shift_sum + jnp.sum(grad, axis=0, keepdims=True)
        mixed = s.grad_resid[at, :] + norm_back(grad, scaled, inverse, gain_two[...])
        s.grad_resid[at, :] = mixed
        s.grad_att[at, :] = dot_nt(mixed.astype(half), s.out_w[...]).astype(half)
        for g in range(per_row):
            owner = r * per_row + g
            if step < rows - 1:
                grad_copy(owner, me).start()
            else:

                @pl.when(owner != me)
                def _():
                    grad_copy(owner, me).start()

                @pl.when(owner == me)
                def _():
                    pltpu.make_async_copy(
                        s.grad_att.at[row_span(my_row), pl.ds(first_column, own_width)],
                        s.grad_heads.at[nr_rows(me), :], s.own_sem.at[2],
                    ).start()
        ticks(Site.norm_two)
    put_small(Small.gain_two, 0, gain_sum)
    put_small(Small.shift_two, 0, shift_sum)

    def second_residual(r, carry):
        at = row_span(r)
        value = s.residual[at, :] + dot_nn(s.activated[at, :], s.outer_w[...])
        s.normed_two[at, :] = (value + outer_bias[...]).astype(half)
        return carry

    for r in range(rows):
        second_residual(r, 0)
        ticks(Site.second)
    for k in range(3):
        at = slice(k * width, (k + 1) * width)
        put_product(tile_at(Product.up, k, 0), dot_tn(s.normed_two[...], s.dy[:, at]))
        ticks(Site.up)
    put_product(tile_at(Product.out, 0, 0), dot_tn(s.att[...], s.grad_resid[...].astype(half)))
    ticks(Site.out)

    up_row = jnp.concatenate(
        [up_bias[c : c + 128].reshape(1, 128) for c in range(0, 3 * width, 128)], axis=1
    )

    def raise_row(r, carry):
        for k in range(3):
            at = slice(k * width, (k + 1) * width)
            raised = dot_nn(s.normed_two[row_span(r), :], s.up_w[:, at])
            put_third(8 + k, raised + up_row[:, at])
        whole = jnp.concatenate([stage[c, 8 : 8 + 3 * block, :] for c in range(lanes)], axis=1)
        s.raised[r] = (s.raised[r].astype(full) + whole).astype(half)
        return carry

    loads.x.wait()
    for r in range(rows):
        raise_row(r, 0)
        ticks(Site.rise)
    output_copy = pltpu.make_async_copy(s.raised, output_hbm, s.own_sem.at[3])
    output_copy.start()

    blank = jnp.zeros((width, 128), half)
    for name in (Product.query, Product.key, Product.value):
        for c in range(lanes):
            s.mine[pl.ds(tile_at(name, 0, c), width), :] = blank

    pltpu.make_async_copy(
        s.grad_att.at[row_span(my_row), pl.ds(first_column, own_width)],
        s.grad_heads.at[nr_rows(me), :], s.own_sem.at[2],
    ).wait()
    ticks(Site.heads)
    for k in range(1, size.seq):
        grad_copy((me + k) % size.seq, (me + k) % size.seq).wait_recv()

    half_blocks = size.query_blocks // 2

    def value_tile(p, j):
        lane = pl.multiple_of((p * half_blocks + j // 2) * 128, 128)
        return s.residual.at[(j % 2) * span : (j % 2 + 1) * span, pl.ds(lane, 128)]

    def value_block(p, b):
        lane = pl.multiple_of((p * half_blocks + b // 4) * 128, 128)
        return s.residual.at[row_span(b % 4), pl.ds(lane, 128)]

    def key_tile(p, j):
        at = p * half_blocks + j // 2
        return s.work.at[at, :, (j % 2) * 128 : (j % 2 + 1) * 128]

    def key_block(p, b):
        lane = pl.multiple_of(b // 2 % 2 * 128, 128)
        return s.work.at[p * half_blocks + b // 4, row_span(b % 2), pl.ds(lane, 128)]

    turned = s.work.at[2 * size.reach + 1, 0:own_width, :]

    for i in range(size.query_blocks):
        cols = slice(i * span, (i + 1) * span)
        turned[...] = s.grad_heads[cols, :].astype(full).T
        query_at = (i * span + lax.broadcasted_iota(jnp.int32, (1, span), 1)).astype(full)

        def backward_pair(p, carry):
            for side in range(2):
                h = 2 * p + side
                head = pl.ds(pl.multiple_of(h * 64, 64), 64)
                inverse = s.inverse[h, 0:1, cols]
                grad = turned[head, :] * inverse
                term = jnp.sum(grad * s.mixed[head, cols], axis=0, keepdims=True)
                low = grad.astype(half)
                zeros = jnp.zeros((64, span), half)
                low = jnp.concatenate([low, zeros] if side == 0 else [zeros, low], axis=0)
                query_grad = jnp.zeros((80, span), full)
                for j in near(i):
                    keys = slice(j * span, (j + 1) * span)
                    expo = s.expo[h, tile_of(i, j)]
                    grad_probs = dot_nn(s.v[p, keys, :], low)
                    grad_scores = (expo.astype(full) * (grad_probs - term)).astype(half)
                    to_value = dot_nt(expo, low)
                    to_key = dot_nt(grad_scores, s.qt[h, :, cols])
                    if j == i and side == 0:
                        value_tile(p, j)[...] = to_value
                        key_tile(p, j)[...] = to_key
                    else:
                        value_tile(p, j)[...] += to_value
                        key_tile(p, j)[...] += to_key
                    query_grad = query_grad + dot_nn(s.kt[h, :, keys], grad_scores)
                s.mixed[head, cols] = query_grad[:64, :]
                slope = (
                    query_grad[65:66, :] + query_grad[66:67, :] - query_at * query_grad[64:65, :]
                )
                slope = jnp.broadcast_to(slope, (8, span))
                if i == 0:
                    s.slope_sum[h] = slope
                else:
                    s.slope_sum[h] += slope
            return carry

        for p in range(pairs):
            backward_pair(p, 0)
            ticks(Site.back)

    head_lane = lax.broadcasted_iota(jnp.int32, (1, 128), 1)
    slope_row = jnp.zeros((1, 128), full)
    for h in range(size.own_heads):
        total = jnp.sum(s.slope_sum[h][0:1, :], axis=1, keepdims=True)
        slope_row = slope_row + jnp.where(head_lane == my_group * size.own_heads + h, total, 0.0)
    small_block[0, pl.ds(Small.slopes, 1), :] = slope_row

    scale = size.head_dim ** -0.5

    fit = width // own_width

    def grads_at(which, at=None):
        down = which // fit * length
        if at is None:
            at = pl.ds(down, length)
        else:
            at = pl.ds(pl.multiple_of(at + down, block), block)
        return s.outer_w.at[at, which % fit * own_width : (which % fit + 1) * own_width]

    def settle(b, carry):
        at = nr_rows(b)
        for which in range(3):
            target = grads_at(which, b * block)
            if which == 0:
                target[...] = (s.mixed[:, at].T * scale).astype(half)
                continue
            for p in range(pairs):
                lane = slice(p * 128, (p + 1) * 128)
                if which == 1:
                    target[:, lane] = (key_block(p, b)[...] * scale).astype(half)
                else:
                    target[:, lane] = value_block(p, b)[...].astype(half)
        return carry

    lax.fori_loop(0, size.seq, settle, 0)
    ticks(Site.settle)

    def normed_grad(owner):
        return (
            dot_nt(grads_at(0, owner * block)[...], s.query_w[...])
            + dot_nt(grads_at(1, owner * block)[...], s.key_w[...])
            + dot_nt(grads_at(2, owner * block)[...], s.value_w[...])
        )

    def held(first, owner_level):
        across_at = (first + owner_level // rows) * width
        return s.activated.at[
            row_span(owner_level % rows), pl.ds(pl.multiple_of(across_at, width), width)
        ]

    held_parts = -(-depth // rows)

    def pair_copy(owner_level):
        return remote(
            held(0, owner_level), s.pair_in.at[row_span(owner_level), :],
            s.pair_sent.at[owner_level], s.pair_got.at[owner_level],
            (place.batch, level * 2 + 1 - core),
        )

    def back_copy(owner_level, source_level):
        row, part = source_level // chips, source_level % chips
        return remote(
            held(held_parts, owner_level),
            s.back.at[part, row_span(row), :],
            s.back_sent.at[owner_level], s.back_got.at[source_level],
            (place.batch, owner_level * 2 + core),
        )

    for k in range(depth):
        owner_level = (level + 1 + k) % depth
        held(0, owner_level)[...] = normed_grad(owner_level * 2 + 1 - core).astype(half)
        pair_copy(owner_level).start()
        ticks(Site.pair)
    for k in range(depth):
        owner_level = (level + 1 + k) % depth
        grad = normed_grad(owner_level * 2 + core)
        pair_copy(owner_level).wait_recv()
        grad = grad + s.pair_in[row_span(owner_level), :].astype(full)
        held(held_parts, owner_level)[...] = grad.astype(half)
        if k < depth - 1:
            back_copy(owner_level, level).start()
        else:
            back_own = pltpu.make_async_copy(
                held(held_parts, level),
                s.back.at[level % chips, row_span(level // chips), :],
                s.own_sem.at[4],
            )
            back_own.start()
        ticks(Site.give)

    for which, name in enumerate((Product.query, Product.key, Product.value)):
        value = dot_tn(nr[...], grads_at(which)[...])
        base = products.index((name, 0)) * product_rows
        for c in range(own_width // 128):
            at = pl.multiple_of(base + (my_group * (own_width // 128) + c) * width, width)
            s.mine[pl.ds(at, width), :] = value[:, c * 128 : (c + 1) * 128].astype(half)
        ticks(Site.weights)

    ticks(Site.rows)
    back_own.wait()
    for k in range(1, depth):
        source_level = (level + k) % depth
        back_copy(source_level, source_level).wait_recv()

    def first_norm(r, carry):
        at = row_span(r)
        grad = s.back[0, at, :].astype(full)
        for part in range(1, chips):
            grad = grad + s.back[part, at, :].astype(full)
        scaled, inverse = centred_rows(s.pooled[at, :])
        low = s.grad_resid[at, :] + norm_back(grad, scaled, inverse, gain_one[...])
        low = low.astype(half)
        s.normed[at, :] = low
        for k in range(3):
            put_third(6 + k, dot_nt(low, s.pool_w[k * width : (k + 1) * width, :]))
        for c in range(lanes):
            lane = slice(c * 128, (c + 1) * 128)
            s.edge_out[r, :, lane] = stage[c, 0:8, :]
            s.edge_end[r, :, lane] = stage[c, 3 * block - 8 : 3 * block + 8, :]
            s.raised[r, :, lane] = stage[c, 8 : 8 + 3 * block, :].astype(half)
        return (
            carry[0] + jnp.sum(grad * scaled, axis=0, keepdims=True),
            carry[1] + jnp.sum(grad, axis=0, keepdims=True),
            carry[2] + jnp.sum(low.astype(full), axis=0, keepdims=True),
        )

    output_copy.wait()
    for k in range(1, depth):
        row_from((level + k) % depth).wait_send()
    nothing = jnp.zeros((1, width), full)
    totals = (nothing,) * 3
    for r in range(rows):
        totals = first_norm(r, totals)
        ticks(Site.norm_one)
    put_small(Small.gain_one, 0, totals[0])
    put_small(Small.shift_one, 0, totals[1])
    put_small(Small.pool_bias, 0, totals[2])
    edge_copy = remote(
        s.edge_out, s.edge_in, s.rim_sem.at[2], s.rim_sem.at[3],
        (place.batch, (me + size.seq - 1) % size.seq),
    )

    @pl.when(me > 0)
    def _():
        edge_copy.start()

    small = SumSmall(place, small_block, s.small_landing,
                     [s.small_sem.at[0], s.small_sem.at[1]])
    small.send(0)
    for k in range(3):
        at = slice(k * width, (k + 1) * width)
        put_product(tile_at(Product.pool, k, 0), dot_tn(s.groups[:, at], s.normed[...]))
        ticks(Site.pool)

    @pl.when(me < size.seq - 1)
    def _():
        edge_copy.wait_recv()

    edge_row = lax.broadcasted_iota(jnp.int32, (16, width), 0)
    for r in range(rows):
        edge = jnp.where(me < size.seq - 1, s.edge_in[r], 0.0)
        edge = jnp.concatenate([edge, edge], axis=0)
        edge = jnp.where(edge_row >= 14, edge, s.edge_end[r])
        s.raised[r, 3 * block - 16 : 3 * block, :] = edge.astype(half)
    shift_copy = pltpu.make_async_copy(s.raised, shift_hbm, s.own_sem.at[5])
    shift_copy.start()

    rest = [chunk_of[name] for name in finish_order if name in chunk_of]
    small_stage, last_stage = 0, len(place.sizes)
    for number, c in enumerate(rest):
        if reached[c] < big.events:
            sum_step(c)
        if number % 4 == 3 and small_stage < last_stage:
            small.receive(small_stage)
            small_stage += 1
            if small_stage < last_stage:
                small.send(small_stage)
    while small_stage < last_stage:
        small.receive(small_stage)
        small_stage += 1
        if small_stage < last_stage:
            small.send(small_stage)
    for c in range(len(chunks)):
        while reached[c] < big.events:
            sum_step(c)
    small_out[...] = small_block[last_stage]

    shift_copy.wait()

    @pl.when(me < size.seq - 1)
    def _():
        rim_copy.wait_send()

    @pl.when(me > 0)
    def _():
        edge_copy.wait_send()

    for k in range(1, depth):
        other = (level + k) % depth
        back_copy(other, other).wait_send()
    for k in range(depth):
        across(k, core).wait_send()
        pair_copy(k).wait_send()
    for k in range(1, size.seq):
        other = (me + k) % size.seq
        att_copy(other, other // per_row, other % per_row, other).wait_send()
        grad_copy(other, other).wait_send()
    big.finish()
    small.finish()


def scratch_plan(size, chunks):
    tokens, length, width, hidden = size.tokens, size.length, size.width, size.hidden
    rows, block, depth = size.rows, size.block, size.depth
    own, pairs, heads = size.own_width, size.pairs, size.own_heads
    near = size.reach + 1
    stages = stage_sizes(size.batch, size.seq)
    orders = axis_orders(size, len(chunks))
    slots = sum_slots(size.batch, size.seq)
    dma = pltpu.SemaphoreType.DMA
    total = sum(chunks)
    return dict(
        x=pltpu.VMEM((2, 3 * block, width), half),
        raised=pltpu.VMEM((rows, 3 * block, width), half),
        pool_w=pltpu.VMEM((3 * width, width), half),
        up_w=pltpu.VMEM((width, 3 * width), half),
        query_w=pltpu.VMEM((width, own), half),
        key_w=pltpu.VMEM((width, own), half),
        value_w=pltpu.VMEM((width, own), half),
        outer_w=pltpu.VMEM((hidden, width), half),
        inner_w=pltpu.VMEM((width, hidden), half),
        out_w=pltpu.VMEM((width, width), half),
        rim=pltpu.VMEM((rows, 16, width), half),
        stage=pltpu.VMEM((size.lanes, 3 * block + 8, 128), full),
        groups=pltpu.VMEM((tokens, 3 * width), half),
        dy=pltpu.VMEM((tokens, 3 * width), half),
        grad_resid=pltpu.VMEM((tokens, width), full),
        grad_branch=pltpu.VMEM((tokens, width), half),
        pooled=pltpu.VMEM((tokens, width), full),
        normed=pltpu.VMEM((tokens, width), half),
        nr=pltpu.VMEM((length, width), half),
        grad_inner=pltpu.VMEM((tokens, hidden), half),
        activated=pltpu.VMEM((tokens, hidden), half),
        qt=pltpu.VMEM((heads, 128, length), half),
        kt=pltpu.VMEM((heads, 80, length), half),
        vt=pltpu.VMEM((own, length), half),
        k=pltpu.VMEM((pairs, length, 128), half),
        v=pltpu.VMEM((pairs, length, 128), half),
        work=pltpu.VMEM((2 * near, size.span, size.span), full),
        expo=pltpu.VMEM((heads, len(size.tiles), size.span, size.span), half),
        inverse=pltpu.VMEM((heads, 8, length), full),
        mixed=pltpu.VMEM((own, length), full),
        att_out=pltpu.VMEM((length, own), half),
        att=pltpu.VMEM((tokens, width), half),
        residual=pltpu.VMEM((tokens, width), full),
        normed_two=pltpu.VMEM((tokens, width), half),
        grad_att=pltpu.VMEM((tokens, width), half),
        grad_heads=pltpu.VMEM((length, own), half),
        slope_sum=pltpu.VMEM((heads, 8, size.span), full),
        pair_in=pltpu.VMEM((depth * block, width), half),
        back=pltpu.VMEM((size.chips_per_row, tokens, width), half),
        edge_out=pltpu.VMEM((rows, 8, width), full),
        edge_in=pltpu.VMEM((rows, 8, width), full),
        edge_end=pltpu.VMEM((rows, 16, width), full),
        mine=pltpu.VMEM((total, 128), half),
        landing=pltpu.VMEM((SumPieces.landing_rows(size.batch, size.seq, chunks, orders), 128), half),
        piece=pltpu.VMEM((total // (size.batch * size.seq), 128), half),
        small_block=pltpu.VMEM((len(stages) + 1, small_rows, 128), full),
        small_landing=pltpu.VMEM((sum(stages), small_rows, 128), full),
        load_sem=dma((10,)),
        x_sem=dma((2,)),
        rim_sem=dma((4,)),
        own_sem=dma((6,)),
        row_sent=dma((depth,)),
        row_got=dma((depth,)),
        across_sent=dma((depth,)),
        across_got=dma((depth,)),
        att_sent=dma((size.seq,)),
        att_got=dma((size.seq,)),
        grad_sent=dma((size.seq,)),
        grad_got=dma((size.seq,)),
        pair_sent=dma((depth,)),
        pair_got=dma((depth,)),
        back_sent=dma((depth,)),
        back_got=dma((depth,)),
        sum_sem=dma((4, len(chunks), slots)),
        keep_sem=dma((len(chunks),)),
        small_sem=dma((2, slots)),
    )


def widen_kernel(plan, steps, places, sums, shift, cotangent, small, *refs):
    outs = dict(zip(plan, refs[: len(plan)]))
    grad_inputs = refs[len(plan)]
    vectors = refs[len(plan) + 1 : len(plan) + 1 + len(places)]
    source, target, moved, kept, result, load_sem, store_sem, row_sem = refs[
        len(plan) + 1 + len(places) :
    ]
    rows = shift.shape[0]
    deep = source.shape[0]
    product_rows = source.shape[1]
    width = target.shape[1]

    def load(i):
        return pltpu.make_async_copy(
            sums.at[pl.ds(i * product_rows, product_rows), :], source.at[i % deep],
            load_sem.at[i % deep],
        )

    def store(i):
        name, part = steps[i]
        out = outs[name]
        if out.shape[0] > width:
            out = out.at[pl.ds(part * width, width), :]
        elif out.shape[1] > width:
            out = out.at[:, pl.ds(part * width, width)]
        return pltpu.make_async_copy(target.at[i % deep], out, store_sem.at[i % deep])

    def row_loads(r):
        return (
            pltpu.make_async_copy(shift.at[r], moved.at[r % 2], row_sem.at[0, r % 2]),
            pltpu.make_async_copy(cotangent.at[r], kept.at[r % 2], row_sem.at[1, r % 2]),
        )

    def row_store(r):
        return pltpu.make_async_copy(result.at[r % 2], grad_inputs.at[r], row_sem.at[2, r % 2])

    for i in range(deep - 1):
        load(i).start()
    for at, out in zip(places, vectors):
        count = out.shape[-1]
        for c in range(0, count, 128):
            part = min(128, count - c)
            if len(out.shape) == 1:
                out[c : c + part] = small[at + c // 128, :part]
            else:
                out[:, c : c + part] = small[at + c // 128 : at + c // 128 + 1, :part]
    for copy in row_loads(0):
        copy.start()
    for r in range(rows):
        if r + 1 < rows:
            for copy in row_loads(r + 1):
                copy.start()
        for copy in row_loads(r):
            copy.wait()
        if r >= 2:
            row_store(r - 2).wait()

        def add_rows(b, carry):
            at = pl.ds(pl.multiple_of(b * 64, 64), 64)
            result[r % 2, at, :] = moved[r % 2, at, :].astype(full) + kept[
                r % 2, at, :
            ].astype(full)
            return carry

        lax.fori_loop(0, result.shape[1] // 64, add_rows, 0)
        row_store(r).start()
    for i in range(len(steps)):
        if i + deep - 1 < len(steps):
            load(i + deep - 1).start()
        load(i).wait()
        if i >= deep:
            store(i - deep).wait()

        def convert(b, carry):
            at = pl.multiple_of(b * 64, 64)
            for c in range(product_rows // width):
                target[i % deep, pl.ds(at, 64), c * 128 : (c + 1) * 128] = source[
                    i % deep, pl.ds(c * width + at, 64), :
                ].astype(full)
            return carry

        lax.fori_loop(0, width // 64, convert, 0)
        store(i).start()
    for r in range(max(0, rows - 2), rows):
        row_store(r).wait()
    for i in range(max(0, len(steps) - deep), len(steps)):
        store(i).wait()


def widen(sums, shift, cotangent, small, counts, shapes, steps):
    any_space = pl.BlockSpec(memory_space=pl.ANY)
    names = tuple(shapes)
    width = shift.shape[2]
    deep = 6
    outs = [jax.ShapeDtypeStruct(shapes[name], full) for name in names]
    outs.append(jax.ShapeDtypeStruct(shift.shape, full))
    outs += [
        jax.ShapeDtypeStruct(
            (count,) if count % 1024 == 512 and count > 512 else (1, count), full
        )
        for count in counts.values()
    ]
    vmem = pl.BlockSpec(memory_space=pltpu.VMEM)
    row = shift.shape[1:]
    product_rows = sums.shape[0] // len(steps)
    results = pl.pallas_call(
        functools.partial(widen_kernel, names, steps, tuple(counts)),
        out_shape=outs,
        in_specs=[any_space] * 3 + [vmem],
        out_specs=[any_space] * (len(names) + 1) + [vmem] * len(counts),
        scratch_shapes=[
            pltpu.VMEM((deep, product_rows, 128), half),
            pltpu.VMEM((deep, width, width), full),
            pltpu.VMEM((2,) + row, half),
            pltpu.VMEM((2,) + row, half),
            pltpu.VMEM((2,) + row, full),
            pltpu.SemaphoreType.DMA((deep,)),
            pltpu.SemaphoreType.DMA((deep,)),
            pltpu.SemaphoreType.DMA((3, 2)),
        ],
        name="widen",
    )(sums, shift, cotangent, small)
    vectors = {
        at: value.reshape(-1) for at, value in zip(counts, results[len(names) + 1 :])
    }
    return dict(zip(names, results)), results[len(names)], vectors


def local(
    inputs,
    cotangent,
    doc_lengths,
    pool_weight,
    pool_bias,
    gain_one,
    shift_one,
    query_weight,
    key_weight,
    value_weight,
    out_weight,
    slopes,
    gain_two,
    shift_two,
    inner_weight,
    inner_bias,
    outer_weight,
    outer_bias,
    up_weight,
    up_bias,
):
    rows, block_len, width = inputs.shape
    hidden = inner_weight.shape[1]
    size = Sizes(
        lax.axis_size("batch"), lax.axis_size("seq"), rows, block_len // 3, width,
        hidden, slopes.shape[0],
    )
    steps = product_list(size.parts)
    product_rows = width * size.lanes
    chunks = [2 * product_rows] * (len(steps) // 2)
    if product_rows % (16 * size.batch * size.seq) == 0:
        chunks[-1:] = [product_rows] * 2
    total = len(steps) * product_rows
    vmem = pl.BlockSpec(memory_space=pltpu.VMEM)
    smem = pl.BlockSpec(memory_space=pltpu.SMEM)
    any_space = pl.BlockSpec(memory_space=pl.ANY)
    plan = scratch_plan(size, chunks)
    vectors = (
        pool_bias, gain_one, shift_one, gain_two, shift_two, inner_bias, outer_bias, up_bias,
    )
    output, shift, sums, small = pl.pallas_call(
        functools.partial(layer_kernel, size, chunks),
        out_shape=(
            jax.ShapeDtypeStruct(inputs.shape, half),
            jax.ShapeDtypeStruct(inputs.shape, half),
            jax.ShapeDtypeStruct((total, 128), half),
            jax.ShapeDtypeStruct((small_rows, 128), full),
        ),
        in_specs=[smem, smem] + [vmem] * 8 + [any_space] * 10,
        out_specs=(any_space, any_space, any_space, vmem),
        scratch_shapes=list(plan.values()),
        compiler_params=pltpu.CompilerParams(
            collective_id=0, has_side_effects=True, vmem_limit_bytes=67043328
        ),
        name="layer",
    )(
        doc_lengths, slopes, *(v.reshape(1, -1) for v in vectors[:-1]), up_bias,
        inputs, cotangent, pool_weight, query_weight, key_weight, value_weight,
        out_weight, inner_weight, outer_weight, up_weight,
    )
    shapes = {
        Product.inner: inner_weight.shape, Product.outer: outer_weight.shape, Product.up: up_weight.shape,
        Product.out: out_weight.shape, Product.query: query_weight.shape, Product.key: key_weight.shape,
        Product.value: value_weight.shape, Product.pool: pool_weight.shape,
    }
    counts = {
        Small.pool_bias: width, Small.gain_one: width, Small.shift_one: width,
        Small.slopes: slopes.shape[0], Small.gain_two: width, Small.shift_two: width,
        Small.inner_bias: hidden, Small.outer_bias: width, Small.up_bias: 3 * width,
    }
    grads, input_grad, vector = widen(sums, shift, cotangent, small, counts, shapes, steps)

    return (
        output,
        input_grad,
        grads[Product.pool],
        vector[Small.pool_bias],
        vector[Small.gain_one],
        vector[Small.shift_one],
        grads[Product.query],
        grads[Product.key],
        grads[Product.value],
        grads[Product.out],
        vector[Small.slopes],
        vector[Small.gain_two],
        vector[Small.shift_two],
        grads[Product.inner],
        vector[Small.inner_bias],
        grads[Product.outer],
        vector[Small.outer_bias],
        grads[Product.up],
        vector[Small.up_bias],
    )


def solution(mesh):
    blocks = P("batch", "seq", None)
    in_specs = (blocks, blocks, P("batch", None)) + (P(),) * 17
    out_specs = (blocks, blocks) + (P(),) * 17
    return jax.shard_map(local, mesh=mesh, in_specs=in_specs, out_specs=out_specs, check_vma=False)
```

```python
import functools
import math
from types import SimpleNamespace

import jax
import jax.numpy as jnp
from jax import lax
from jax.experimental import pallas as pl
from jax.experimental.pallas import tpu as pltpu
from jax.sharding import PartitionSpec as P

norm_eps = 1e-05
log2_e = math.log2(math.e)

MESH = pl.DeviceIdType.MESH
half = jnp.bfloat16
full = jnp.float32


class Place:
    def __init__(self, batch_size, seq_size):
        side = math.isqrt(batch_size)
        self.depth = seq_size // 2
        self.batch = lax.axis_index("batch")
        self.seq = lax.axis_index("seq")
        self.core = self.seq % 2
        self.level = self.seq // 2
        high, low = self.batch // side, self.batch % side
        self.first = jnp.where(self.core == 0, low, high)
        self.second = jnp.where(self.core == 0, high, low)
        self.side = side
        self.sizes = stage_sizes(batch_size, seq_size)
        bits = [self.level // 2**b % 2 for b in range(len(self.sizes) - 3)]
        self.where = (self.core, self.first, self.second, *bits)

    def batch_at(self, first, second):
        return jnp.where(
            self.core == 0, second * self.side + first, first * self.side + second
        )

    def partner(self, stage, step):
        member = (self.where[stage] + step) % self.sizes[stage]
        if stage == 0:
            return (self.batch, self.level * 2 + member)
        if stage == 1:
            return (self.batch_at(member, self.second), self.seq)
        if stage == 2:
            return (self.batch_at(self.first, member), self.seq)
        other = self.level + (member - self.where[stage]) * 2 ** (stage - 3)
        return (self.batch, other * 2 + self.core)


def stage_sizes(batch_size, seq_size):
    side = math.isqrt(batch_size)
    bits = (seq_size // 2).bit_length() - 1
    return (2, side, side) + (2,) * bits


def sum_slots(batch_size, seq_size):
    return sum(size - 1 for size in stage_sizes(batch_size, seq_size))


class SumPieces:
    def __init__(self, place, chunks, orders, mine, landing, piece, out, sems, keep):
        self.place, self.chunks, self.orders = place, chunks, orders
        self.mine, self.landing, self.piece, self.out = mine, landing, piece, out
        self.keep = keep
        self.sent, self.got, self.back_sent, self.back_got = sems
        self.starts = [sum(chunks[:c]) for c in range(len(chunks))]
        sizes = place.sizes
        self.last = len(sizes) - 1
        self.events = 2 * len(sizes) + 1
        self.land = {}
        at = 0
        for c in range(len(chunks)):
            for stage in range(len(sizes)):
                for step in self.steps(c, stage):
                    self.land[c, stage, step] = at
                    at += self.rows(c, stage)

    @staticmethod
    def landing_rows(batch_size, seq_size, chunks, orders):
        sizes, rows = stage_sizes(batch_size, seq_size), 0
        for left, order in zip(chunks, orders):
            for axis in order:
                left //= sizes[axis]
                rows += left * (sizes[axis] - 1)
        return rows

    def size_at(self, c, stage):
        return self.place.sizes[self.orders[c][stage]]

    def where_at(self, c, stage):
        return self.place.where[self.orders[c][stage]]

    def slot(self, c, stage):
        return sum(self.size_at(c, t) - 1 for t in range(stage))

    def rows(self, c, stage):
        count = self.chunks[c]
        for t in range(stage + 1):
            count //= self.size_at(c, t)
        return count

    def begin(self, c, stage):
        at = self.starts[c]
        for t in range(stage):
            at = at + self.where_at(c, t) * self.rows(c, t)
        return at

    def scatter(self, c, stage, step):
        count = self.rows(c, stage)
        member = (self.where_at(c, stage) + step) % self.size_at(c, stage)
        at = pl.multiple_of(self.begin(c, stage) + member * count, 16)
        slot = self.slot(c, stage) + step - 1
        return pltpu.make_async_remote_copy(
            src_ref=self.mine.at[pl.ds(at, count), :],
            dst_ref=self.landing.at[pl.ds(self.land[c, stage, step], count), :],
            send_sem=self.sent.at[c, slot],
            recv_sem=self.got.at[c, slot],
            device_id=self.place.partner(self.orders[c][stage], step),
            device_id_type=MESH,
        )

    def piece_span(self, c):
        count = self.rows(c, self.last)
        return pl.ds(self.starts[c] * count // self.chunks[c], count)

    def keep_copy(self, c):
        at = pl.multiple_of(self.begin(c, self.last + 1), 16)
        return pltpu.make_async_copy(
            self.piece.at[self.piece_span(c), :],
            self.out.at[pl.ds(at, self.rows(c, self.last)), :],
            self.keep.at[c],
        )

    def gather(self, c, stage, step):
        count = self.rows(c, stage)
        at = pl.multiple_of(self.begin(c, stage + 1), 16)
        slot = self.slot(c, stage) + step - 1
        source = self.out.at[pl.ds(at, count), :]
        if stage == self.last:
            source = self.piece.at[self.piece_span(c), :]
        return pltpu.make_async_remote_copy(
            src_ref=source,
            dst_ref=self.out.at[pl.ds(at, count), :],
            send_sem=self.back_sent.at[c, slot],
            recv_sem=self.back_got.at[c, slot],
            device_id=self.place.partner(self.orders[c][stage], step),
            device_id_type=MESH,
        )

    def add(self, c, stage):
        count = self.rows(c, stage)
        at = self.begin(c, stage + 1)
        part = min(count, 512)

        def body(i, carry):
            here = pl.ds(pl.multiple_of(at + i * part, 16), part)
            if self.size_at(c, stage) == 2:
                there = pl.multiple_of(self.land[c, stage, 1] + i * part, 16)
                total = self.mine[here, :] + self.landing[pl.ds(there, part), :]
            else:
                total = self.mine[here, :].astype(full)
                for step in self.steps(c, stage):
                    there = pl.multiple_of(self.land[c, stage, step] + i * part, 16)
                    total = total + self.landing[pl.ds(there, part), :].astype(full)
                total = total.astype(half)
            if stage == self.last:
                first = self.piece_span(c).start
                self.piece[pl.ds(pl.multiple_of(first + i * part, 16), part), :] = total
            else:
                self.mine[here, :] = total
            return carry

        lax.fori_loop(0, count // part, body, 0)

    def steps(self, c, stage):
        return range(1, self.size_at(c, stage))

    def advance(self, c, event):
        count = self.last + 1
        if 1 <= event <= count:
            for step in self.steps(c, event - 1):
                self.scatter(c, event - 1, step).wait_recv()
            self.add(c, event - 1)
        if event < count:
            for step in self.steps(c, event):
                self.scatter(c, event, step).start()
            return
        stage = 2 * count - 1 - event
        if event == count:
            self.keep_copy(c).start()
        else:
            for step in self.steps(c, stage + 1):
                self.gather(c, stage + 1, step).wait_recv()
        if event == count + 1:
            self.keep_copy(c).wait()
        if stage >= 0:
            for step in self.steps(c, stage):
                self.gather(c, stage, step).start()

    def finish(self):
        for c in range(len(self.chunks)):
            for stage in range(self.last + 1):
                for step in self.steps(c, stage):
                    self.scatter(c, stage, step).wait_send()
                    self.gather(c, stage, step).wait_send()


class SumSmall:
    def __init__(self, place, block, landing, sems):
        self.place, self.block, self.landing = place, block, landing
        self.sent, self.got = sems
        sizes = place.sizes
        self.slot = [sum(s - 1 for s in sizes[:stage]) for stage in range(len(sizes))]
        self.base = [sum(sizes[:stage]) for stage in range(len(sizes))]

    def copy(self, stage, step):
        slot = self.slot[stage] + step - 1
        return pltpu.make_async_remote_copy(
            src_ref=self.block.at[stage],
            dst_ref=self.landing.at[self.base[stage] + self.place.where[stage]],
            send_sem=self.sent.at[slot],
            recv_sem=self.got.at[slot],
            device_id=self.place.partner(stage, step),
            device_id_type=MESH,
        )

    def send(self, stage):
        self.landing[self.base[stage] + self.place.where[stage]] = self.block[stage]
        for step in range(1, self.place.sizes[stage]):
            self.copy(stage, step).start()

    def receive(self, stage):
        for step in range(1, self.place.sizes[stage]):
            self.copy(stage, step).wait_recv()
        total = self.landing[self.base[stage]]
        for member in range(1, self.place.sizes[stage]):
            total = total + self.landing[self.base[stage] + member]
        self.block[stage + 1] = total

    def finish(self):
        for stage in range(len(self.place.sizes)):
            for step in range(1, self.place.sizes[stage]):
                self.copy(stage, step).wait_send()


def dot_nn(left, right):
    return lax.dot_general(
        left, right, (((1,), (0,)), ((), ())), preferred_element_type=full
    )


def dot_nt(left, right):
    return lax.dot_general(
        left, right, (((1,), (1,)), ((), ())), preferred_element_type=full
    )


def dot_tn(left, right):
    return lax.dot_general(
        left, right, (((0,), (0,)), ((), ())), preferred_element_type=full
    )


def centred_rows(values_in):
    centre = values_in - jnp.mean(values_in, axis=-1, keepdims=True)
    spread = jnp.mean(centre * centre, axis=-1, keepdims=True)
    inverse = lax.rsqrt(spread + norm_eps)
    return centre * inverse, inverse


def norm_back(grad_normed, scaled, inverse, gain):
    inner = grad_normed * gain
    first = jnp.mean(inner, axis=-1, keepdims=True)
    second = jnp.mean(inner * scaled, axis=-1, keepdims=True)
    return inverse * (inner - first - scaled * second)


class Sizes:
    def __init__(self, batch_size, seq_size, rows, block, width, hidden, heads):
        self.batch, self.seq = batch_size, seq_size
        self.rows, self.block, self.width, self.hidden = rows, block, width, hidden
        self.heads = heads
        self.tokens = rows * block
        self.length = seq_size * block
        self.depth = seq_size // 2
        self.per_row = seq_size // rows
        self.chips_per_row = self.per_row // 2
        self.own_width = width // self.per_row
        self.own_heads = heads // self.per_row
        self.pairs = self.own_heads // 2
        self.head_dim = width // heads
        self.span = 2 * block
        self.query_blocks = self.length // self.span
        self.reach = self.query_blocks // 2
        self.tiles = []
        for i in range(self.query_blocks):
            for j in range(max(0, i - self.reach), i + 1):
                self.tiles.append((i, j))
        self.lanes = width // 128
        self.parts = hidden // width


def product_list(parts):
    order = []
    for j in range(parts):
        order += [(Product.inner, j), (Product.outer, j)]
    order += [(Product.up, 0), (Product.up, 1), (Product.up, 2), (Product.out, 0)]
    order += [(Product.query, 0), (Product.key, 0), (Product.value, 0)]
    order += [(Product.pool, 0), (Product.pool, 1), (Product.pool, 2)]
    return order


class Product:
    inner, outer, up, out, query, key, value, pool = range(8)


class Small:
    pool_bias, gain_one, shift_one, slopes = 0, 4, 8, 12
    gain_two, shift_two, inner_bias, outer_bias, up_bias = 13, 17, 21, 37, 41


class Site:
    feed, norm_two, second, up, out, rise, heads, back, settle = range(9)
    pair, give, weights, rows, norm_one, pool = range(9, 15)


small_rows = 56


pace = {
    (Site.feed, 0): (0,),
    (Site.feed, 1): (1,),
    (Site.feed, 2): (0, 2,),
    (Site.feed, 3): (1, 3,),
    (Site.norm_two, 0): (2,),
    (Site.norm_two, 1): (0,),
    (Site.norm_two, 2): (3,),
    (Site.second, 0): (1,),
    (Site.up, 1): (4,),
    (Site.up, 2): (2,),
    (Site.out, 0): (5,),
    (Site.rise, 0): (0,),
    (Site.rise, 3): (4,),
    (Site.heads, 0): (3, 5, 1, 2, 0,),
    (Site.back, 3): (1,),
    (Site.back, 4): (4, 2, 3, 0,),
    (Site.back, 6): (1, 5,),
    (Site.back, 7): (2, 4, 3,),
    (Site.settle, 0): (0,),
    (Site.pair, 0): (1, 5,),
    (Site.pair, 3): (2,),
    (Site.give, 0): (4,),
    (Site.give, 2): (3, 0,),
    (Site.weights, 0): (1,),
    (Site.weights, 1): (6,),
    (Site.weights, 2): (5,),
    (Site.rows, 0): (2, 0, 1, 6, 2, 0,),
    (Site.norm_one, 1): (0,),
    (Site.norm_one, 2): (1,),
    (Site.pool, 0): (7,),
    (Site.pool, 1): (6, 8,),
    (Site.pool, 2): (4, 1, 3, 9,),
}
finish_order = (
    5, 7, 2, 8, 6, 9, 4, 2, 3, 5, 7, 6, 8, 4, 9, 5,
    3, 6, 7, 8, 6, 4, 7, 9, 8, 5, 6, 9, 7, 3, 8, 9,
    3, 7, 8, 4, 9, 4, 7, 8, 5, 9, 6, 5, 7, 8, 9, 6,
    6, 7, 8, 7, 8, 9, 9,
)
level_first = ()


def axis_orders(size, count):
    axes = tuple(range(len(stage_sizes(size.batch, size.seq))))
    return [
        axes[:2] + axes[3:] + axes[2:3] if c in level_first else axes for c in range(count)
    ]


def layer_kernel(size, chunks, docs, slopes, pool_bias, gain_one, shift_one,
                 gain_two, shift_two, inner_bias, outer_bias, up_bias,
                 inputs_hbm, cotangent_hbm, pool_hbm, query_hbm, key_hbm, value_hbm,
                 out_hbm, inner_hbm, outer_hbm, up_hbm,
                 output_hbm, shift_hbm, sums_hbm, small_out,
                 *scratch_refs):
    s = SimpleNamespace(**dict(zip(scratch_plan(size, chunks), scratch_refs)))
    place = Place(size.batch, size.seq)
    me, core, level = place.seq, place.core, place.level
    rows, block, width, hidden = size.rows, size.block, size.width, size.hidden
    tokens, length, depth = size.tokens, size.length, size.depth
    per_row, chips = size.per_row, size.chips_per_row
    own_width, pairs = size.own_width, size.pairs
    my_row, my_group = me // per_row, me % per_row
    lanes, parts, span = size.lanes, size.parts, size.span
    products = product_list(parts)
    product_rows = width * lanes

    def tile_at(name, part, lane):
        return products.index((name, part)) * product_rows + lane * width

    barrier = pltpu.get_barrier_semaphore()
    greeted = [(place.batch, (me + k) % size.seq) for k in range(1, size.seq)]
    for stage in (1, 2):
        greeted += [place.partner(stage, k) for k in range(1, place.sizes[stage])]
    for device in greeted:
        pl.semaphore_signal(barrier, inc=1, device_id=device, device_id_type=MESH)

    loads = SimpleNamespace()

    def load(source, target):
        copy = pltpu.make_async_copy(source, target, s.load_sem.at[len(vars(loads))])
        copy.start()
        return copy

    first_column = pl.multiple_of(my_group * own_width, own_width)

    def x_load(step):
        return pltpu.make_async_copy(
            inputs_hbm.at[(my_row + 1 + step) % rows], s.x.at[step % 2],
            s.x_sem.at[step % 2],
        )

    x_load(0).start()
    loads.dy = load(cotangent_hbm, s.raised)
    loads.up = load(up_hbm, s.up_w)
    loads.pool = load(pool_hbm, s.pool_w)
    loads.outer = load(outer_hbm, s.outer_w)
    loads.query = load(query_hbm.at[:, pl.ds(first_column, own_width)], s.query_w)
    loads.key = load(key_hbm.at[:, pl.ds(first_column, own_width)], s.key_w)
    loads.value = load(value_hbm.at[:, pl.ds(first_column, own_width)], s.value_w)
    loads.out = load(out_hbm, s.out_w)
    loads.inner = load(inner_hbm, s.inner_w)

    def remote(source, target, sent, got, device):
        return pltpu.make_async_remote_copy(
            src_ref=source, dst_ref=target, send_sem=sent, recv_sem=got,
            device_id=device, device_id_type=MESH,
        )

    small_block = s.small_block
    small_block[0] = jnp.zeros((small_rows, 128), full)

    def put_small(name, at, values):
        for c in range(values.shape[1] // 128):
            small_block[0, pl.ds(name + at // 128 + c, 1), :] = values[
                :, c * 128 : (c + 1) * 128
            ]

    stage = s.stage

    def spread_rows(at, values):
        for c in range(lanes):
            stage[c, pl.ds(at, values.shape[0]), :] = values[:, c * 128 : (c + 1) * 128]

    def every_third(at):
        return jnp.concatenate(
            [stage[c, pl.ds(at, block, stride=3), :] for c in range(lanes)], axis=1
        )

    def put_third(at, values):
        for c in range(lanes):
            stage[c, pl.ds(at, block, stride=3), :] = values[:, c * 128 : (c + 1) * 128]

    def row_span(r):
        return pl.ds(pl.multiple_of(r * block, block), block)

    loads.dy.wait()
    loads.up.wait()
    up_sum = jnp.zeros((1, width), full)

    def split_cotangent(r, carry):
        spread_rows(8, s.raised[r].astype(full))
        totals = []
        grad = jnp.zeros((block, width), full)
        for k in range(3):
            part = every_third(8 + k)
            totals.append(carry[k] + jnp.sum(part, axis=0, keepdims=True))
            low = part.astype(half)
            s.dy[row_span(r), k * width : (k + 1) * width] = low
            grad = grad + dot_nt(low, s.up_w[:, k * width : (k + 1) * width])
        s.grad_resid[row_span(r), :] = grad
        low = grad.astype(half)
        s.grad_branch[row_span(r), :] = low
        totals.append(carry[3] + jnp.sum(low.astype(full), axis=0, keepdims=True))
        return tuple(totals)

    sums = lax.fori_loop(0, rows, split_cotangent, (up_sum,) * 4)
    loads.x = load(inputs_hbm, s.raised)
    for k in range(3):
        put_small(Small.up_bias, k * width, sums[k])
    put_small(Small.outer_bias, 0, sums[3])

    pl.semaphore_wait(barrier, len(greeted))
    rim_copy = remote(
        inputs_hbm.at[:, pl.ds(3 * block - 16, 16), :], s.rim,
        s.rim_sem.at[0], s.rim_sem.at[1], (place.batch, (me + 1) % size.seq),
    )

    @pl.when(me < size.seq - 1)
    def _():
        rim_copy.start()

    loads.outer.wait()

    def before_activation(j, carry):
        at = pl.ds(pl.multiple_of(j * width, width), width)
        grad = dot_nt(s.grad_branch[...], s.outer_w[at, :])
        s.grad_inner[:, at] = grad.astype(half)
        return carry

    lax.fori_loop(0, parts, before_activation, 0)

    @pl.when(me > 0)
    def _():
        rim_copy.wait_recv()

    loads.pool.wait()
    nr = s.nr

    def nr_rows(owner):
        return pl.ds(pl.multiple_of(owner * block, block), block)

    def row_copy(r, target_level):
        return remote(
            s.normed.at[row_span(r), :], nr.at[nr_rows(me), :],
            s.row_sent.at[target_level], s.row_got.at[level],
            (place.batch, target_level * 2 + core),
        )

    def row_from(source_level):
        return remote(
            s.normed.at[row_span(0), :], nr.at[nr_rows(source_level * 2 + core), :],
            s.row_sent.at[source_level], s.row_got.at[source_level],
            (place.batch, source_level * 2 + core),
        )

    for step in range(rows):
        r = (my_row + 1 + step) % rows
        rim_rows = s.rim[r].astype(full)[8:16, :]
        rim_rows = jnp.where(me > 0, rim_rows, 0.0)
        spread_rows(0, rim_rows)
        x_load(step).wait()
        if step + 1 < rows:
            x_load(step + 1).start()
        spread_rows(8, s.x[step % 2].astype(full))
        pooled = jnp.zeros((block, width), full) + pool_bias[...]
        for k in range(3):
            part = every_third(6 + k).astype(half)
            s.groups[row_span(r), k * width : (k + 1) * width] = part
            pooled = pooled + dot_nn(part, s.pool_w[k * width : (k + 1) * width, :])
        s.pooled[row_span(r), :] = pooled
        scaled, _ = centred_rows(pooled)
        s.normed[row_span(r), :] = (scaled * gain_one[...] + shift_one[...]).astype(half)
        if step < rows - 1:
            for i in range(chips):
                row_copy(r, r * chips + i).start()
        else:
            for i in range(1, chips):
                row_copy(r, r * chips + (level % chips + i) % chips).start()
            own_copy = pltpu.make_async_copy(
                s.normed.at[row_span(r), :], nr.at[nr_rows(me), :], s.own_sem.at[0]
            )
            own_copy.start()

    def across(source_level, owner_core):
        owner = source_level * 2 + owner_core
        return remote(
            nr.at[nr_rows(owner), :], nr.at[nr_rows(owner), :],
            s.across_sent.at[source_level], s.across_got.at[source_level],
            (place.batch, level * 2 + 1 - core),
        )

    loads.query.wait()
    loads.key.wait()
    loads.value.wait()

    def project(owner):
        at = nr_rows(owner)
        source = nr[at, :]
        q = dot_nn(source, s.query_w[...])
        k = dot_nn(source, s.key_w[...])
        v = dot_nn(source, s.value_w[...])
        qt, kt, vt = q.T, k.T, v.T
        s.vt[:, at] = vt.astype(half)
        zeros = jnp.zeros((64, block), half)
        line = lax.broadcasted_iota(jnp.int32, (16, block), 0)
        key_at = owner * block + lax.broadcasted_iota(jnp.int32, (16, block), 1)
        fine = (key_at % 128).astype(full)
        coarse = (key_at - key_at % 128).astype(full)
        extra = jnp.where(line == 0, 1.0, jnp.where(line == 1, fine, coarse))
        extra = jnp.where(line < 3, extra, 0.0).astype(half)
        for p in range(pairs):
            s.k[p, at, :] = k[:, p * 128 : (p + 1) * 128].astype(half)
            s.v[p, at, :] = v[:, p * 128 : (p + 1) * 128].astype(half)
            for side in range(2):
                h = 2 * p + side
                piece = qt[h * 64 : (h + 1) * 64, :].astype(half)
                s.qt[h, :, at] = jnp.concatenate(
                    [piece, zeros] if side == 0 else [zeros, piece], axis=0
                )
                piece = kt[h * 64 : (h + 1) * 64, :].astype(half)
                s.kt[h, :, at] = jnp.concatenate([piece, extra], axis=0)

    order = [0]
    for k in range(1, depth):
        order.append((k + 1) // 2 if k % 2 else depth - k // 2)
    for k in order:
        source_level = (level + k) % depth
        if k == 0:
            own_copy.wait()
        else:
            row_from(source_level).wait_recv()
        across(source_level, core).start()
    for k in order:
        source_level = (level + k) % depth
        project(source_level * 2 + core)
        across(source_level, 1 - core).wait_recv()
        project(source_level * 2 + 1 - core)

    ends = []
    total = 0
    for d in range(docs.shape[1]):
        total = total + docs[my_row, d]
        ends.append(total)
    key_line = lax.broadcasted_iota(jnp.int32, (span, span), 0)
    query_line = lax.broadcasted_iota(jnp.int32, (span, span), 1)
    scale_two = size.head_dim ** -0.5 * log2_e

    def tile_of(i, j):
        return size.tiles.index((i, j))

    def near(i):
        return range(max(0, i - size.reach), i + 1)

    def att_copy(owner, at_row, at_group, slot):
        return remote(
            s.att_out.at[nr_rows(owner), :],
            s.att.at[row_span(at_row), pl.ds(pl.multiple_of(at_group * own_width, own_width), own_width)],
            s.att_sent.at[owner], s.att_got.at[slot], (place.batch, owner),
        )

    def head_slope(h):
        return slopes[my_group * size.own_heads + h]

    turns = [
        t // 2 if t % 2 == 0 else size.query_blocks - 1 - t // 2
        for t in range(size.query_blocks)
    ]
    for i in turns:
        cols = slice(i * span, (i + 1) * span)
        place_q = 3 * (i * span + lax.broadcasted_iota(jnp.int32, (1, span), 1))
        start = jnp.zeros((1, span), jnp.int32)
        for end in ends:
            start = jnp.where(end <= place_q, jnp.maximum(start, end), start)
        for w, j in enumerate(near(i)):
            allowed = 3 * (j * span + key_line) >= start
            if j == i:
                allowed = allowed & (key_line <= query_line)
            s.work[size.reach + 1 + w] = jnp.where(allowed, 0.0, -1e30)

        def forward_pair(p, carry):
            for side in range(2):
                h = 2 * p + side
                slope_two = head_slope(h) * log2_e
                top = None
                for w, j in enumerate(near(i)):
                    score = dot_nn(s.k[p, j * span : (j + 1) * span, :], s.qt[h, :, cols])
                    away = (key_line + (j - i) * span).astype(full)
                    score = score * scale_two + (away * slope_two + s.work[size.reach + 1 + w])
                    s.work[w] = score
                    best = jnp.max(score, axis=0, keepdims=True)
                    top = best if top is None else jnp.maximum(top, best)
                total = jnp.zeros((1, span), full)
                mixed = jnp.zeros((64, span), full)
                for w, j in enumerate(near(i)):
                    expo = jnp.exp2(s.work[w] - top)
                    total = total + jnp.sum(expo, axis=0, keepdims=True)
                    low = expo.astype(half)
                    s.expo[h, tile_of(i, j)] = low
                    at = pl.multiple_of(h * 64, 64)
                    mixed = mixed + dot_nn(
                        s.vt[pl.ds(at, 64), j * span : (j + 1) * span], low
                    )
                inverse = 1.0 / total
                s.inverse[h, :, cols] = jnp.broadcast_to(inverse, (8, span))
                s.mixed[pl.ds(pl.multiple_of(h * 64, 64), 64), cols] = mixed * inverse
            return carry

        lax.fori_loop(0, pairs, forward_pair, 0)
        s.att_out[cols, :] = s.mixed[:, cols].T.astype(half)
        for owner in (2 * i, 2 * i + 1):

            @pl.when(me == owner)
            def _():
                copy = pltpu.make_async_copy(
                    s.att_out.at[nr_rows(owner), :],
                    s.att.at[row_span(my_row), pl.ds(first_column, own_width)],
                    s.own_sem.at[1],
                )
                copy.start()

            @pl.when(me != owner)
            def _():
                att_copy(owner, my_row, my_group, me).start()

    loads.out.wait()
    loads.inner.wait()
    pltpu.make_async_copy(
        s.att_out.at[nr_rows(0), :],
        s.att.at[row_span(my_row), pl.ds(first_column, own_width)],
        s.own_sem.at[1],
    ).wait()
    for k in range(1, size.seq):
        source = (me + k) % size.seq
        att_copy(source, source // per_row, source % per_row, source).wait_recv()

    def second_norm(r, carry):
        at = row_span(r)
        residual = s.pooled[at, :] + dot_nn(s.att[at, :], s.out_w[...])
        s.residual[at, :] = residual
        scaled, _ = centred_rows(residual)
        s.normed_two[at, :] = (scaled * gain_two[...] + shift_two[...]).astype(half)
        return carry

    lax.fori_loop(0, rows, second_norm, 0)

    big = SumPieces(place, chunks, axis_orders(size, len(chunks)), s.mine, s.landing, s.piece, sums_hbm,
                    [s.sum_sem.at[k] for k in range(4)], s.keep_sem)
    reached = [0] * len(chunks)
    visits = {}
    split = len(chunks) * 2 * product_rows > sum(chunks)
    chunk_of = {name: name for name in range(len(chunks))}
    if not split:
        del chunk_of[len(chunks) - 1]
        chunk_of[len(chunks)] = len(chunks) - 1

    def sum_step(c):
        big.advance(c, reached[c])
        reached[c] += 1

    def ticks(where):
        visit = visits.get(where, 0)
        visits[where] = visit + 1
        for name in pace.get((where, visit), ()):
            if name in chunk_of:
                sum_step(chunk_of[name])

    def put_product(at, value):
        for c in range(value.shape[1] // 128):
            s.mine[pl.ds(at + c * width, width), :] = value[
                :, c * 128 : (c + 1) * 128
            ].astype(half)

    for j in range(parts):
        at = slice(j * width, (j + 1) * width)

        def feed(r, carry):
            here = row_span(r)
            value = dot_nn(s.normed_two[here, :], s.inner_w[:, at]) + inner_bias[:, at]
            share = 0.5 + 0.5 * lax.erf(value * (0.5 ** 0.5))
            density = jnp.exp(-0.5 * value * value) * (0.5 / math.pi) ** 0.5
            s.activated[here, at] = (value * share).astype(half)
            grad = s.grad_inner[here, at].astype(full) * (share + value * density)
            low = grad.astype(half)
            s.grad_inner[here, at] = low
            return carry + jnp.sum(low.astype(full), axis=0, keepdims=True)

        total = lax.fori_loop(0, rows, feed, jnp.zeros((1, width), full))
        put_small(Small.inner_bias, j * width, total)
        put_product(tile_at(Product.inner, j, 0), dot_tn(s.normed_two[...], s.grad_inner[:, at]))
        put_product(tile_at(Product.outer, j, 0), dot_tn(s.activated[:, at], s.grad_branch[...]))
        ticks(Site.feed)

    def grad_copy(owner, slot):
        row, group = owner // per_row, owner % per_row
        column = pl.ds(pl.multiple_of(group * own_width, own_width), own_width)
        return remote(
            s.grad_att.at[row_span(row), column], s.grad_heads.at[nr_rows(slot), :],
            s.grad_sent.at[owner], s.grad_got.at[slot], (place.batch, owner),
        )

    gain_sum = jnp.zeros((1, width), full)
    shift_sum = jnp.zeros((1, width), full)
    for step in range(rows):
        r = (my_row + 1 + step) % rows
        at = row_span(r)
        grad = dot_nt(s.grad_inner[at, :], s.inner_w[...])
        scaled, inverse = centred_rows(s.residual[at, :])
        gain_sum = gain_sum + jnp.sum(grad * scaled, axis=0, keepdims=True)
        shift_sum = shift_sum + jnp.sum(grad, axis=0, keepdims=True)
        mixed = s.grad_resid[at, :] + norm_back(grad, scaled, inverse, gain_two[...])
        s.grad_resid[at, :] = mixed
        s.grad_att[at, :] = dot_nt(mixed.astype(half), s.out_w[...]).astype(half)
        for g in range(per_row):
            owner = r * per_row + g
            if step < rows - 1:
                grad_copy(owner, me).start()
            else:

                @pl.when(owner != me)
                def _():
                    grad_copy(owner, me).start()

                @pl.when(owner == me)
                def _():
                    pltpu.make_async_copy(
                        s.grad_att.at[row_span(my_row), pl.ds(first_column, own_width)],
                        s.grad_heads.at[nr_rows(me), :], s.own_sem.at[2],
                    ).start()
        ticks(Site.norm_two)
    put_small(Small.gain_two, 0, gain_sum)
    put_small(Small.shift_two, 0, shift_sum)

    def second_residual(r, carry):
        at = row_span(r)
        value = s.residual[at, :] + dot_nn(s.activated[at, :], s.outer_w[...])
        s.normed_two[at, :] = (value + outer_bias[...]).astype(half)
        return carry

    for r in range(rows):
        second_residual(r, 0)
        ticks(Site.second)
    for k in range(3):
        at = slice(k * width, (k + 1) * width)
        put_product(tile_at(Product.up, k, 0), dot_tn(s.normed_two[...], s.dy[:, at]))
        ticks(Site.up)
    put_product(tile_at(Product.out, 0, 0), dot_tn(s.att[...], s.grad_resid[...].astype(half)))
    ticks(Site.out)

    up_row = jnp.concatenate(
        [up_bias[c : c + 128].reshape(1, 128) for c in range(0, 3 * width, 128)], axis=1
    )

    def raise_row(r, carry):
        for k in range(3):
            at = slice(k * width, (k + 1) * width)
            raised = dot_nn(s.normed_two[row_span(r), :], s.up_w[:, at])
            put_third(8 + k, raised + up_row[:, at])
        whole = jnp.concatenate([stage[c, 8 : 8 + 3 * block, :] for c in range(lanes)], axis=1)
        s.raised[r] = (s.raised[r].astype(full) + whole).astype(half)
        return carry

    loads.x.wait()
    for r in range(rows):
        raise_row(r, 0)
        ticks(Site.rise)
    output_copy = pltpu.make_async_copy(s.raised, output_hbm, s.own_sem.at[3])
    output_copy.start()

    blank = jnp.zeros((width, 128), half)
    for name in (Product.query, Product.key, Product.value):
        for c in range(lanes):
            s.mine[pl.ds(tile_at(name, 0, c), width), :] = blank

    pltpu.make_async_copy(
        s.grad_att.at[row_span(my_row), pl.ds(first_column, own_width)],
        s.grad_heads.at[nr_rows(me), :], s.own_sem.at[2],
    ).wait()
    ticks(Site.heads)
    for k in range(1, size.seq):
        grad_copy((me + k) % size.seq, (me + k) % size.seq).wait_recv()

    half_blocks = size.query_blocks // 2

    def value_tile(p, j):
        lane = pl.multiple_of((p * half_blocks + j // 2) * 128, 128)
        return s.residual.at[(j % 2) * span : (j % 2 + 1) * span, pl.ds(lane, 128)]

    def value_block(p, b):
        lane = pl.multiple_of((p * half_blocks + b // 4) * 128, 128)
        return s.residual.at[row_span(b % 4), pl.ds(lane, 128)]

    def key_tile(p, j):
        at = p * half_blocks + j // 2
        return s.work.at[at, :, (j % 2) * 128 : (j % 2 + 1) * 128]

    def key_block(p, b):
        lane = pl.multiple_of(b // 2 % 2 * 128, 128)
        return s.work.at[p * half_blocks + b // 4, row_span(b % 2), pl.ds(lane, 128)]

    turned = s.work.at[2 * size.reach + 1, 0:own_width, :]

    for i in range(size.query_blocks):
        cols = slice(i * span, (i + 1) * span)
        turned[...] = s.grad_heads[cols, :].astype(full).T
        query_at = (i * span + lax.broadcasted_iota(jnp.int32, (1, span), 1)).astype(full)

        def backward_pair(p, carry):
            for side in range(2):
                h = 2 * p + side
                head = pl.ds(pl.multiple_of(h * 64, 64), 64)
                inverse = s.inverse[h, 0:1, cols]
                grad = turned[head, :] * inverse
                term = jnp.sum(grad * s.mixed[head, cols], axis=0, keepdims=True)
                low = grad.astype(half)
                zeros = jnp.zeros((64, span), half)
                low = jnp.concatenate([low, zeros] if side == 0 else [zeros, low], axis=0)
                query_grad = jnp.zeros((80, span), full)
                for j in near(i):
                    keys = slice(j * span, (j + 1) * span)
                    expo = s.expo[h, tile_of(i, j)]
                    grad_probs = dot_nn(s.v[p, keys, :], low)
                    grad_scores = (expo.astype(full) * (grad_probs - term)).astype(half)
                    to_value = dot_nt(expo, low)
                    to_key = dot_nt(grad_scores, s.qt[h, :, cols])
                    if j == i and side == 0:
                        value_tile(p, j)[...] = to_value
                        key_tile(p, j)[...] = to_key
                    else:
                        value_tile(p, j)[...] += to_value
                        key_tile(p, j)[...] += to_key
                    query_grad = query_grad + dot_nn(s.kt[h, :, keys], grad_scores)
                s.mixed[head, cols] = query_grad[:64, :]
                slope = (
                    query_grad[65:66, :] + query_grad[66:67, :] - query_at * query_grad[64:65, :]
                )
                slope = jnp.broadcast_to(slope, (8, span))
                if i == 0:
                    s.slope_sum[h] = slope
                else:
                    s.slope_sum[h] += slope
            return carry

        for p in range(pairs):
            backward_pair(p, 0)
            ticks(Site.back)

    head_lane = lax.broadcasted_iota(jnp.int32, (1, 128), 1)
    slope_row = jnp.zeros((1, 128), full)
    for h in range(size.own_heads):
        total = jnp.sum(s.slope_sum[h][0:1, :], axis=1, keepdims=True)
        slope_row = slope_row + jnp.where(head_lane == my_group * size.own_heads + h, total, 0.0)
    small_block[0, pl.ds(Small.slopes, 1), :] = slope_row

    scale = size.head_dim ** -0.5

    fit = width // own_width

    def grads_at(which, at=None):
        down = which // fit * length
        if at is None:
            at = pl.ds(down, length)
        else:
            at = pl.ds(pl.multiple_of(at + down, block), block)
        return s.outer_w.at[at, which % fit * own_width : (which % fit + 1) * own_width]

    def settle(b, carry):
        at = nr_rows(b)
        for which in range(3):
            target = grads_at(which, b * block)
            if which == 0:
                target[...] = (s.mixed[:, at].T * scale).astype(half)
                continue
            for p in range(pairs):
                lane = slice(p * 128, (p + 1) * 128)
                if which == 1:
                    target[:, lane] = (key_block(p, b)[...] * scale).astype(half)
                else:
                    target[:, lane] = value_block(p, b)[...].astype(half)
        return carry

    lax.fori_loop(0, size.seq, settle, 0)
    ticks(Site.settle)

    def normed_grad(owner):
        return (
            dot_nt(grads_at(0, owner * block)[...], s.query_w[...])
            + dot_nt(grads_at(1, owner * block)[...], s.key_w[...])
            + dot_nt(grads_at(2, owner * block)[...], s.value_w[...])
        )

    def held(first, owner_level):
        across_at = (first + owner_level // rows) * width
        return s.activated.at[
            row_span(owner_level % rows), pl.ds(pl.multiple_of(across_at, width), width)
        ]

    held_parts = -(-depth // rows)

    def pair_copy(owner_level):
        return remote(
            held(0, owner_level), s.pair_in.at[row_span(owner_level), :],
            s.pair_sent.at[owner_level], s.pair_got.at[owner_level],
            (place.batch, level * 2 + 1 - core),
        )

    def back_copy(owner_level, source_level):
        row, part = source_level // chips, source_level % chips
        return remote(
            held(held_parts, owner_level),
            s.back.at[part, row_span(row), :],
            s.back_sent.at[owner_level], s.back_got.at[source_level],
            (place.batch, owner_level * 2 + core),
        )

    for k in range(depth):
        owner_level = (level + 1 + k) % depth
        held(0, owner_level)[...] = normed_grad(owner_level * 2 + 1 - core).astype(half)
        pair_copy(owner_level).start()
        ticks(Site.pair)
    for k in range(depth):
        owner_level = (level + 1 + k) % depth
        grad = normed_grad(owner_level * 2 + core)
        pair_copy(owner_level).wait_recv()
        grad = grad + s.pair_in[row_span(owner_level), :].astype(full)
        held(held_parts, owner_level)[...] = grad.astype(half)
        if k < depth - 1:
            back_copy(owner_level, level).start()
        else:
            back_own = pltpu.make_async_copy(
                held(held_parts, level),
                s.back.at[level % chips, row_span(level // chips), :],
                s.own_sem.at[4],
            )
            back_own.start()
        ticks(Site.give)

    for which, name in enumerate((Product.query, Product.key, Product.value)):
        value = dot_tn(nr[...], grads_at(which)[...])
        base = products.index((name, 0)) * product_rows
        for c in range(own_width // 128):
            at = pl.multiple_of(base + (my_group * (own_width // 128) + c) * width, width)
            s.mine[pl.ds(at, width), :] = value[:, c * 128 : (c + 1) * 128].astype(half)
        ticks(Site.weights)

    ticks(Site.rows)
    back_own.wait()
    for k in range(1, depth):
        source_level = (level + k) % depth
        back_copy(source_level, source_level).wait_recv()

    def first_norm(r, carry):
        at = row_span(r)
        grad = s.back[0, at, :].astype(full)
        for part in range(1, chips):
            grad = grad + s.back[part, at, :].astype(full)
        scaled, inverse = centred_rows(s.pooled[at, :])
        low = s.grad_resid[at, :] + norm_back(grad, scaled, inverse, gain_one[...])
        low = low.astype(half)
        s.normed[at, :] = low
        for k in range(3):
            put_third(6 + k, dot_nt(low, s.pool_w[k * width : (k + 1) * width, :]))
        for c in range(lanes):
            lane = slice(c * 128, (c + 1) * 128)
            s.edge_out[r, :, lane] = stage[c, 0:8, :]
            s.edge_end[r, :, lane] = stage[c, 3 * block - 8 : 3 * block + 8, :]
            s.raised[r, :, lane] = stage[c, 8 : 8 + 3 * block, :].astype(half)
        return (
            carry[0] + jnp.sum(grad * scaled, axis=0, keepdims=True),
            carry[1] + jnp.sum(grad, axis=0, keepdims=True),
            carry[2] + jnp.sum(low.astype(full), axis=0, keepdims=True),
        )

    output_copy.wait()
    for k in range(1, depth):
        row_from((level + k) % depth).wait_send()
    nothing = jnp.zeros((1, width), full)
    totals = (nothing,) * 3
    for r in range(rows):
        totals = first_norm(r, totals)
        ticks(Site.norm_one)
    put_small(Small.gain_one, 0, totals[0])
    put_small(Small.shift_one, 0, totals[1])
    put_small(Small.pool_bias, 0, totals[2])
    edge_copy = remote(
        s.edge_out, s.edge_in, s.rim_sem.at[2], s.rim_sem.at[3],
        (place.batch, (me + size.seq - 1) % size.seq),
    )

    @pl.when(me > 0)
    def _():
        edge_copy.start()

    small = SumSmall(place, small_block, s.small_landing,
                     [s.small_sem.at[0], s.small_sem.at[1]])
    small.send(0)
    for k in range(3):
        at = slice(k * width, (k + 1) * width)
        put_product(tile_at(Product.pool, k, 0), dot_tn(s.groups[:, at], s.normed[...]))
        ticks(Site.pool)

    @pl.when(me < size.seq - 1)
    def _():
        edge_copy.wait_recv()

    edge_row = lax.broadcasted_iota(jnp.int32, (16, width), 0)
    for r in range(rows):
        edge = jnp.where(me < size.seq - 1, s.edge_in[r], 0.0)
        edge = jnp.concatenate([edge, edge], axis=0)
        edge = jnp.where(edge_row >= 14, edge, s.edge_end[r])
        s.raised[r, 3 * block - 16 : 3 * block, :] = edge.astype(half)
    shift_copy = pltpu.make_async_copy(s.raised, shift_hbm, s.own_sem.at[5])
    shift_copy.start()

    rest = [chunk_of[name] for name in finish_order if name in chunk_of]
    small_stage, last_stage = 0, len(place.sizes)
    for number, c in enumerate(rest):
        if reached[c] < big.events:
            sum_step(c)
        if number % 4 == 3 and small_stage < last_stage:
            small.receive(small_stage)
            small_stage += 1
            if small_stage < last_stage:
                small.send(small_stage)
    while small_stage < last_stage:
        small.receive(small_stage)
        small_stage += 1
        if small_stage < last_stage:
            small.send(small_stage)
    for c in range(len(chunks)):
        while reached[c] < big.events:
            sum_step(c)
    small_out[...] = small_block[last_stage]

    shift_copy.wait()

    @pl.when(me < size.seq - 1)
    def _():
        rim_copy.wait_send()

    @pl.when(me > 0)
    def _():
        edge_copy.wait_send()

    for k in range(1, depth):
        other = (level + k) % depth
        back_copy(other, other).wait_send()
    for k in range(depth):
        across(k, core).wait_send()
        pair_copy(k).wait_send()
    for k in range(1, size.seq):
        other = (me + k) % size.seq
        att_copy(other, other // per_row, other % per_row, other).wait_send()
        grad_copy(other, other).wait_send()
    big.finish()
    small.finish()


def scratch_plan(size, chunks):
    tokens, length, width, hidden = size.tokens, size.length, size.width, size.hidden
    rows, block, depth = size.rows, size.block, size.depth
    own, pairs, heads = size.own_width, size.pairs, size.own_heads
    near = size.reach + 1
    stages = stage_sizes(size.batch, size.seq)
    orders = axis_orders(size, len(chunks))
    slots = sum_slots(size.batch, size.seq)
    dma = pltpu.SemaphoreType.DMA
    total = sum(chunks)
    return dict(
        x=pltpu.VMEM((2, 3 * block, width), half),
        raised=pltpu.VMEM((rows, 3 * block, width), half),
        pool_w=pltpu.VMEM((3 * width, width), half),
        up_w=pltpu.VMEM((width, 3 * width), half),
        query_w=pltpu.VMEM((width, own), half),
        key_w=pltpu.VMEM((width, own), half),
        value_w=pltpu.VMEM((width, own), half),
        outer_w=pltpu.VMEM((hidden, width), half),
        inner_w=pltpu.VMEM((width, hidden), half),
        out_w=pltpu.VMEM((width, width), half),
        rim=pltpu.VMEM((rows, 16, width), half),
        stage=pltpu.VMEM((size.lanes, 3 * block + 8, 128), full),
        groups=pltpu.VMEM((tokens, 3 * width), half),
        dy=pltpu.VMEM((tokens, 3 * width), half),
        grad_resid=pltpu.VMEM((tokens, width), full),
        grad_branch=pltpu.VMEM((tokens, width), half),
        pooled=pltpu.VMEM((tokens, width), full),
        normed=pltpu.VMEM((tokens, width), half),
        nr=pltpu.VMEM((length, width), half),
        grad_inner=pltpu.VMEM((tokens, hidden), half),
        activated=pltpu.VMEM((tokens, hidden), half),
        qt=pltpu.VMEM((heads, 128, length), half),
        kt=pltpu.VMEM((heads, 80, length), half),
        vt=pltpu.VMEM((own, length), half),
        k=pltpu.VMEM((pairs, length, 128), half),
        v=pltpu.VMEM((pairs, length, 128), half),
        work=pltpu.VMEM((2 * near, size.span, size.span), full),
        expo=pltpu.VMEM((heads, len(size.tiles), size.span, size.span), half),
        inverse=pltpu.VMEM((heads, 8, length), full),
        mixed=pltpu.VMEM((own, length), full),
        att_out=pltpu.VMEM((length, own), half),
        att=pltpu.VMEM((tokens, width), half),
        residual=pltpu.VMEM((tokens, width), full),
        normed_two=pltpu.VMEM((tokens, width), half),
        grad_att=pltpu.VMEM((tokens, width), half),
        grad_heads=pltpu.VMEM((length, own), half),
        slope_sum=pltpu.VMEM((heads, 8, size.span), full),
        pair_in=pltpu.VMEM((depth * block, width), half),
        back=pltpu.VMEM((size.chips_per_row, tokens, width), half),
        edge_out=pltpu.VMEM((rows, 8, width), full),
        edge_in=pltpu.VMEM((rows, 8, width), full),
        edge_end=pltpu.VMEM((rows, 16, width), full),
        mine=pltpu.VMEM((total, 128), half),
        landing=pltpu.VMEM((SumPieces.landing_rows(size.batch, size.seq, chunks, orders), 128), half),
        piece=pltpu.VMEM((total // (size.batch * size.seq), 128), half),
        small_block=pltpu.VMEM((len(stages) + 1, small_rows, 128), full),
        small_landing=pltpu.VMEM((sum(stages), small_rows, 128), full),
        load_sem=dma((10,)),
        x_sem=dma((2,)),
        rim_sem=dma((4,)),
        own_sem=dma((6,)),
        row_sent=dma((depth,)),
        row_got=dma((depth,)),
        across_sent=dma((depth,)),
        across_got=dma((depth,)),
        att_sent=dma((size.seq,)),
        att_got=dma((size.seq,)),
        grad_sent=dma((size.seq,)),
        grad_got=dma((size.seq,)),
        pair_sent=dma((depth,)),
        pair_got=dma((depth,)),
        back_sent=dma((depth,)),
        back_got=dma((depth,)),
        sum_sem=dma((4, len(chunks), slots)),
        keep_sem=dma((len(chunks),)),
        small_sem=dma((2, slots)),
    )


def widen_kernel(plan, steps, places, sums, shift, cotangent, small, *refs):
    outs = dict(zip(plan, refs[: len(plan)]))
    grad_inputs = refs[len(plan)]
    vectors = refs[len(plan) + 1 : len(plan) + 1 + len(places)]
    source, target, moved, kept, result, load_sem, store_sem, row_sem = refs[
        len(plan) + 1 + len(places) :
    ]
    rows = shift.shape[0]
    deep = source.shape[0]
    product_rows = source.shape[1]
    width = target.shape[1]

    def load(i):
        return pltpu.make_async_copy(
            sums.at[pl.ds(i * product_rows, product_rows), :], source.at[i % deep],
            load_sem.at[i % deep],
        )

    def store(i):
        name, part = steps[i]
        out = outs[name]
        if out.shape[0] > width:
            out = out.at[pl.ds(part * width, width), :]
        elif out.shape[1] > width:
            out = out.at[:, pl.ds(part * width, width)]
        return pltpu.make_async_copy(target.at[i % deep], out, store_sem.at[i % deep])

    def row_loads(r):
        return (
            pltpu.make_async_copy(shift.at[r], moved.at[r % 2], row_sem.at[0, r % 2]),
            pltpu.make_async_copy(cotangent.at[r], kept.at[r % 2], row_sem.at[1, r % 2]),
        )

    def row_store(r):
        return pltpu.make_async_copy(result.at[r % 2], grad_inputs.at[r], row_sem.at[2, r % 2])

    for i in range(deep - 1):
        load(i).start()
    for at, out in zip(places, vectors):
        count = out.shape[-1]
        for c in range(0, count, 128):
            part = min(128, count - c)
            if len(out.shape) == 1:
                out[c : c + part] = small[at + c // 128, :part]
            else:
                out[:, c : c + part] = small[at + c // 128 : at + c // 128 + 1, :part]
    for copy in row_loads(0):
        copy.start()
    for r in range(rows):
        if r + 1 < rows:
            for copy in row_loads(r + 1):
                copy.start()
        for copy in row_loads(r):
            copy.wait()
        if r >= 2:
            row_store(r - 2).wait()

        def add_rows(b, carry):
            at = pl.ds(pl.multiple_of(b * 64, 64), 64)
            result[r % 2, at, :] = moved[r % 2, at, :].astype(full) + kept[
                r % 2, at, :
            ].astype(full)
            return carry

        lax.fori_loop(0, result.shape[1] // 64, add_rows, 0)
        row_store(r).start()
    for i in range(len(steps)):
        if i + deep - 1 < len(steps):
            load(i + deep - 1).start()
        load(i).wait()
        if i >= deep:
            store(i - deep).wait()

        def convert(b, carry):
            at = pl.multiple_of(b * 64, 64)
            for c in range(product_rows // width):
                target[i % deep, pl.ds(at, 64), c * 128 : (c + 1) * 128] = source[
                    i % deep, pl.ds(c * width + at, 64), :
                ].astype(full)
            return carry

        lax.fori_loop(0, width // 64, convert, 0)
        store(i).start()
    for r in range(max(0, rows - 2), rows):
        row_store(r).wait()
    for i in range(max(0, len(steps) - deep), len(steps)):
        store(i).wait()


def widen(sums, shift, cotangent, small, counts, shapes, steps):
    any_space = pl.BlockSpec(memory_space=pl.ANY)
    names = tuple(shapes)
    width = shift.shape[2]
    deep = 6
    outs = [jax.ShapeDtypeStruct(shapes[name], full) for name in names]
    outs.append(jax.ShapeDtypeStruct(shift.shape, full))
    outs += [
        jax.ShapeDtypeStruct(
            (count,) if count % 1024 == 512 and count > 512 else (1, count), full
        )
        for count in counts.values()
    ]
    vmem = pl.BlockSpec(memory_space=pltpu.VMEM)
    row = shift.shape[1:]
    product_rows = sums.shape[0] // len(steps)
    results = pl.pallas_call(
        functools.partial(widen_kernel, names, steps, tuple(counts)),
        out_shape=outs,
        in_specs=[any_space] * 3 + [vmem],
        out_specs=[any_space] * (len(names) + 1) + [vmem] * len(counts),
        scratch_shapes=[
            pltpu.VMEM((deep, product_rows, 128), half),
            pltpu.VMEM((deep, width, width), full),
            pltpu.VMEM((2,) + row, half),
            pltpu.VMEM((2,) + row, half),
            pltpu.VMEM((2,) + row, full),
            pltpu.SemaphoreType.DMA((deep,)),
            pltpu.SemaphoreType.DMA((deep,)),
            pltpu.SemaphoreType.DMA((3, 2)),
        ],
        name="widen",
    )(sums, shift, cotangent, small)
    vectors = {
        at: value.reshape(-1) for at, value in zip(counts, results[len(names) + 1 :])
    }
    return dict(zip(names, results)), results[len(names)], vectors


def local(
    inputs,
    cotangent,
    doc_lengths,
    pool_weight,
    pool_bias,
    gain_one,
    shift_one,
    query_weight,
    key_weight,
    value_weight,
    out_weight,
    slopes,
    gain_two,
    shift_two,
    inner_weight,
    inner_bias,
    outer_weight,
    outer_bias,
    up_weight,
    up_bias,
):
    rows, block_len, width = inputs.shape
    hidden = inner_weight.shape[1]
    size = Sizes(
        lax.axis_size("batch"), lax.axis_size("seq"), rows, block_len // 3, width,
        hidden, slopes.shape[0],
    )
    steps = product_list(size.parts)
    product_rows = width * size.lanes
    chunks = [2 * product_rows] * (len(steps) // 2)
    if product_rows % (16 * size.batch * size.seq) == 0:
        chunks[-1:] = [product_rows] * 2
    total = len(steps) * product_rows
    vmem = pl.BlockSpec(memory_space=pltpu.VMEM)
    smem = pl.BlockSpec(memory_space=pltpu.SMEM)
    any_space = pl.BlockSpec(memory_space=pl.ANY)
    plan = scratch_plan(size, chunks)
    vectors = (
        pool_bias, gain_one, shift_one, gain_two, shift_two, inner_bias, outer_bias, up_bias,
    )
    output, shift, sums, small = pl.pallas_call(
        functools.partial(layer_kernel, size, chunks),
        out_shape=(
            jax.ShapeDtypeStruct(inputs.shape, half),
            jax.ShapeDtypeStruct(inputs.shape, half),
            jax.ShapeDtypeStruct((total, 128), half),
            jax.ShapeDtypeStruct((small_rows, 128), full),
        ),
        in_specs=[smem, smem] + [vmem] * 8 + [any_space] * 10,
        out_specs=(any_space, any_space, any_space, vmem),
        scratch_shapes=list(plan.values()),
        compiler_params=pltpu.CompilerParams(
            collective_id=0, has_side_effects=True, vmem_limit_bytes=67043328
        ),
        name="layer",
    )(
        doc_lengths, slopes, *(v.reshape(1, -1) for v in vectors[:-1]), up_bias,
        inputs, cotangent, pool_weight, query_weight, key_weight, value_weight,
        out_weight, inner_weight, outer_weight, up_weight,
    )
    shapes = {
        Product.inner: inner_weight.shape, Product.outer: outer_weight.shape, Product.up: up_weight.shape,
        Product.out: out_weight.shape, Product.query: query_weight.shape, Product.key: key_weight.shape,
        Product.value: value_weight.shape, Product.pool: pool_weight.shape,
    }
    counts = {
        Small.pool_bias: width, Small.gain_one: width, Small.shift_one: width,
        Small.slopes: slopes.shape[0], Small.gain_two: width, Small.shift_two: width,
        Small.inner_bias: hidden, Small.outer_bias: width, Small.up_bias: 3 * width,
    }
    grads, input_grad, vector = widen(sums, shift, cotangent, small, counts, shapes, steps)

    return (
        output,
        input_grad,
        grads[Product.pool],
        vector[Small.pool_bias],
        vector[Small.gain_one],
        vector[Small.shift_one],
        grads[Product.query],
        grads[Product.key],
        grads[Product.value],
        grads[Product.out],
        vector[Small.slopes],
        vector[Small.gain_two],
        vector[Small.shift_two],
        grads[Product.inner],
        vector[Small.inner_bias],
        grads[Product.outer],
        vector[Small.outer_bias],
        grads[Product.up],
        vector[Small.up_bias],
    )


def solution(mesh):
    blocks = P("batch", "seq", None)
    in_specs = (blocks, blocks, P("batch", None)) + (P(),) * 17
    out_specs = (blocks, blocks) + (P(),) * 17
    return jax.shard_map(local, mesh=mesh, in_specs=in_specs, out_specs=out_specs, check_vma=False)
```

```python
import functools
import math
from types import SimpleNamespace

import jax
import jax.numpy as jnp
from jax import lax
from jax.experimental import pallas as pl
from jax.experimental.pallas import tpu as pltpu
from jax.sharding import PartitionSpec as P

norm_eps = 1e-05
log2_e = math.log2(math.e)

MESH = pl.DeviceIdType.MESH
half = jnp.bfloat16
full = jnp.float32


class Place:
    def __init__(self, batch_size, seq_size):
        side = math.isqrt(batch_size)
        self.depth = seq_size // 2
        self.batch = lax.axis_index("batch")
        self.seq = lax.axis_index("seq")
        self.core = self.seq % 2
        self.level = self.seq // 2
        high, low = self.batch // side, self.batch % side
        self.first = jnp.where(self.core == 0, low, high)
        self.second = jnp.where(self.core == 0, high, low)
        self.side = side
        self.sizes = stage_sizes(batch_size, seq_size)
        bits = [self.level // 2**b % 2 for b in range(len(self.sizes) - 3)]
        self.where = (self.core, self.first, self.second, *bits)

    def batch_at(self, first, second):
        return jnp.where(
            self.core == 0, second * self.side + first, first * self.side + second
        )

    def partner(self, stage, step):
        member = (self.where[stage] + step) % self.sizes[stage]
        if stage == 0:
            return (self.batch, self.level * 2 + member)
        if stage == 1:
            return (self.batch_at(member, self.second), self.seq)
        if stage == 2:
            return (self.batch_at(self.first, member), self.seq)
        other = self.level + (member - self.where[stage]) * 2 ** (stage - 3)
        return (self.batch, other * 2 + self.core)


def stage_sizes(batch_size, seq_size):
    side = math.isqrt(batch_size)
    bits = (seq_size // 2).bit_length() - 1
    return (2, side, side) + (2,) * bits


def sum_slots(batch_size, seq_size):
    return sum(size - 1 for size in stage_sizes(batch_size, seq_size))


class SumPieces:
    def __init__(self, place, chunks, orders, mine, landing, piece, out, sems, keep):
        self.place, self.chunks, self.orders = place, chunks, orders
        self.mine, self.landing, self.piece, self.out = mine, landing, piece, out
        self.keep = keep
        self.sent, self.got, self.back_sent, self.back_got = sems
        self.starts = [sum(chunks[:c]) for c in range(len(chunks))]
        sizes = place.sizes
        self.last = len(sizes) - 1
        self.events = 2 * len(sizes) + 1
        self.land = {}
        at = 0
        for c in range(len(chunks)):
            for stage in range(len(sizes)):
                for step in self.steps(c, stage):
                    self.land[c, stage, step] = at
                    at += self.rows(c, stage)

    @staticmethod
    def landing_rows(batch_size, seq_size, chunks, orders):
        sizes, rows = stage_sizes(batch_size, seq_size), 0
        for left, order in zip(chunks, orders):
            for axis in order:
                left //= sizes[axis]
                rows += left * (sizes[axis] - 1)
        return rows

    def size_at(self, c, stage):
        return self.place.sizes[self.orders[c][stage]]

    def where_at(self, c, stage):
        return self.place.where[self.orders[c][stage]]

    def slot(self, c, stage):
        return sum(self.size_at(c, t) - 1 for t in range(stage))

    def rows(self, c, stage):
        count = self.chunks[c]
        for t in range(stage + 1):
            count //= self.size_at(c, t)
        return count

    def begin(self, c, stage):
        at = self.starts[c]
        for t in range(stage):
            at = at + self.where_at(c, t) * self.rows(c, t)
        return at

    def scatter(self, c, stage, step):
        count = self.rows(c, stage)
        member = (self.where_at(c, stage) + step) % self.size_at(c, stage)
        at = pl.multiple_of(self.begin(c, stage) + member * count, 16)
        slot = self.slot(c, stage) + step - 1
        return pltpu.make_async_remote_copy(
            src_ref=self.mine.at[pl.ds(at, count), :],
            dst_ref=self.landing.at[pl.ds(self.land[c, stage, step], count), :],
            send_sem=self.sent.at[c, slot],
            recv_sem=self.got.at[c, slot],
            device_id=self.place.partner(self.orders[c][stage], step),
            device_id_type=MESH,
        )

    def piece_span(self, c):
        count = self.rows(c, self.last)
        return pl.ds(self.starts[c] * count // self.chunks[c], count)

    def keep_copy(self, c):
        at = pl.multiple_of(self.begin(c, self.last + 1), 16)
        return pltpu.make_async_copy(
            self.piece.at[self.piece_span(c), :],
            self.out.at[pl.ds(at, self.rows(c, self.last)), :],
            self.keep.at[c],
        )

    def gather(self, c, stage, step):
        count = self.rows(c, stage)
        at = pl.multiple_of(self.begin(c, stage + 1), 16)
        slot = self.slot(c, stage) + step - 1
        source = self.out.at[pl.ds(at, count), :]
        if stage == self.last:
            source = self.piece.at[self.piece_span(c), :]
        return pltpu.make_async_remote_copy(
            src_ref=source,
            dst_ref=self.out.at[pl.ds(at, count), :],
            send_sem=self.back_sent.at[c, slot],
            recv_sem=self.back_got.at[c, slot],
            device_id=self.place.partner(self.orders[c][stage], step),
            device_id_type=MESH,
        )

    def add(self, c, stage):
        count = self.rows(c, stage)
        at = self.begin(c, stage + 1)
        part = min(count, 512)

        def body(i, carry):
            here = pl.ds(pl.multiple_of(at + i * part, 16), part)
            if self.size_at(c, stage) == 2:
                there = pl.multiple_of(self.land[c, stage, 1] + i * part, 16)
                total = self.mine[here, :] + self.landing[pl.ds(there, part), :]
            else:
                total = self.mine[here, :].astype(full)
                for step in self.steps(c, stage):
                    there = pl.multiple_of(self.land[c, stage, step] + i * part, 16)
                    total = total + self.landing[pl.ds(there, part), :].astype(full)
                total = total.astype(half)
            if stage == self.last:
                first = self.piece_span(c).start
                self.piece[pl.ds(pl.multiple_of(first + i * part, 16), part), :] = total
            else:
                self.mine[here, :] = total
            return carry

        lax.fori_loop(0, count // part, body, 0)

    def steps(self, c, stage):
        return range(1, self.size_at(c, stage))

    def advance(self, c, event):
        count = self.last + 1
        if 1 <= event <= count:
            for step in self.steps(c, event - 1):
                self.scatter(c, event - 1, step).wait_recv()
            self.add(c, event - 1)
        if event < count:
            for step in self.steps(c, event):
                self.scatter(c, event, step).start()
            return
        stage = 2 * count - 1 - event
        if event == count:
            self.keep_copy(c).start()
        else:
            for step in self.steps(c, stage + 1):
                self.gather(c, stage + 1, step).wait_recv()
        if event == count + 1:
            self.keep_copy(c).wait()
        if stage >= 0:
            for step in self.steps(c, stage):
                self.gather(c, stage, step).start()

    def finish(self):
        for c in range(len(self.chunks)):
            for stage in range(self.last + 1):
                for step in self.steps(c, stage):
                    self.scatter(c, stage, step).wait_send()
                    self.gather(c, stage, step).wait_send()


class SumSmall:
    def __init__(self, place, block, landing, sems):
        self.place, self.block, self.landing = place, block, landing
        self.sent, self.got = sems
        sizes = place.sizes
        self.slot = [sum(s - 1 for s in sizes[:stage]) for stage in range(len(sizes))]
        self.base = [sum(sizes[:stage]) for stage in range(len(sizes))]

    def copy(self, stage, step):
        slot = self.slot[stage] + step - 1
        return pltpu.make_async_remote_copy(
            src_ref=self.block.at[stage],
            dst_ref=self.landing.at[self.base[stage] + self.place.where[stage]],
            send_sem=self.sent.at[slot],
            recv_sem=self.got.at[slot],
            device_id=self.place.partner(stage, step),
            device_id_type=MESH,
        )

    def send(self, stage):
        self.landing[self.base[stage] + self.place.where[stage]] = self.block[stage]
        for step in range(1, self.place.sizes[stage]):
            self.copy(stage, step).start()

    def receive(self, stage):
        for step in range(1, self.place.sizes[stage]):
            self.copy(stage, step).wait_recv()
        total = self.landing[self.base[stage]]
        for member in range(1, self.place.sizes[stage]):
            total = total + self.landing[self.base[stage] + member]
        self.block[stage + 1] = total

    def finish(self):
        for stage in range(len(self.place.sizes)):
            for step in range(1, self.place.sizes[stage]):
                self.copy(stage, step).wait_send()


def dot_nn(left, right):
    return lax.dot_general(
        left, right, (((1,), (0,)), ((), ())), preferred_element_type=full
    )


def dot_nt(left, right):
    return lax.dot_general(
        left, right, (((1,), (1,)), ((), ())), preferred_element_type=full
    )


def dot_tn(left, right):
    return lax.dot_general(
        left, right, (((0,), (0,)), ((), ())), preferred_element_type=full
    )


def centred_rows(values_in):
    centre = values_in - jnp.mean(values_in, axis=-1, keepdims=True)
    spread = jnp.mean(centre * centre, axis=-1, keepdims=True)
    inverse = lax.rsqrt(spread + norm_eps)
    return centre * inverse, inverse


def norm_back(grad_normed, scaled, inverse, gain):
    inner = grad_normed * gain
    first = jnp.mean(inner, axis=-1, keepdims=True)
    second = jnp.mean(inner * scaled, axis=-1, keepdims=True)
    return inverse * (inner - first - scaled * second)


class Sizes:
    def __init__(self, batch_size, seq_size, rows, block, width, hidden, heads):
        self.batch, self.seq = batch_size, seq_size
        self.rows, self.block, self.width, self.hidden = rows, block, width, hidden
        self.heads = heads
        self.tokens = rows * block
        self.length = seq_size * block
        self.depth = seq_size // 2
        self.per_row = seq_size // rows
        self.chips_per_row = self.per_row // 2
        self.own_width = width // self.per_row
        self.own_heads = heads // self.per_row
        self.pairs = self.own_heads // 2
        self.head_dim = width // heads
        self.span = 2 * block
        self.query_blocks = self.length // self.span
        self.reach = self.query_blocks // 2
        self.tiles = []
        for i in range(self.query_blocks):
            for j in range(max(0, i - self.reach), i + 1):
                self.tiles.append((i, j))
        self.lanes = width // 128
        self.parts = hidden // width


def product_list(parts):
    order = []
    for j in range(parts):
        order += [(Product.inner, j), (Product.outer, j)]
    order += [(Product.up, 0), (Product.up, 1), (Product.up, 2), (Product.out, 0)]
    order += [(Product.query, 0), (Product.key, 0), (Product.value, 0)]
    order += [(Product.pool, 0), (Product.pool, 1), (Product.pool, 2)]
    return order


class Product:
    inner, outer, up, out, query, key, value, pool = range(8)


class Small:
    pool_bias, gain_one, shift_one, slopes = 0, 4, 8, 12
    gain_two, shift_two, inner_bias, outer_bias, up_bias = 13, 17, 21, 37, 41


class Site:
    feed, norm_two, second, up, out, rise, heads, back, settle = range(9)
    pair, give, weights, rows, norm_one, pool = range(9, 15)


small_rows = 56


pace = {
    (Site.feed, 0): (0,),
    (Site.feed, 1): (1,),
    (Site.feed, 2): (0, 2,),
    (Site.feed, 3): (1, 3,),
    (Site.norm_two, 0): (2,),
    (Site.norm_two, 1): (0,),
    (Site.norm_two, 2): (3,),
    (Site.second, 0): (1,),
    (Site.up, 1): (4,),
    (Site.up, 2): (2,),
    (Site.out, 0): (5,),
    (Site.rise, 0): (0,),
    (Site.rise, 3): (4,),
    (Site.heads, 0): (3, 5, 1, 2, 0,),
    (Site.back, 3): (1,),
    (Site.back, 4): (4, 2, 3, 0,),
    (Site.back, 6): (1, 5,),
    (Site.back, 7): (2, 4, 3,),
    (Site.settle, 0): (0,),
    (Site.pair, 0): (1, 5,),
    (Site.pair, 3): (2,),
    (Site.give, 0): (4,),
    (Site.give, 2): (3, 0,),
    (Site.weights, 0): (1,),
    (Site.weights, 1): (6,),
    (Site.weights, 2): (5,),
    (Site.rows, 0): (2, 0, 1, 6, 2, 0,),
    (Site.norm_one, 1): (0,),
    (Site.norm_one, 2): (1,),
    (Site.pool, 0): (7,),
    (Site.pool, 1): (6, 8,),
    (Site.pool, 2): (4, 1, 3, 9,),
}
finish_order = (
    5, 7, 2, 8, 6, 9, 4, 2, 3, 5, 7, 6, 8, 4, 9, 5,
    3, 6, 7, 8, 6, 4, 7, 9, 8, 5, 6, 9, 7, 3, 8, 9,
    3, 7, 8, 4, 9, 4, 7, 8, 5, 9, 6, 5, 7, 8, 9, 6,
    6, 7, 8, 7, 8, 9, 9,
)
level_first = ()


def axis_orders(size, count):
    axes = tuple(range(len(stage_sizes(size.batch, size.seq))))
    return [
        axes[:2] + axes[3:] + axes[2:3] if c in level_first else axes for c in range(count)
    ]


def layer_kernel(size, chunks, docs, slopes, pool_bias, gain_one, shift_one,
                 gain_two, shift_two, inner_bias, outer_bias, up_bias,
                 inputs_hbm, cotangent_hbm, pool_hbm, query_hbm, key_hbm, value_hbm,
                 out_hbm, inner_hbm, outer_hbm, up_hbm,
                 output_hbm, shift_hbm, sums_hbm, small_out,
                 *scratch_refs):
    s = SimpleNamespace(**dict(zip(scratch_plan(size, chunks), scratch_refs)))
    place = Place(size.batch, size.seq)
    me, core, level = place.seq, place.core, place.level
    rows, block, width, hidden = size.rows, size.block, size.width, size.hidden
    tokens, length, depth = size.tokens, size.length, size.depth
    per_row, chips = size.per_row, size.chips_per_row
    own_width, pairs = size.own_width, size.pairs
    my_row, my_group = me // per_row, me % per_row
    lanes, parts, span = size.lanes, size.parts, size.span
    products = product_list(parts)
    product_rows = width * lanes

    def tile_at(name, part, lane):
        return products.index((name, part)) * product_rows + lane * width

    barrier = pltpu.get_barrier_semaphore()
    greeted = [(place.batch, (me + k) % size.seq) for k in range(1, size.seq)]
    for stage in (1, 2):
        greeted += [place.partner(stage, k) for k in range(1, place.sizes[stage])]
    for device in greeted:
        pl.semaphore_signal(barrier, inc=1, device_id=device, device_id_type=MESH)

    loads = SimpleNamespace()

    def load(source, target):
        copy = pltpu.make_async_copy(source, target, s.load_sem.at[len(vars(loads))])
        copy.start()
        return copy

    first_column = pl.multiple_of(my_group * own_width, own_width)

    def x_load(step):
        return pltpu.make_async_copy(
            inputs_hbm.at[(my_row + 1 + step) % rows], s.x.at[step % 2],
            s.x_sem.at[step % 2],
        )

    x_load(0).start()
    loads.dy = load(cotangent_hbm, s.raised)
    loads.up = load(up_hbm, s.up_w)
    loads.pool = load(pool_hbm, s.pool_w)
    loads.outer = load(outer_hbm, s.outer_w)
    loads.query = load(query_hbm.at[:, pl.ds(first_column, own_width)], s.query_w)
    loads.key = load(key_hbm.at[:, pl.ds(first_column, own_width)], s.key_w)
    loads.value = load(value_hbm.at[:, pl.ds(first_column, own_width)], s.value_w)
    loads.out = load(out_hbm, s.out_w)
    loads.inner = load(inner_hbm, s.inner_w)

    def remote(source, target, sent, got, device):
        return pltpu.make_async_remote_copy(
            src_ref=source, dst_ref=target, send_sem=sent, recv_sem=got,
            device_id=device, device_id_type=MESH,
        )

    small_block = s.small_block
    small_block[0] = jnp.zeros((small_rows, 128), full)

    def put_small(name, at, values):
        for c in range(values.shape[1] // 128):
            small_block[0, pl.ds(name + at // 128 + c, 1), :] = values[
                :, c * 128 : (c + 1) * 128
            ]

    stage = s.stage

    def spread_rows(at, values):
        for c in range(lanes):
            stage[c, pl.ds(at, values.shape[0]), :] = values[:, c * 128 : (c + 1) * 128]

    def every_third(at):
        return jnp.concatenate(
            [stage[c, pl.ds(at, block, stride=3), :] for c in range(lanes)], axis=1
        )

    def put_third(at, values):
        for c in range(lanes):
            stage[c, pl.ds(at, block, stride=3), :] = values[:, c * 128 : (c + 1) * 128]

    def row_span(r):
        return pl.ds(pl.multiple_of(r * block, block), block)

    loads.dy.wait()
    loads.up.wait()
    up_sum = jnp.zeros((1, width), full)

    def split_cotangent(r, carry):
        spread_rows(8, s.raised[r].astype(full))
        totals = []
        grad = jnp.zeros((block, width), full)
        for k in range(3):
            part = every_third(8 + k)
            totals.append(carry[k] + jnp.sum(part, axis=0, keepdims=True))
            low = part.astype(half)
            s.dy[row_span(r), k * width : (k + 1) * width] = low
            grad = grad + dot_nt(low, s.up_w[:, k * width : (k + 1) * width])
        s.grad_resid[row_span(r), :] = grad
        low = grad.astype(half)
        s.grad_branch[row_span(r), :] = low
        totals.append(carry[3] + jnp.sum(low.astype(full), axis=0, keepdims=True))
        return tuple(totals)

    sums = lax.fori_loop(0, rows, split_cotangent, (up_sum,) * 4)
    loads.x = load(inputs_hbm, s.raised)
    for k in range(3):
        put_small(Small.up_bias, k * width, sums[k])
    put_small(Small.outer_bias, 0, sums[3])

    pl.semaphore_wait(barrier, len(greeted))
    rim_copy = remote(
        inputs_hbm.at[:, pl.ds(3 * block - 16, 16), :], s.rim,
        s.rim_sem.at[0], s.rim_sem.at[1], (place.batch, (me + 1) % size.seq),
    )

    @pl.when(me < size.seq - 1)
    def _():
        rim_copy.start()

    loads.outer.wait()

    def before_activation(j, carry):
        at = pl.ds(pl.multiple_of(j * width, width), width)
        grad = dot_nt(s.grad_branch[...], s.outer_w[at, :])
        s.grad_inner[:, at] = grad.astype(half)
        return carry

    lax.fori_loop(0, parts, before_activation, 0)

    @pl.when(me > 0)
    def _():
        rim_copy.wait_recv()

    loads.pool.wait()
    nr = s.nr

    def nr_rows(owner):
        return pl.ds(pl.multiple_of(owner * block, block), block)

    def row_copy(r, target_level):
        return remote(
            s.normed.at[row_span(r), :], nr.at[nr_rows(me), :],
            s.row_sent.at[target_level], s.row_got.at[level],
            (place.batch, target_level * 2 + core),
        )

    def row_from(source_level):
        return remote(
            s.normed.at[row_span(0), :], nr.at[nr_rows(source_level * 2 + core), :],
            s.row_sent.at[source_level], s.row_got.at[source_level],
            (place.batch, source_level * 2 + core),
        )

    for step in range(rows):
        r = (my_row + 1 + step) % rows
        rim_rows = s.rim[r].astype(full)[8:16, :]
        rim_rows = jnp.where(me > 0, rim_rows, 0.0)
        spread_rows(0, rim_rows)
        x_load(step).wait()
        if step + 1 < rows:
            x_load(step + 1).start()
        spread_rows(8, s.x[step % 2].astype(full))
        pooled = jnp.zeros((block, width), full) + pool_bias[...]
        for k in range(3):
            part = every_third(6 + k).astype(half)
            s.groups[row_span(r), k * width : (k + 1) * width] = part
            pooled = pooled + dot_nn(part, s.pool_w[k * width : (k + 1) * width, :])
        s.pooled[row_span(r), :] = pooled
        scaled, _ = centred_rows(pooled)
        s.normed[row_span(r), :] = (scaled * gain_one[...] + shift_one[...]).astype(half)
        if step < rows - 1:
            for i in range(chips):
                row_copy(r, r * chips + i).start()
        else:
            for i in range(1, chips):
                row_copy(r, r * chips + (level % chips + i) % chips).start()
            own_copy = pltpu.make_async_copy(
                s.normed.at[row_span(r), :], nr.at[nr_rows(me), :], s.own_sem.at[0]
            )
            own_copy.start()

    def across(source_level, owner_core):
        owner = source_level * 2 + owner_core
        return remote(
            nr.at[nr_rows(owner), :], nr.at[nr_rows(owner), :],
            s.across_sent.at[source_level], s.across_got.at[source_level],
            (place.batch, level * 2 + 1 - core),
        )

    loads.query.wait()
    loads.key.wait()
    loads.value.wait()

    def project(owner):
        at = nr_rows(owner)
        source = nr[at, :]
        q = dot_nn(source, s.query_w[...])
        k = dot_nn(source, s.key_w[...])
        v = dot_nn(source, s.value_w[...])
        qt, kt, vt = q.T, k.T, v.T
        s.vt[:, at] = vt.astype(half)
        zeros = jnp.zeros((64, block), half)
        line = lax.broadcasted_iota(jnp.int32, (16, block), 0)
        key_at = owner * block + lax.broadcasted_iota(jnp.int32, (16, block), 1)
        fine = (key_at % 128).astype(full)
        coarse = (key_at - key_at % 128).astype(full)
        extra = jnp.where(line == 0, 1.0, jnp.where(line == 1, fine, coarse))
        extra = jnp.where(line < 3, extra, 0.0).astype(half)
        for p in range(pairs):
            s.k[p, at, :] = k[:, p * 128 : (p + 1) * 128].astype(half)
            s.v[p, at, :] = v[:, p * 128 : (p + 1) * 128].astype(half)
            for side in range(2):
                h = 2 * p + side
                piece = qt[h * 64 : (h + 1) * 64, :].astype(half)
                s.qt[h, :, at] = jnp.concatenate(
                    [piece, zeros] if side == 0 else [zeros, piece], axis=0
                )
                piece = kt[h * 64 : (h + 1) * 64, :].astype(half)
                s.kt[h, :, at] = jnp.concatenate([piece, extra], axis=0)

    order = [0]
    for k in range(1, depth):
        order.append((k + 1) // 2 if k % 2 else depth - k // 2)
    for k in order:
        source_level = (level + k) % depth
        if k == 0:
            own_copy.wait()
        else:
            row_from(source_level).wait_recv()
        across(source_level, core).start()
    for k in order:
        source_level = (level + k) % depth
        project(source_level * 2 + core)
        across(source_level, 1 - core).wait_recv()
        project(source_level * 2 + 1 - core)

    ends = []
    total = 0
    for d in range(docs.shape[1]):
        total = total + docs[my_row, d]
        ends.append(total)
    key_line = lax.broadcasted_iota(jnp.int32, (span, span), 0)
    query_line = lax.broadcasted_iota(jnp.int32, (span, span), 1)
    scale_two = size.head_dim ** -0.5 * log2_e

    def tile_of(i, j):
        return size.tiles.index((i, j))

    def near(i):
        return range(max(0, i - size.reach), i + 1)

    def att_copy(owner, at_row, at_group, slot):
        return remote(
            s.att_out.at[nr_rows(owner), :],
            s.att.at[row_span(at_row), pl.ds(pl.multiple_of(at_group * own_width, own_width), own_width)],
            s.att_sent.at[owner], s.att_got.at[slot], (place.batch, owner),
        )

    def head_slope(h):
        return slopes[my_group * size.own_heads + h]

    turns = [
        t // 2 if t % 2 == 0 else size.query_blocks - 1 - t // 2
        for t in range(size.query_blocks)
    ]
    for i in turns:
        cols = slice(i * span, (i + 1) * span)
        place_q = 3 * (i * span + lax.broadcasted_iota(jnp.int32, (1, span), 1))
        start = jnp.zeros((1, span), jnp.int32)
        for end in ends:
            start = jnp.where(end <= place_q, jnp.maximum(start, end), start)
        for w, j in enumerate(near(i)):
            allowed = 3 * (j * span + key_line) >= start
            if j == i:
                allowed = allowed & (key_line <= query_line)
            s.work[size.reach + 1 + w] = jnp.where(allowed, 0.0, -1e30)

        def forward_pair(p, carry):
            for side in range(2):
                h = 2 * p + side
                slope_two = head_slope(h) * log2_e
                top = None
                for w, j in enumerate(near(i)):
                    score = dot_nn(s.k[p, j * span : (j + 1) * span, :], s.qt[h, :, cols])
                    away = (key_line + (j - i) * span).astype(full)
                    score = score * scale_two + (away * slope_two + s.work[size.reach + 1 + w])
                    s.work[w] = score
                    best = jnp.max(score, axis=0, keepdims=True)
                    top = best if top is None else jnp.maximum(top, best)
                total = jnp.zeros((1, span), full)
                mixed = jnp.zeros((64, span), full)
                for w, j in enumerate(near(i)):
                    expo = jnp.exp2(s.work[w] - top)
                    total = total + jnp.sum(expo, axis=0, keepdims=True)
                    low = expo.astype(half)
                    s.expo[h, tile_of(i, j)] = low
                    at = pl.multiple_of(h * 64, 64)
                    mixed = mixed + dot_nn(
                        s.vt[pl.ds(at, 64), j * span : (j + 1) * span], low
                    )
                inverse = 1.0 / total
                s.inverse[h, :, cols] = jnp.broadcast_to(inverse, (8, span))
                s.mixed[pl.ds(pl.multiple_of(h * 64, 64), 64), cols] = mixed * inverse
            return carry

        lax.fori_loop(0, pairs, forward_pair, 0)
        s.att_out[cols, :] = s.mixed[:, cols].T.astype(half)
        for owner in (2 * i, 2 * i + 1):

            @pl.when(me == owner)
            def _():
                copy = pltpu.make_async_copy(
                    s.att_out.at[nr_rows(owner), :],
                    s.att.at[row_span(my_row), pl.ds(first_column, own_width)],
                    s.own_sem.at[1],
                )
                copy.start()

            @pl.when(me != owner)
            def _():
                att_copy(owner, my_row, my_group, me).start()

    loads.out.wait()
    loads.inner.wait()
    pltpu.make_async_copy(
        s.att_out.at[nr_rows(0), :],
        s.att.at[row_span(my_row), pl.ds(first_column, own_width)],
        s.own_sem.at[1],
    ).wait()
    for k in range(1, size.seq):
        source = (me + k) % size.seq
        att_copy(source, source // per_row, source % per_row, source).wait_recv()

    def second_norm(r, carry):
        at = row_span(r)
        residual = s.pooled[at, :] + dot_nn(s.att[at, :], s.out_w[...])
        s.residual[at, :] = residual
        scaled, _ = centred_rows(residual)
        s.normed_two[at, :] = (scaled * gain_two[...] + shift_two[...]).astype(half)
        return carry

    lax.fori_loop(0, rows, second_norm, 0)

    big = SumPieces(place, chunks, axis_orders(size, len(chunks)), s.mine, s.landing, s.piece, sums_hbm,
                    [s.sum_sem.at[k] for k in range(4)], s.keep_sem)
    reached = [0] * len(chunks)
    visits = {}
    split = len(chunks) * 2 * product_rows > sum(chunks)
    chunk_of = {name: name for name in range(len(chunks))}
    if not split:
        del chunk_of[len(chunks) - 1]
        chunk_of[len(chunks)] = len(chunks) - 1

    def sum_step(c):
        big.advance(c, reached[c])
        reached[c] += 1

    def ticks(where):
        visit = visits.get(where, 0)
        visits[where] = visit + 1
        for name in pace.get((where, visit), ()):
            if name in chunk_of:
                sum_step(chunk_of[name])

    def put_product(at, value):
        for c in range(value.shape[1] // 128):
            s.mine[pl.ds(at + c * width, width), :] = value[
                :, c * 128 : (c + 1) * 128
            ].astype(half)

    for j in range(parts):
        at = slice(j * width, (j + 1) * width)

        def feed(r, carry):
            here = row_span(r)
            value = dot_nn(s.normed_two[here, :], s.inner_w[:, at]) + inner_bias[:, at]
            share = 0.5 + 0.5 * lax.erf(value * (0.5 ** 0.5))
            density = jnp.exp(-0.5 * value * value) * (0.5 / math.pi) ** 0.5
            s.activated[here, at] = (value * share).astype(half)
            grad = s.grad_inner[here, at].astype(full) * (share + value * density)
            low = grad.astype(half)
            s.grad_inner[here, at] = low
            return carry + jnp.sum(low.astype(full), axis=0, keepdims=True)

        total = lax.fori_loop(0, rows, feed, jnp.zeros((1, width), full))
        put_small(Small.inner_bias, j * width, total)
        put_product(tile_at(Product.inner, j, 0), dot_tn(s.normed_two[...], s.grad_inner[:, at]))
        put_product(tile_at(Product.outer, j, 0), dot_tn(s.activated[:, at], s.grad_branch[...]))
        ticks(Site.feed)

    def grad_copy(owner, slot):
        row, group = owner // per_row, owner % per_row
        column = pl.ds(pl.multiple_of(group * own_width, own_width), own_width)
        return remote(
            s.grad_att.at[row_span(row), column], s.grad_heads.at[nr_rows(slot), :],
            s.grad_sent.at[owner], s.grad_got.at[slot], (place.batch, owner),
        )

    gain_sum = jnp.zeros((1, width), full)
    shift_sum = jnp.zeros((1, width), full)
    for step in range(rows):
        r = (my_row + 1 + step) % rows
        at = row_span(r)
        grad = dot_nt(s.grad_inner[at, :], s.inner_w[...])
        scaled, inverse = centred_rows(s.residual[at, :])
        gain_sum = gain_sum + jnp.sum(grad * scaled, axis=0, keepdims=True)
        shift_sum = shift_sum + jnp.sum(grad, axis=0, keepdims=True)
        mixed = s.grad_resid[at, :] + norm_back(grad, scaled, inverse, gain_two[...])
        s.grad_resid[at, :] = mixed
        s.grad_att[at, :] = dot_nt(mixed.astype(half), s.out_w[...]).astype(half)
        for g in range(per_row):
            owner = r * per_row + g
            if step < rows - 1:
                grad_copy(owner, me).start()
            else:

                @pl.when(owner != me)
                def _():
                    grad_copy(owner, me).start()

                @pl.when(owner == me)
                def _():
                    pltpu.make_async_copy(
                        s.grad_att.at[row_span(my_row), pl.ds(first_column, own_width)],
                        s.grad_heads.at[nr_rows(me), :], s.own_sem.at[2],
                    ).start()
        ticks(Site.norm_two)
    put_small(Small.gain_two, 0, gain_sum)
    put_small(Small.shift_two, 0, shift_sum)

    def second_residual(r, carry):
        at = row_span(r)
        value = s.residual[at, :] + dot_nn(s.activated[at, :], s.outer_w[...])
        s.normed_two[at, :] = (value + outer_bias[...]).astype(half)
        return carry

    for r in range(rows):
        second_residual(r, 0)
        ticks(Site.second)
    for k in range(3):
        at = slice(k * width, (k + 1) * width)
        put_product(tile_at(Product.up, k, 0), dot_tn(s.normed_two[...], s.dy[:, at]))
        ticks(Site.up)
    put_product(tile_at(Product.out, 0, 0), dot_tn(s.att[...], s.grad_resid[...].astype(half)))
    ticks(Site.out)

    up_row = jnp.concatenate(
        [up_bias[c : c + 128].reshape(1, 128) for c in range(0, 3 * width, 128)], axis=1
    )

    def raise_row(r, carry):
        for k in range(3):
            at = slice(k * width, (k + 1) * width)
            raised = dot_nn(s.normed_two[row_span(r), :], s.up_w[:, at])
            put_third(8 + k, raised + up_row[:, at])
        whole = jnp.concatenate([stage[c, 8 : 8 + 3 * block, :] for c in range(lanes)], axis=1)
        s.raised[r] = (s.raised[r].astype(full) + whole).astype(half)
        return carry

    loads.x.wait()
    for r in range(rows):
        raise_row(r, 0)
        ticks(Site.rise)
    output_copy = pltpu.make_async_copy(s.raised, output_hbm, s.own_sem.at[3])
    output_copy.start()

    blank = jnp.zeros((width, 128), half)
    for name in (Product.query, Product.key, Product.value):
        for c in range(lanes):
            s.mine[pl.ds(tile_at(name, 0, c), width), :] = blank

    pltpu.make_async_copy(
        s.grad_att.at[row_span(my_row), pl.ds(first_column, own_width)],
        s.grad_heads.at[nr_rows(me), :], s.own_sem.at[2],
    ).wait()
    ticks(Site.heads)
    for k in range(1, size.seq):
        grad_copy((me + k) % size.seq, (me + k) % size.seq).wait_recv()

    half_blocks = size.query_blocks // 2

    def value_tile(p, j):
        lane = pl.multiple_of((p * half_blocks + j // 2) * 128, 128)
        return s.residual.at[(j % 2) * span : (j % 2 + 1) * span, pl.ds(lane, 128)]

    def value_block(p, b):
        lane = pl.multiple_of((p * half_blocks + b // 4) * 128, 128)
        return s.residual.at[row_span(b % 4), pl.ds(lane, 128)]

    def key_tile(p, j):
        at = p * half_blocks + j // 2
        return s.work.at[at, :, (j % 2) * 128 : (j % 2 + 1) * 128]

    def key_block(p, b):
        lane = pl.multiple_of(b // 2 % 2 * 128, 128)
        return s.work.at[p * half_blocks + b // 4, row_span(b % 2), pl.ds(lane, 128)]

    turned = s.work.at[2 * size.reach + 1, 0:own_width, :]

    for i in range(size.query_blocks):
        cols = slice(i * span, (i + 1) * span)
        turned[...] = s.grad_heads[cols, :].astype(full).T
        query_at = (i * span + lax.broadcasted_iota(jnp.int32, (1, span), 1)).astype(full)

        def backward_pair(p, carry):
            for side in range(2):
                h = 2 * p + side
                head = pl.ds(pl.multiple_of(h * 64, 64), 64)
                inverse = s.inverse[h, 0:1, cols]
                grad = turned[head, :] * inverse
                term = jnp.sum(grad * s.mixed[head, cols], axis=0, keepdims=True)
                low = grad.astype(half)
                zeros = jnp.zeros((64, span), half)
                low = jnp.concatenate([low, zeros] if side == 0 else [zeros, low], axis=0)
                query_grad = jnp.zeros((80, span), full)
                for j in near(i):
                    keys = slice(j * span, (j + 1) * span)
                    expo = s.expo[h, tile_of(i, j)]
                    grad_probs = dot_nn(s.v[p, keys, :], low)
                    grad_scores = (expo.astype(full) * (grad_probs - term)).astype(half)
                    to_value = dot_nt(expo, low)
                    to_key = dot_nt(grad_scores, s.qt[h, :, cols])
                    if j == i and side == 0:
                        value_tile(p, j)[...] = to_value
                        key_tile(p, j)[...] = to_key
                    else:
                        value_tile(p, j)[...] += to_value
                        key_tile(p, j)[...] += to_key
                    query_grad = query_grad + dot_nn(s.kt[h, :, keys], grad_scores)
                s.mixed[head, cols] = query_grad[:64, :]
                slope = (
                    query_grad[65:66, :] + query_grad[66:67, :] - query_at * query_grad[64:65, :]
                )
                slope = jnp.broadcast_to(slope, (8, span))
                if i == 0:
                    s.slope_sum[h] = slope
                else:
                    s.slope_sum[h] += slope
            return carry

        for p in range(pairs):
            backward_pair(p, 0)
            ticks(Site.back)

    head_lane = lax.broadcasted_iota(jnp.int32, (1, 128), 1)
    slope_row = jnp.zeros((1, 128), full)
    for h in range(size.own_heads):
        total = jnp.sum(s.slope_sum[h][0:1, :], axis=1, keepdims=True)
        slope_row = slope_row + jnp.where(head_lane == my_group * size.own_heads + h, total, 0.0)
    small_block[0, pl.ds(Small.slopes, 1), :] = slope_row

    scale = size.head_dim ** -0.5

    fit = width // own_width

    def grads_at(which, at=None):
        down = which // fit * length
        if at is None:
            at = pl.ds(down, length)
        else:
            at = pl.ds(pl.multiple_of(at + down, block), block)
        return s.outer_w.at[at, which % fit * own_width : (which % fit + 1) * own_width]

    def settle(b, carry):
        at = nr_rows(b)
        for which in range(3):
            target = grads_at(which, b * block)
            if which == 0:
                target[...] = (s.mixed[:, at].T * scale).astype(half)
                continue
            for p in range(pairs):
                lane = slice(p * 128, (p + 1) * 128)
                if which == 1:
                    target[:, lane] = (key_block(p, b)[...] * scale).astype(half)
                else:
                    target[:, lane] = value_block(p, b)[...].astype(half)
        return carry

    lax.fori_loop(0, size.seq, settle, 0)
    ticks(Site.settle)

    def normed_grad(owner):
        return (
            dot_nt(grads_at(0, owner * block)[...], s.query_w[...])
            + dot_nt(grads_at(1, owner * block)[...], s.key_w[...])
            + dot_nt(grads_at(2, owner * block)[...], s.value_w[...])
        )

    def held(first, owner_level):
        across_at = (first + owner_level // rows) * width
        return s.activated.at[
            row_span(owner_level % rows), pl.ds(pl.multiple_of(across_at, width), width)
        ]

    held_parts = -(-depth // rows)

    def pair_copy(owner_level):
        return remote(
            held(0, owner_level), s.pair_in.at[row_span(owner_level), :],
            s.pair_sent.at[owner_level], s.pair_got.at[owner_level],
            (place.batch, level * 2 + 1 - core),
        )

    def back_copy(owner_level, source_level):
        row, part = source_level // chips, source_level % chips
        return remote(
            held(held_parts, owner_level),
            s.back.at[part, row_span(row), :],
            s.back_sent.at[owner_level], s.back_got.at[source_level],
            (place.batch, owner_level * 2 + core),
        )

    for k in range(depth):
        owner_level = (level + 1 + k) % depth
        held(0, owner_level)[...] = normed_grad(owner_level * 2 + 1 - core).astype(half)
        pair_copy(owner_level).start()
        ticks(Site.pair)
    for k in range(depth):
        owner_level = (level + 1 + k) % depth
        grad = normed_grad(owner_level * 2 + core)
        pair_copy(owner_level).wait_recv()
        grad = grad + s.pair_in[row_span(owner_level), :].astype(full)
        held(held_parts, owner_level)[...] = grad.astype(half)
        if k < depth - 1:
            back_copy(owner_level, level).start()
        else:
            back_own = pltpu.make_async_copy(
                held(held_parts, level),
                s.back.at[level % chips, row_span(level // chips), :],
                s.own_sem.at[4],
            )
            back_own.start()
        ticks(Site.give)

    for which, name in enumerate((Product.query, Product.key, Product.value)):
        value = dot_tn(nr[...], grads_at(which)[...])
        base = products.index((name, 0)) * product_rows
        for c in range(own_width // 128):
            at = pl.multiple_of(base + (my_group * (own_width // 128) + c) * width, width)
            s.mine[pl.ds(at, width), :] = value[:, c * 128 : (c + 1) * 128].astype(half)
        ticks(Site.weights)

    ticks(Site.rows)
    back_own.wait()
    for k in range(1, depth):
        source_level = (level + k) % depth
        back_copy(source_level, source_level).wait_recv()

    def first_norm(r, carry):
        at = row_span(r)
        grad = s.back[0, at, :].astype(full)
        for part in range(1, chips):
            grad = grad + s.back[part, at, :].astype(full)
        scaled, inverse = centred_rows(s.pooled[at, :])
        low = s.grad_resid[at, :] + norm_back(grad, scaled, inverse, gain_one[...])
        low = low.astype(half)
        s.normed[at, :] = low
        for k in range(3):
            put_third(6 + k, dot_nt(low, s.pool_w[k * width : (k + 1) * width, :]))
        for c in range(lanes):
            lane = slice(c * 128, (c + 1) * 128)
            s.edge_out[r, :, lane] = stage[c, 0:8, :]
            s.edge_end[r, :, lane] = stage[c, 3 * block - 8 : 3 * block + 8, :]
            s.raised[r, :, lane] = stage[c, 8 : 8 + 3 * block, :].astype(half)
        return (
            carry[0] + jnp.sum(grad * scaled, axis=0, keepdims=True),
            carry[1] + jnp.sum(grad, axis=0, keepdims=True),
            carry[2] + jnp.sum(low.astype(full), axis=0, keepdims=True),
        )

    output_copy.wait()
    for k in range(1, depth):
        row_from((level + k) % depth).wait_send()
    nothing = jnp.zeros((1, width), full)
    totals = (nothing,) * 3
    for r in range(rows):
        totals = first_norm(r, totals)
        ticks(Site.norm_one)
    put_small(Small.gain_one, 0, totals[0])
    put_small(Small.shift_one, 0, totals[1])
    put_small(Small.pool_bias, 0, totals[2])
    edge_copy = remote(
        s.edge_out, s.edge_in, s.rim_sem.at[2], s.rim_sem.at[3],
        (place.batch, (me + size.seq - 1) % size.seq),
    )

    @pl.when(me > 0)
    def _():
        edge_copy.start()

    small = SumSmall(place, small_block, s.small_landing,
                     [s.small_sem.at[0], s.small_sem.at[1]])
    small.send(0)
    for k in range(3):
        at = slice(k * width, (k + 1) * width)
        put_product(tile_at(Product.pool, k, 0), dot_tn(s.groups[:, at], s.normed[...]))
        ticks(Site.pool)

    @pl.when(me < size.seq - 1)
    def _():
        edge_copy.wait_recv()

    edge_row = lax.broadcasted_iota(jnp.int32, (16, width), 0)
    for r in range(rows):
        edge = jnp.where(me < size.seq - 1, s.edge_in[r], 0.0)
        edge = jnp.concatenate([edge, edge], axis=0)
        edge = jnp.where(edge_row >= 14, edge, s.edge_end[r])
        s.raised[r, 3 * block - 16 : 3 * block, :] = edge.astype(half)
    shift_copy = pltpu.make_async_copy(s.raised, shift_hbm, s.own_sem.at[5])
    shift_copy.start()

    rest = [chunk_of[name] for name in finish_order if name in chunk_of]
    small_stage, last_stage = 0, len(place.sizes)
    for number, c in enumerate(rest):
        if reached[c] < big.events:
            sum_step(c)
        if number % 4 == 3 and small_stage < last_stage:
            small.receive(small_stage)
            small_stage += 1
            if small_stage < last_stage:
                small.send(small_stage)
    while small_stage < last_stage:
        small.receive(small_stage)
        small_stage += 1
        if small_stage < last_stage:
            small.send(small_stage)
    for c in range(len(chunks)):
        while reached[c] < big.events:
            sum_step(c)
    small_out[...] = small_block[last_stage]

    shift_copy.wait()

    @pl.when(me < size.seq - 1)
    def _():
        rim_copy.wait_send()

    @pl.when(me > 0)
    def _():
        edge_copy.wait_send()

    for k in range(1, depth):
        other = (level + k) % depth
        back_copy(other, other).wait_send()
    for k in range(depth):
        across(k, core).wait_send()
        pair_copy(k).wait_send()
    for k in range(1, size.seq):
        other = (me + k) % size.seq
        att_copy(other, other // per_row, other % per_row, other).wait_send()
        grad_copy(other, other).wait_send()
    big.finish()
    small.finish()


def scratch_plan(size, chunks):
    tokens, length, width, hidden = size.tokens, size.length, size.width, size.hidden
    rows, block, depth = size.rows, size.block, size.depth
    own, pairs, heads = size.own_width, size.pairs, size.own_heads
    near = size.reach + 1
    stages = stage_sizes(size.batch, size.seq)
    orders = axis_orders(size, len(chunks))
    slots = sum_slots(size.batch, size.seq)
    dma = pltpu.SemaphoreType.DMA
    total = sum(chunks)
    return dict(
        x=pltpu.VMEM((2, 3 * block, width), half),
        raised=pltpu.VMEM((rows, 3 * block, width), half),
        pool_w=pltpu.VMEM((3 * width, width), half),
        up_w=pltpu.VMEM((width, 3 * width), half),
        query_w=pltpu.VMEM((width, own), half),
        key_w=pltpu.VMEM((width, own), half),
        value_w=pltpu.VMEM((width, own), half),
        outer_w=pltpu.VMEM((hidden, width), half),
        inner_w=pltpu.VMEM((width, hidden), half),
        out_w=pltpu.VMEM((width, width), half),
        rim=pltpu.VMEM((rows, 16, width), half),
        stage=pltpu.VMEM((size.lanes, 3 * block + 8, 128), full),
        groups=pltpu.VMEM((tokens, 3 * width), half),
        dy=pltpu.VMEM((tokens, 3 * width), half),
        grad_resid=pltpu.VMEM((tokens, width), full),
        grad_branch=pltpu.VMEM((tokens, width), half),
        pooled=pltpu.VMEM((tokens, width), full),
        normed=pltpu.VMEM((tokens, width), half),
        nr=pltpu.VMEM((length, width), half),
        grad_inner=pltpu.VMEM((tokens, hidden), half),
        activated=pltpu.VMEM((tokens, hidden), half),
        qt=pltpu.VMEM((heads, 128, length), half),
        kt=pltpu.VMEM((heads, 80, length), half),
        vt=pltpu.VMEM((own, length), half),
        k=pltpu.VMEM((pairs, length, 128), half),
        v=pltpu.VMEM((pairs, length, 128), half),
        work=pltpu.VMEM((2 * near, size.span, size.span), full),
        expo=pltpu.VMEM((heads, len(size.tiles), size.span, size.span), half),
        inverse=pltpu.VMEM((heads, 8, length), full),
        mixed=pltpu.VMEM((own, length), full),
        att_out=pltpu.VMEM((length, own), half),
        att=pltpu.VMEM((tokens, width), half),
        residual=pltpu.VMEM((tokens, width), full),
        normed_two=pltpu.VMEM((tokens, width), half),
        grad_att=pltpu.VMEM((tokens, width), half),
        grad_heads=pltpu.VMEM((length, own), half),
        slope_sum=pltpu.VMEM((heads, 8, size.span), full),
        pair_in=pltpu.VMEM((depth * block, width), half),
        back=pltpu.VMEM((size.chips_per_row, tokens, width), half),
        edge_out=pltpu.VMEM((rows, 8, width), full),
        edge_in=pltpu.VMEM((rows, 8, width), full),
        edge_end=pltpu.VMEM((rows, 16, width), full),
        mine=pltpu.VMEM((total, 128), half),
        landing=pltpu.VMEM((SumPieces.landing_rows(size.batch, size.seq, chunks, orders), 128), half),
        piece=pltpu.VMEM((total // (size.batch * size.seq), 128), half),
        small_block=pltpu.VMEM((len(stages) + 1, small_rows, 128), full),
        small_landing=pltpu.VMEM((sum(stages), small_rows, 128), full),
        load_sem=dma((10,)),
        x_sem=dma((2,)),
        rim_sem=dma((4,)),
        own_sem=dma((6,)),
        row_sent=dma((depth,)),
        row_got=dma((depth,)),
        across_sent=dma((depth,)),
        across_got=dma((depth,)),
        att_sent=dma((size.seq,)),
        att_got=dma((size.seq,)),
        grad_sent=dma((size.seq,)),
        grad_got=dma((size.seq,)),
        pair_sent=dma((depth,)),
        pair_got=dma((depth,)),
        back_sent=dma((depth,)),
        back_got=dma((depth,)),
        sum_sem=dma((4, len(chunks), slots)),
        keep_sem=dma((len(chunks),)),
        small_sem=dma((2, slots)),
    )


def widen_kernel(plan, steps, places, sums, shift, cotangent, small, *refs):
    outs = dict(zip(plan, refs[: len(plan)]))
    grad_inputs = refs[len(plan)]
    vectors = refs[len(plan) + 1 : len(plan) + 1 + len(places)]
    source, target, moved, kept, result, load_sem, store_sem, row_sem = refs[
        len(plan) + 1 + len(places) :
    ]
    rows = shift.shape[0]
    deep = source.shape[0]
    product_rows = source.shape[1]
    width = target.shape[1]

    def load(i):
        return pltpu.make_async_copy(
            sums.at[pl.ds(i * product_rows, product_rows), :], source.at[i % deep],
            load_sem.at[i % deep],
        )

    def store(i):
        name, part = steps[i]
        out = outs[name]
        if out.shape[0] > width:
            out = out.at[pl.ds(part * width, width), :]
        elif out.shape[1] > width:
            out = out.at[:, pl.ds(part * width, width)]
        return pltpu.make_async_copy(target.at[i % deep], out, store_sem.at[i % deep])

    def row_loads(r):
        return (
            pltpu.make_async_copy(shift.at[r], moved.at[r % 2], row_sem.at[0, r % 2]),
            pltpu.make_async_copy(cotangent.at[r], kept.at[r % 2], row_sem.at[1, r % 2]),
        )

    def row_store(r):
        return pltpu.make_async_copy(result.at[r % 2], grad_inputs.at[r], row_sem.at[2, r % 2])

    for i in range(deep - 1):
        load(i).start()
    for at, out in zip(places, vectors):
        count = out.shape[-1]
        for c in range(0, count, 128):
            part = min(128, count - c)
            if len(out.shape) == 1:
                out[c : c + part] = small[at + c // 128, :part]
            else:
                out[:, c : c + part] = small[at + c // 128 : at + c // 128 + 1, :part]
    for copy in row_loads(0):
        copy.start()
    for r in range(rows):
        if r + 1 < rows:
            for copy in row_loads(r + 1):
                copy.start()
        for copy in row_loads(r):
            copy.wait()
        if r >= 2:
            row_store(r - 2).wait()

        def add_rows(b, carry):
            at = pl.ds(pl.multiple_of(b * 64, 64), 64)
            result[r % 2, at, :] = moved[r % 2, at, :].astype(full) + kept[
                r % 2, at, :
            ].astype(full)
            return carry

        lax.fori_loop(0, result.shape[1] // 64, add_rows, 0)
        row_store(r).start()
    for i in range(len(steps)):
        if i + deep - 1 < len(steps):
            load(i + deep - 1).start()
        load(i).wait()
        if i >= deep:
            store(i - deep).wait()

        def convert(b, carry):
            at = pl.multiple_of(b * 64, 64)
            for c in range(product_rows // width):
                target[i % deep, pl.ds(at, 64), c * 128 : (c + 1) * 128] = source[
                    i % deep, pl.ds(c * width + at, 64), :
                ].astype(full)
            return carry

        lax.fori_loop(0, width // 64, convert, 0)
        store(i).start()
    for r in range(max(0, rows - 2), rows):
        row_store(r).wait()
    for i in range(max(0, len(steps) - deep), len(steps)):
        store(i).wait()


def widen(sums, shift, cotangent, small, counts, shapes, steps):
    any_space = pl.BlockSpec(memory_space=pl.ANY)
    names = tuple(shapes)
    width = shift.shape[2]
    deep = 9
    outs = [jax.ShapeDtypeStruct(shapes[name], full) for name in names]
    outs.append(jax.ShapeDtypeStruct(shift.shape, full))
    outs += [
        jax.ShapeDtypeStruct(
            (count,) if count % 1024 == 512 and count > 512 else (1, count), full
        )
        for count in counts.values()
    ]
    vmem = pl.BlockSpec(memory_space=pltpu.VMEM)
    row = shift.shape[1:]
    product_rows = sums.shape[0] // len(steps)
    results = pl.pallas_call(
        functools.partial(widen_kernel, names, steps, tuple(counts)),
        out_shape=outs,
        in_specs=[any_space] * 3 + [vmem],
        out_specs=[any_space] * (len(names) + 1) + [vmem] * len(counts),
        scratch_shapes=[
            pltpu.VMEM((deep, product_rows, 128), half),
            pltpu.VMEM((deep, width, width), full),
            pltpu.VMEM((2,) + row, half),
            pltpu.VMEM((2,) + row, half),
            pltpu.VMEM((2,) + row, full),
            pltpu.SemaphoreType.DMA((deep,)),
            pltpu.SemaphoreType.DMA((deep,)),
            pltpu.SemaphoreType.DMA((3, 2)),
        ],
        name="widen",
    )(sums, shift, cotangent, small)
    vectors = {
        at: value.reshape(-1) for at, value in zip(counts, results[len(names) + 1 :])
    }
    return dict(zip(names, results)), results[len(names)], vectors


def local(
    inputs,
    cotangent,
    doc_lengths,
    pool_weight,
    pool_bias,
    gain_one,
    shift_one,
    query_weight,
    key_weight,
    value_weight,
    out_weight,
    slopes,
    gain_two,
    shift_two,
    inner_weight,
    inner_bias,
    outer_weight,
    outer_bias,
    up_weight,
    up_bias,
):
    rows, block_len, width = inputs.shape
    hidden = inner_weight.shape[1]
    size = Sizes(
        lax.axis_size("batch"), lax.axis_size("seq"), rows, block_len // 3, width,
        hidden, slopes.shape[0],
    )
    steps = product_list(size.parts)
    product_rows = width * size.lanes
    chunks = [2 * product_rows] * (len(steps) // 2)
    if product_rows % (16 * size.batch * size.seq) == 0:
        chunks[-1:] = [product_rows] * 2
    total = len(steps) * product_rows
    vmem = pl.BlockSpec(memory_space=pltpu.VMEM)
    smem = pl.BlockSpec(memory_space=pltpu.SMEM)
    any_space = pl.BlockSpec(memory_space=pl.ANY)
    plan = scratch_plan(size, chunks)
    vectors = (
        pool_bias, gain_one, shift_one, gain_two, shift_two, inner_bias, outer_bias, up_bias,
    )
    output, shift, sums, small = pl.pallas_call(
        functools.partial(layer_kernel, size, chunks),
        out_shape=(
            jax.ShapeDtypeStruct(inputs.shape, half),
            jax.ShapeDtypeStruct(inputs.shape, half),
            jax.ShapeDtypeStruct((total, 128), half),
            jax.ShapeDtypeStruct((small_rows, 128), full),
        ),
        in_specs=[smem, smem] + [vmem] * 8 + [any_space] * 10,
        out_specs=(any_space, any_space, any_space, vmem),
        scratch_shapes=list(plan.values()),
        compiler_params=pltpu.CompilerParams(
            collective_id=0, has_side_effects=True, vmem_limit_bytes=67043328
        ),
        name="layer",
    )(
        doc_lengths, slopes, *(v.reshape(1, -1) for v in vectors[:-1]), up_bias,
        inputs, cotangent, pool_weight, query_weight, key_weight, value_weight,
        out_weight, inner_weight, outer_weight, up_weight,
    )
    shapes = {
        Product.inner: inner_weight.shape, Product.outer: outer_weight.shape, Product.up: up_weight.shape,
        Product.out: out_weight.shape, Product.query: query_weight.shape, Product.key: key_weight.shape,
        Product.value: value_weight.shape, Product.pool: pool_weight.shape,
    }
    counts = {
        Small.pool_bias: width, Small.gain_one: width, Small.shift_one: width,
        Small.slopes: slopes.shape[0], Small.gain_two: width, Small.shift_two: width,
        Small.inner_bias: hidden, Small.outer_bias: width, Small.up_bias: 3 * width,
    }
    grads, input_grad, vector = widen(sums, shift, cotangent, small, counts, shapes, steps)

    return (
        output,
        input_grad,
        grads[Product.pool],
        vector[Small.pool_bias],
        vector[Small.gain_one],
        vector[Small.shift_one],
        grads[Product.query],
        grads[Product.key],
        grads[Product.value],
        grads[Product.out],
        vector[Small.slopes],
        vector[Small.gain_two],
        vector[Small.shift_two],
        grads[Product.inner],
        vector[Small.inner_bias],
        grads[Product.outer],
        vector[Small.outer_bias],
        grads[Product.up],
        vector[Small.up_bias],
    )


def solution(mesh):
    blocks = P("batch", "seq", None)
    in_specs = (blocks, blocks, P("batch", None)) + (P(),) * 17
    out_specs = (blocks, blocks) + (P(),) * 17
    return jax.shard_map(local, mesh=mesh, in_specs=in_specs, out_specs=out_specs, check_vma=False)
```
